32 devices in a mesh: dp: 8 (over y, x, core), tensor: 4 (over z).
Axes of the slice: x: 2, y: 2, z: 4, core: 2. Of those that a mesh axis runs over, the one named last changes fastest.
Arguments:
- inputs: bfloat16 [8192, 512], P(('dp', 'tensor'))
- out_grad: bfloat16 [8192, 512], P(('dp', 'tensor')), may hold values from -6 to 6
- norm_gains: float32 [5, 512], P(None, ('dp', 'tensor')), may hold values from 0.5 to 1.5
- first_up: bfloat16 [512, 2048], P('dp', 'tensor'), may hold values from -0.25 to 0.25
- first_down: bfloat16 [2048, 512], P('tensor', 'dp'), may hold values from -0.125 to 0.125
- attend_in: bfloat16 [4, 512, 512], P(None, 'dp', 'tensor'), may hold values from -0.25 to 0.25
- attend_out: bfloat16 [512, 512], P('tensor', 'dp'), may hold values from -1 to 1
- position_bias: bfloat16 [2, 8, 64], P(None, 'tensor', 'dp'), may hold values from -3 to 3
- convolve_in: bfloat16 [512, 2, 512], P('dp', None, 'tensor'), may hold values from -0.25 to 0.25
- depth_kernel: float32 [512, 31], P('tensor'), may hold values from -1 to 1
- batch_norm: float32 [2, 512], P(None, 'tensor'), may hold values from 0.5 to 1.5
- convolve_out: bfloat16 [512, 512], P('tensor', 'dp'), may hold values from -0.25 to 0.25
- second_up: bfloat16 [512, 2048], P('dp', 'tensor'), may hold values from -0.25 to 0.25
- second_down: bfloat16 [2048, 512], P('tensor', 'dp'), may hold values from -0.125 to 0.125
Outputs:
- output_rows: float32 [8192, 512], P(('dp', 'tensor'))
- input_grad: float32 [8192, 512], P(('dp', 'tensor'))
- grad_norm_gains: float32 [5, 512], P(None, ('dp', 'tensor'))
- grad_first_up: float32 [512, 2048], P('dp', 'tensor')
- grad_first_down: float32 [2048, 512], P('tensor', 'dp')
- grad_attend_in: float32 [4, 512, 512], P(None, 'dp', 'tensor')
- grad_attend_out: float32 [512, 512], P('tensor', 'dp')
- grad_position_bias: float32 [2, 8, 64], P(None, 'tensor', 'dp')
- grad_convolve_in: float32 [512, 2, 512], P('dp', None, 'tensor')
- grad_depth_kernel: float32 [512, 31], P('tensor')
- grad_batch_norm: float32 [2, 512], P(None, 'tensor')
- grad_convolve_out: float32 [512, 512], P('tensor', 'dp')
- grad_second_up: float32 [512, 2048], P('dp', 'tensor')
- grad_second_down: float32 [2048, 512], P('tensor', 'dp')
The draws below stay inside these ranges and needn't reach their ends.
All inputs are finite; a program needn't handle non-finite values.
Results may differ from the reference program's by a relative error of at most 0.023.
Values may be sent and summed in bfloat16 or wider, within the bound.
A program may use at most 128 MiB of HBM per device.

```python
import math
import jax
import jax.numpy as jnp
from jax import lax

D = 512
HEADS = 8
DH = 64
FF = 2048
KERNEL = 31
FRAMES = 1024
BLOCK = 512
UTTS = 8
TOKENS = 8192


def draw_inputs(key, part):
    noise_key = jax.random.fold_in(key, 11)
    shape_key = jax.random.fold_in(key, 23)
    noise = jnp.clip(jax.random.normal(noise_key, (TOKENS, D), jnp.float32), -4.0, 4.0)
    top_level = 4.0
    pattern = jnp.clip(jax.random.normal(shape_key, (D,), jnp.float32), -3.0, 3.0)
    utterance = jnp.arange(TOKENS, dtype=jnp.int32) // FRAMES
    ramp = utterance.astype(jnp.float32) / max(UTTS - 1, 1)
    strength = 0.5 + (top_level - 0.5) * ramp
    return (noise + strength[:, None] * pattern[None, :]).astype(jnp.bfloat16)


def shard_levels(stream_key, dims, split, smallest, top_value):
    factor_of, own = 1.0, jax.random.fold_in(stream_key, 6)
    for axis_at, blocks in split:
        heights = jnp.exp(jax.random.uniform(jax.random.fold_in(own, axis_at), (blocks,), jnp.float32, smallest / len(split), top_value / len(split)))
        factor_of = factor_of * jnp.repeat(heights, dims[axis_at] // blocks).reshape([-1 if axis == axis_at else 1 for axis in range(len(dims))])
    return factor_of


def normal_values(stream_key, shape, spread, limit, pieces=(), kind=jnp.bfloat16):
    drawn = jax.random.normal(stream_key, shape, jnp.float32) * spread
    if len(pieces) > 0:
        drawn = shard_levels(stream_key, shape, pieces, -0.22, 0.18) * drawn
    return jnp.clip(drawn, min=-limit, max=limit).astype(kind)


def setup_inputs(seed: int = 0) -> dict:
    streams_of = jax.random.split(jax.random.key(seed), 15)
    return {
        "inputs": draw_inputs(jax.random.fold_in(streams_of[14], 71), 0),
        "out_grad": normal_values(streams_of[1], (TOKENS, D), 1.0, 6.0, ((0, 32),)),
        "norm_gains": jnp.clip(1.0 + 0.1 * jax.random.normal(streams_of[2], (5, D), jnp.float32), 0.5, 1.5),
        "first_up": normal_values(streams_of[3], (D, FF), D ** -0.5, 0.25, ((0, 8), (1, 4))),
        "first_down": normal_values(streams_of[4], (FF, D), FF ** -0.5, 0.125, ((0, 4), (1, 8))),
        "attend_in": normal_values(streams_of[5], (4, D, D), D ** -0.5, 0.25, ((1, 8), (2, 4))),
        "attend_out": normal_values(streams_of[6], (D, D), (D // 16) ** -0.5, 1.0, ((0, 4), (1, 8))),
        "position_bias": normal_values(streams_of[7], (2, HEADS, DH), 0.5, 3.0, ((1, 4), (2, 8))),
        "convolve_in": normal_values(streams_of[8], (D, 2, D), D ** -0.5, 0.25, ((0, 8), (2, 4))),
        "depth_kernel": normal_values(streams_of[9], (D, KERNEL), KERNEL ** -0.5, 1.0, ((0, 4),), jnp.float32),
        "batch_norm": jnp.clip(0.5 + 1.0 * jax.random.uniform(streams_of[10], (2, D), jnp.float32) ** shard_levels(streams_of[10], (2, D), ((1, 4),), -0.2, 0.2), 0.5, 1.5),
        "convolve_out": normal_values(streams_of[11], (D, D), D ** -0.5, 0.25, ((0, 4), (1, 8))),
        "second_up": normal_values(streams_of[12], (D, FF), D ** -0.5, 0.25, ((0, 8), (1, 4))),
        "second_down": normal_values(streams_of[13], (FF, D), FF ** -0.5, 0.125, ((0, 4), (1, 8))),
    }


@jax.custom_vjp
def low(v):
    return lax.optimization_barrier(v.astype(jnp.bfloat16)).astype(jnp.float32)

@jax.custom_vjp
def low_back(v):
    return v

def low_keep(v):
    return (low(v), None)

def low_pass(kept, grad):
    return (grad,)

def back_keep(v):
    return (v, None)

def back_low(kept, grad):
    return (low(grad),)
low.defvjp(low_keep, low_pass)
low_back.defvjp(back_keep, back_low)
norm_eps = 1e-05

def matmul_high(left, right):
    return jnp.dot(left, right, precision=lax.Precision.HIGHEST, preferred_element_type=jnp.float32)

def einsum_high(form, left, right):
    return jnp.einsum(form, left, right, precision=lax.Precision.HIGHEST, preferred_element_type=jnp.float32)

def norm_rows(values, gain_row):
    centred = values - lax.optimization_barrier(jnp.mean(values, axis=-1, keepdims=True))
    variance = lax.optimization_barrier(jnp.mean(centred * centred, axis=-1, keepdims=True))
    return centred * lax.rsqrt(variance + norm_eps) * gain_row

def swish_act(values):
    return values * jax.nn.sigmoid(values)

def position_table():
    row_index = jnp.arange(2 * FRAMES - 1, dtype=jnp.float32)
    distance = FRAMES - 1 - row_index
    frequency = jnp.exp(jnp.arange(D // 2, dtype=jnp.float32) * (-2.0 * math.log(10000.0) / D))
    angles = distance[:, None] * frequency[None, :]
    sinusoid = jnp.concatenate([jnp.sin(angles), jnp.cos(angles)], axis=1)
    return low(sinusoid)

def skew_rows(wide_scores, frames):
    head_count, block_rows, full_width = wide_scores.shape
    flattened = wide_scores.reshape(head_count, block_rows * full_width)
    trimmed = lax.slice_in_dim(flattened, block_rows - 1, block_rows - 1 + block_rows * (full_width - 1), axis=1)
    return trimmed.reshape(head_count, block_rows, full_width - 1)[:, :, :frames]

def feed_layer(residual, gain_row, up_weight, down_weight):

    def one_utterance(utterance):
        normed = low(norm_rows(utterance, gain_row))
        pre_act = low_back(matmul_high(normed, up_weight))
        hidden = low(swish_act(pre_act))
        return low_back(matmul_high(hidden, down_weight))
    branch = lax.map(jax.checkpoint(one_utterance), residual.reshape(UTTS, FRAMES, D))
    return residual + 0.5 * branch.reshape(TOKENS, D)

def attend_one(normed, weights, bias_pair, positions):
    score_scale = DH ** (-0.5)
    queries = low_back(matmul_high(normed, weights[0])).reshape(FRAMES, HEADS, DH)
    key_rows = low(low_back(matmul_high(normed, weights[1]))).reshape(FRAMES, HEADS, DH)
    value_rows = low(low_back(matmul_high(normed, weights[2]))).reshape(FRAMES, HEADS, DH)
    content_q = low(queries + bias_pair[0])
    position_q = low(queries + bias_pair[1])
    pos_span = BLOCK + FRAMES - 1

    def one_block(row_start):
        content_blk = lax.dynamic_slice_in_dim(content_q, row_start, BLOCK, 0)
        position_blk = lax.dynamic_slice_in_dim(position_q, row_start, BLOCK, 0)
        pos_blk = lax.dynamic_slice_in_dim(positions, FRAMES - BLOCK - row_start, pos_span, 0)
        content = einsum_high('bhe,fhe->hbf', content_blk, key_rows)
        wide_scores = einsum_high('bhe,mhe->hbm', position_blk, pos_blk)
        scores = low_back((content + skew_rows(wide_scores, FRAMES)) * score_scale)
        softmax_w = low(jax.nn.softmax(scores, axis=-1))
        return einsum_high('hbf,fhe->bhe', softmax_w, value_rows)
    starts = jnp.arange(FRAMES // BLOCK, dtype=jnp.int32) * BLOCK
    mixture = lax.map(jax.checkpoint(one_block), starts)
    return low(low_back(mixture.reshape(FRAMES, D)))

def attention_layer(residual, gain_row, weights, out_weight, bias_pair, sinusoid):
    normed = low(norm_rows(residual, gain_row))
    positions = low(matmul_high(sinusoid, weights[3])).reshape(2 * FRAMES - 1, HEADS, DH)

    def one_utterance(utterance):
        return attend_one(utterance, weights, bias_pair, positions)
    mixture = lax.map(jax.checkpoint(one_utterance), normed.reshape(UTTS, FRAMES, D))
    return residual + low_back(matmul_high(mixture.reshape(TOKENS, D), out_weight))

def convolve_layer(residual, gain_row, convolve_in, depth_kernel, batch_norm, convolve_out):
    normed = low(norm_rows(residual, gain_row))
    pre_act = low_back(matmul_high(normed, convolve_in.reshape(D, 2 * D)))
    gated_rows = (pre_act[:, :D] * jax.nn.sigmoid(pre_act[:, D:])).reshape(UTTS, FRAMES, D)
    half_width = KERNEL // 2
    padded = jnp.pad(gated_rows, ((0, 0), (half_width, half_width), (0, 0)))
    convolved = jnp.zeros_like(gated_rows)
    for tap_index in range(KERNEL):
        convolved = convolved + depth_kernel[:, tap_index] * padded[:, tap_index:tap_index + FRAMES, :]
    batch_mean = lax.optimization_barrier(jnp.mean(convolved, axis=(0, 1)))
    variance = lax.optimization_barrier(jnp.mean(convolved * convolved, axis=(0, 1))) - batch_mean * batch_mean
    normal_out = (convolved - batch_mean) * lax.rsqrt(variance + norm_eps) * batch_norm[0] + batch_norm[1]
    activated = low(swish_act(normal_out))
    return residual + low_back(matmul_high(activated.reshape(TOKENS, D), convolve_out))

def forward(residual, norm_gains, first_up, first_down, attend_in, attend_out, position_bias, convolve_in, depth_kernel, batch_norm, convolve_out, second_up, second_down):
    sinusoid = position_table()
    residual = feed_layer(residual, norm_gains[0], first_up, first_down)
    residual = attention_layer(residual, norm_gains[1], attend_in, attend_out, position_bias, sinusoid)
    residual = convolve_layer(residual, norm_gains[2], convolve_in, depth_kernel, batch_norm, convolve_out)
    residual = feed_layer(residual, norm_gains[3], second_up, second_down)
    return norm_rows(residual, norm_gains[4])

def reference(inputs, out_grad, norm_gains, first_up, first_down, attend_in, attend_out, position_bias, convolve_in, depth_kernel, batch_norm, convolve_out, second_up, second_down):
    output_rows, pullback = jax.vjp(forward, inputs.astype(jnp.float32), norm_gains.astype(jnp.float32), first_up.astype(jnp.float32), first_down.astype(jnp.float32), attend_in.astype(jnp.float32), attend_out.astype(jnp.float32), position_bias.astype(jnp.float32), convolve_in.astype(jnp.float32), depth_kernel.astype(jnp.float32), batch_norm.astype(jnp.float32), convolve_out.astype(jnp.float32), second_up.astype(jnp.float32), second_down.astype(jnp.float32))
    gradients = pullback(out_grad.astype(jnp.float32))
    return (output_rows, gradients[0], gradients[1], gradients[2], gradients[3], gradients[4], gradients[5], gradients[6], gradients[7], gradients[8], gradients[9], gradients[10], gradients[11], gradients[12])
```

```python
import functools
import math

import jax
import jax.numpy as jnp
from jax import lax
from jax.experimental import pallas as pl
from jax.experimental.pallas import tpu as pltpu
from jax.sharding import PartitionSpec as P

MESH = pl.DeviceIdType.MESH
CHUNKS = 6
CORE = 1


def flip(index, mask):
    result = index
    bit = 1
    while bit <= mask:
        if mask & bit:
            result = result + bit - 2 * bit * ((index // bit) % 2)
        bit *= 2
    return result


def span(bits):
    masks = [0]
    for bit in bits:
        masks = masks + [mask ^ bit for mask in masks]
    return masks


def link_orders(n_dp):
    bits = [1 << k for k in range(1, n_dp.bit_length() - 1)]
    return (bits, bits[::-1])


def greet(peers):
    barrier = pltpu.get_barrier_semaphore()
    for peer in peers:
        pl.semaphore_signal(barrier, inc=1, device_id=peer, device_id_type=MESH)
    pl.semaphore_wait(barrier, len(peers))


def tensor_peers(d, t, n_t):
    return [(d, lax.rem(t + step, n_t)) for step in range(1, n_t)]


def remote(src, dst, send_sem, recv_sem, peer):
    return pltpu.make_async_remote_copy(
        src_ref=src, dst_ref=dst, send_sem=send_sem, recv_sem=recv_sem,
        device_id=peer, device_id_type=MESH)


def gather_body(n_dp, n_t, p_ref, e_ref, f_ref, g_ref, ge_ref, gf_ref, local_sem, z_send, z_recv, d_send, d_recv,
                fz_send, fz_recv):
    d = lax.axis_index("dp")
    t = lax.axis_index("tensor")
    rows, width = p_ref.shape[1], p_ref.shape[2]
    e_rows = e_ref.shape[0]
    half = n_t * width // 2
    orders = [order + [CORE] for order in link_orders(n_dp)]
    stages = len(orders[0])
    z_peers = tensor_peers(d, t, n_t)
    greet(z_peers + [(flip(d, bit), t) for bit in orders[0]])

    def block(c, mask, start, size):
        if c == CHUNKS:
            return ge_ref.at[:, pl.ds(pl.multiple_of(flip(d, mask) * e_rows, e_rows), e_rows), :]
        first = pl.multiple_of(flip(d, mask) * rows, rows)
        return g_ref.at[c, pl.ds(first, rows), pl.ds(start, size)]

    def own(c):
        if c == CHUNKS:
            return ge_ref.at[t, pl.ds(pl.multiple_of(d * e_rows, e_rows), e_rows), :]
        return block(c, 0, pl.multiple_of(t * width, width), width)

    def source(c):
        return e_ref if c == CHUNKS else p_ref.at[c]

    def z_copy(c, step):
        return remote(source(c), own(c), z_send.at[c, step], z_recv.at[c, step], z_peers[step])

    def f_copy(step):
        return remote(f_ref, gf_ref.at[t], fz_send.at[step], fz_recv.at[step], z_peers[step])

    def local_copy(c):
        return pltpu.make_async_copy(source(c), own(c), local_sem.at[c])

    def dp_copies(c, stage):
        copies = []
        for h in range(1 if c == CHUNKS else 2):
            bit = orders[h][stage]
            masks = span(orders[h][:stage])
            for j, mask in enumerate(masks):
                slot = len(masks) - 1 + j
                window = block(c, mask, h * half, half)
                copies.append(remote(window, window, d_send.at[c, h, slot], d_recv.at[c, h, slot], (flip(d, bit), t)))
        return copies

    everything = [CHUNKS] + list(range(CHUNKS))
    own_f = pltpu.make_async_copy(f_ref, gf_ref.at[t], local_sem.at[CHUNKS + 1])
    own_f.start()
    for c in everything:
        local_copy(c).start()
        for step in range(n_t - 1):
            z_copy(c, step).start()
        if c == CHUNKS:
            for step in range(n_t - 1):
                f_copy(step).start()
    for tick in range(len(everything) + stages):
        for stage in range(stages + 1):
            place = tick - stage
            if 0 <= place < len(everything):
                c = everything[place]
                if stage == 0:
                    local_copy(c).wait()
                    for step in range(n_t - 1):
                        z_copy(c, step).wait_recv()
                else:
                    for copy in dp_copies(c, stage - 1):
                        copy.wait_recv()
                if stage < stages:
                    for copy in dp_copies(c, stage):
                        copy.start()
    for step in range(n_t - 1):
        f_copy(step).wait()
    own_f.wait()
    for c in everything:
        for step in range(n_t - 1):
            z_copy(c, step).wait_send()
        for stage in range(stages):
            for copy in dp_copies(c, stage):
                copy.wait_send()


def gather_weights(n_dp, n_t, packed, small, taps):
    _, rows, width = packed.shape
    e_rows = small.shape[0]
    dma = pltpu.SemaphoreType.DMA
    vmem = pl.BlockSpec(memory_space=pltpu.VMEM)
    hbm = pl.BlockSpec(memory_space=pl.ANY)
    return pl.pallas_call(
        functools.partial(gather_body, n_dp, n_t),
        name="gather_weights",
        out_shape=(
            jax.ShapeDtypeStruct((CHUNKS, n_dp * rows, n_t * width), packed.dtype),
            jax.ShapeDtypeStruct((n_t, n_dp * e_rows, 128), jnp.float32),
            jax.ShapeDtypeStruct((n_t,) + taps.shape, jnp.float32)),
        in_specs=[vmem, vmem, vmem],
        out_specs=(hbm, hbm, hbm),
        scratch_shapes=[
            dma((CHUNKS + 2,)), dma((CHUNKS + 1, n_t - 1)), dma((CHUNKS + 1, n_t - 1)),
            dma((CHUNKS + 1, 2, n_dp - 1)), dma((CHUNKS + 1, 2, n_dp - 1)),
            dma((n_t - 1,)), dma((n_t - 1,))],
        compiler_params=pltpu.CompilerParams(collective_id=0, has_side_effects=True, vmem_limit_bytes=16 << 20),
    )(packed, small, taps)


def fold_body(n_dp, n_t, x_ref, s_ref, o_ref, so_ref, acc, core_buf, dp_buf, z_buf, small_acc, small_buf, small_z,
              local_sem, core_send, core_recv, d_send, d_recv, z_send, z_recv, s_send, s_recv, sz_send, sz_recv):
    d = lax.axis_index("dp")
    t = lax.axis_index("tensor")
    rows, width = o_ref.shape[1], o_ref.shape[2]
    half = n_t * width // 2
    orders = [order[::-1] for order in link_orders(n_dp)]
    stages = len(orders[0])
    z_peers = tensor_peers(d, t, n_t)
    all_bits = [CORE] + orders[0]
    greet(z_peers + [(flip(d, bit), t) for bit in all_bits])
    groups = span(link_orders(n_dp)[0])

    def x_block(c, mask):
        return x_ref.at[c, pl.ds(pl.multiple_of(flip(d, mask) * rows, rows), rows), :]

    def local_copy(c, k):
        return pltpu.make_async_copy(x_block(c, groups[k]), acc.at[c, k], local_sem.at[c, k])

    def core_copy(c, k):
        return remote(x_block(c, groups[k] ^ CORE), core_buf.at[c, k], core_send.at[c, k], core_recv.at[c, k],
                      (flip(d, CORE), t))

    def dp_moves(c, stage):
        moves = []
        for h in range(2):
            bit = orders[h][stage]
            masks = span(orders[h][stage + 1:])
            base = len(groups) - 2 * len(masks)
            for j, mask in enumerate(masks):
                slot = base + j
                cols = pl.ds(h * half, half)
                copy = remote(acc.at[c, groups.index(mask ^ bit), :, cols], dp_buf.at[c, h, slot],
                              d_send.at[c, h, slot], d_recv.at[c, h, slot], (flip(d, bit), t))
                moves.append((copy, groups.index(mask), cols, h, slot))
        return moves

    def z_copy(c, step):
        target = lax.rem(t + step + 1, n_t)
        return remote(acc.at[c, 0, :, pl.ds(pl.multiple_of(target * width, width), width)], z_buf.at[c, step],
                      z_send.at[c, step], z_recv.at[c, step], z_peers[step])

    def small_copy(k):
        return remote(small_acc.at[k], small_buf.at[k], s_send.at[k], s_recv.at[k], (flip(d, all_bits[k]), t))

    def small_z_copy(step):
        target = lax.rem(t + step + 1, n_t)
        return remote(small_acc.at[len(all_bits), target], small_z.at[step], sz_send.at[step], sz_recv.at[step],
                      z_peers[step])

    for c in range(CHUNKS):
        for k in range(len(groups)):
            core_copy(c, k).start()
            local_copy(c, k).start()
    small_acc[0] = s_ref[...]
    small_copy(0).start()
    for k in range(1, len(all_bits) + 1):
        small_copy(k - 1).wait_recv()
        small_acc[k] = small_acc[k - 1] + small_buf[k - 1]
        if k < len(all_bits):
            small_copy(k).start()
    for step in range(n_t - 1):
        small_z_copy(step).start()

    def start_stage(c, stage):
        if stage < stages:
            for move in dp_moves(c, stage):
                move[0].start()
        else:
            for step in range(n_t - 1):
                z_copy(c, step).start()

    for tick in range(CHUNKS + stages + 1):
        for stage in range(stages + 2):
            c = tick - stage
            if not 0 <= c < CHUNKS:
                continue
            if stage == 0:
                for k in range(len(groups)):
                    local_copy(c, k).wait()
                    core_copy(c, k).wait_recv()

                def add_core(step, carry, c=c):
                    k = step // 4
                    part = pl.ds(pl.multiple_of(lax.rem(step, 4) * (rows // 4), rows // 4), rows // 4)
                    acc[c, k, part, :] = (acc[c, k, part, :].astype(jnp.float32)
                                          + core_buf[c, k, part, :].astype(jnp.float32)).astype(jnp.bfloat16)
                    return carry
                lax.fori_loop(0, 4 * len(groups), add_core, 0)
                start_stage(c, 0)
            elif stage <= stages:
                for copy, k, cols, h, slot in dp_moves(c, stage - 1):
                    copy.wait_recv()

                    def add_dp(step, carry, c=c, k=k, cols=cols, h=h, slot=slot):
                        part = pl.ds(pl.multiple_of(step * (rows // 4), rows // 4), rows // 4)
                        acc[c, k, part, cols] = (acc[c, k, part, cols].astype(jnp.float32)
                                                 + dp_buf[c, h, slot, part, :].astype(jnp.float32)).astype(jnp.bfloat16)
                        return carry
                    lax.fori_loop(0, 4, add_dp, 0)
                start_stage(c, stage)
            else:
                for step in range(n_t - 1):
                    z_copy(c, step).wait_recv()
                total = acc[c, 0, :, pl.ds(pl.multiple_of(t * width, width), width)].astype(jnp.float32)
                for step in range(n_t - 1):
                    total = total + z_buf[c, step].astype(jnp.float32)
                o_ref[c] = total
    total = small_acc[len(all_bits), t]
    for step in range(n_t - 1):
        small_z_copy(step).wait_recv()
        total = total + small_z[step]
    so_ref[...] = total
    for k in range(len(all_bits)):
        small_copy(k).wait_send()
    for step in range(n_t - 1):
        small_z_copy(step).wait_send()
    for c in range(CHUNKS):
        for k in range(len(groups)):
            core_copy(c, k).wait_send()
        for stage in range(stages):
            for move in dp_moves(c, stage):
                move[0].wait_send()
        for step in range(n_t - 1):
            z_copy(c, step).wait_send()


def fold_weights(n_dp, n_t, partial, small):
    rows, width = partial.shape[1] // n_dp, partial.shape[2] // n_t
    groups = n_dp // 2
    n_bits = n_dp.bit_length() - 1
    dma = pltpu.SemaphoreType.DMA
    vmem = pl.BlockSpec(memory_space=pltpu.VMEM)
    hbm = pl.BlockSpec(memory_space=pl.ANY)
    bf16 = jnp.bfloat16
    return pl.pallas_call(
        functools.partial(fold_body, n_dp, n_t),
        name="fold_weights",
        out_shape=(jax.ShapeDtypeStruct((CHUNKS, rows, width), jnp.float32),
                   jax.ShapeDtypeStruct(small.shape[1:], jnp.float32)),
        in_specs=[hbm, vmem],
        out_specs=(vmem, vmem),
        scratch_shapes=[
            pltpu.VMEM((CHUNKS, groups, rows, n_t * width), bf16),
            pltpu.VMEM((CHUNKS, groups, rows, n_t * width), bf16),
            pltpu.VMEM((CHUNKS, 2, groups - 1, rows, n_t * width // 2), bf16),
            pltpu.VMEM((CHUNKS, n_t - 1, rows, width), bf16),
            pltpu.VMEM((n_bits + 1,) + small.shape, jnp.float32),
            pltpu.VMEM((n_bits,) + small.shape, jnp.float32),
            pltpu.VMEM((n_t - 1,) + small.shape[1:], jnp.float32),
            dma((CHUNKS, groups)), dma((CHUNKS, groups)), dma((CHUNKS, groups)),
            dma((CHUNKS, 2, groups - 1)), dma((CHUNKS, 2, groups - 1)),
            dma((CHUNKS, n_t - 1)), dma((CHUNKS, n_t - 1)),
            dma((n_bits,)), dma((n_bits,)), dma((n_t - 1,)), dma((n_t - 1,))],
        compiler_params=pltpu.CompilerParams(collective_id=1, has_side_effects=True, vmem_limit_bytes=48 << 20),
    )(partial, small)


def spread_body(n_t, x_ref, y_ref, local_sem, send, recv):
    d = lax.axis_index("dp")
    t = lax.axis_index("tensor")
    peers = tensor_peers(d, t, n_t)
    greet(peers)
    local = pltpu.make_async_copy(x_ref, y_ref.at[t], local_sem.at[0])
    local.start()
    copies = [remote(x_ref, y_ref.at[t], send.at[k], recv.at[k], peers[k]) for k in range(n_t - 1)]
    for copy in copies:
        copy.start()
    local.wait()
    for copy in copies:
        copy.wait()


def spread_frames(n_t, rows_block):
    dma = pltpu.SemaphoreType.DMA
    vmem = pl.BlockSpec(memory_space=pltpu.VMEM)
    hbm = pl.BlockSpec(memory_space=pl.ANY)
    return pl.pallas_call(
        functools.partial(spread_body, n_t),
        name="spread_frames",
        out_shape=jax.ShapeDtypeStruct((n_t,) + rows_block.shape, rows_block.dtype),
        in_specs=[vmem],
        out_specs=hbm,
        scratch_shapes=[dma((1,)), dma((n_t - 1,)), dma((n_t - 1,))],
        compiler_params=pltpu.CompilerParams(collective_id=2, has_side_effects=True),
    )(rows_block)


def reduce_frames_body(n_t, x_ref, o_ref, buf, send, recv):
    d = lax.axis_index("dp")
    t = lax.axis_index("tensor")
    peers = tensor_peers(d, t, n_t)
    greet(peers)
    copies = [remote(x_ref.at[lax.rem(t + k + 1, n_t)], buf.at[k], send.at[k], recv.at[k], peers[k])
              for k in range(n_t - 1)]
    for copy in copies:
        copy.start()
    for copy in copies:
        copy.wait_recv()
    rows = o_ref.shape[0]
    size = rows // 8

    def add_part(step, carry):
        part = pl.ds(pl.multiple_of(step * size, size), size)
        total = x_ref[t, part, :].astype(jnp.float32)
        for k in range(n_t - 1):
            total = total + buf[k, part, :].astype(jnp.float32)
        o_ref[part, :] = total
        return carry
    lax.fori_loop(0, 8, add_part, 0)
    for copy in copies:
        copy.wait_send()


def reduce_frames(n_t, partial):
    dma = pltpu.SemaphoreType.DMA
    vmem = pl.BlockSpec(memory_space=pltpu.VMEM)
    return pl.pallas_call(
        functools.partial(reduce_frames_body, n_t),
        name="reduce_frames",
        out_shape=jax.ShapeDtypeStruct(partial.shape[1:], jnp.float32),
        in_specs=[vmem],
        out_specs=vmem,
        scratch_shapes=[pltpu.VMEM((n_t - 1,) + partial.shape[1:], partial.dtype), dma((n_t - 1,)), dma((n_t - 1,))],
        compiler_params=pltpu.CompilerParams(collective_id=3, has_side_effects=True),
    )(partial)


EDGE = 16


def edge_pieces(n_t, source, edges, send, recv):
    d = lax.axis_index("dp")
    t = lax.axis_index("tensor")
    before = (d, lax.rem(t + n_t - 1, n_t))
    after = (d, lax.rem(t + 1, n_t))
    rows = source.shape[1]
    return [remote(source.at[:, pl.ds(0, EDGE), :], edges.at[1], send.at[0], recv.at[0], before),
            remote(source.at[:, pl.ds(rows - EDGE, EDGE), :], edges.at[0], send.at[1], recv.at[1], after)]


def edges_body(n_t, x_ref, e_ref, send, recv):
    d = lax.axis_index("dp")
    t = lax.axis_index("tensor")
    greet([(d, lax.rem(t + n_t - 1, n_t)), (d, lax.rem(t + 1, n_t))])
    copies = edge_pieces(n_t, x_ref, e_ref, send, recv)
    for copy in copies:
        copy.start()
    for copy in copies:
        copy.wait()


def swap_edges(n_t, x):
    dma = pltpu.SemaphoreType.DMA
    vmem = pl.BlockSpec(memory_space=pltpu.VMEM)
    return pl.pallas_call(
        functools.partial(edges_body, n_t),
        name="swap_edges",
        out_shape=jax.ShapeDtypeStruct((2, x.shape[0], EDGE, x.shape[2]), x.dtype),
        in_specs=[vmem],
        out_specs=vmem,
        scratch_shapes=[dma((2,)), dma((2,))],
        compiler_params=pltpu.CompilerParams(collective_id=4, has_side_effects=True),
    )(x)


def totals_body(n_dp, n_t, with_edges, *refs):
    if with_edges:
        s_ref, x_ref, o_ref, e_ref, mine, dp_buf, mid, z_buf, d_send, d_recv, z_send, z_recv, e_send, e_recv = refs
    else:
        s_ref, o_ref, mine, dp_buf, mid, z_buf, d_send, d_recv, z_send, z_recv = refs
    d = lax.axis_index("dp")
    t = lax.axis_index("tensor")
    z_peers = tensor_peers(d, t, n_t)
    d_peers = [(flip(d, mask), t) for mask in range(1, n_dp)]
    greet(z_peers + d_peers)
    if with_edges:
        edge_copies = edge_pieces(n_t, x_ref, e_ref, e_send, e_recv)
    d_copies = [remote(s_ref, dp_buf.at[k], d_send.at[k], d_recv.at[k], d_peers[k]) for k in range(n_dp - 1)]
    for copy in d_copies:
        copy.start()
    if with_edges:
        for copy in edge_copies:
            copy.start()
    total = s_ref[...]
    for k in range(n_dp - 1):
        d_copies[k].wait_recv()
        total = total + dp_buf[k]
    mid[...] = total
    z_copies = [remote(mid, z_buf.at[k], z_send.at[k], z_recv.at[k], z_peers[k]) for k in range(n_t - 1)]
    for copy in z_copies:
        copy.start()
    for k in range(n_t - 1):
        z_copies[k].wait_recv()
        total = total + z_buf[k]
    o_ref[...] = total
    for copy in d_copies + z_copies:
        copy.wait_send()
    if with_edges:
        for copy in edge_copies:
            copy.wait()


def whole_totals(n_dp, n_t, sums, collective_id, edge_rows=None):
    dma = pltpu.SemaphoreType.DMA
    vmem = pl.BlockSpec(memory_space=pltpu.VMEM)
    shape = jax.ShapeDtypeStruct(sums.shape, jnp.float32)
    scratch = [pltpu.VMEM(sums.shape, jnp.float32), pltpu.VMEM((n_dp - 1,) + sums.shape, jnp.float32),
               pltpu.VMEM(sums.shape, jnp.float32), pltpu.VMEM((n_t - 1,) + sums.shape, jnp.float32),
               dma((n_dp - 1,)), dma((n_dp - 1,)), dma((n_t - 1,)), dma((n_t - 1,))]
    args = [sums]
    outs = [shape]
    if edge_rows is not None:
        args.append(edge_rows)
        outs.append(jax.ShapeDtypeStruct((2, edge_rows.shape[0], EDGE, edge_rows.shape[2]), jnp.float32))
        scratch += [dma((2,)), dma((2,))]
    return pl.pallas_call(
        functools.partial(totals_body, n_dp, n_t, edge_rows is not None),
        name="whole_totals",
        out_shape=tuple(outs),
        in_specs=[vmem] * len(args),
        out_specs=tuple([vmem] * len(outs)),
        scratch_shapes=scratch,
        compiler_params=pltpu.CompilerParams(collective_id=collective_id, has_side_effects=True),
    )(*args)


KERNEL = 31
HALF = KERNEL // 2
norm_eps = 1e-05
f32 = jnp.float32
bf16 = jnp.bfloat16


def norm_rows(values):
    centred = values - jnp.mean(values, axis=-1, keepdims=True)
    inverse = lax.rsqrt(jnp.mean(centred * centred, axis=-1, keepdims=True) + norm_eps)
    return centred * inverse, inverse


def norm_back(incoming, gain_row, saved):
    scaled, inverse = saved
    grad_scaled = incoming * gain_row
    inner = jnp.mean(grad_scaled * scaled, axis=-1, keepdims=True)
    grad_in = inverse * (grad_scaled - jnp.mean(grad_scaled, axis=-1, keepdims=True) - scaled * inner)
    return grad_in, jnp.sum(incoming * scaled, axis=0)


def swish_grad(pre_act):
    sigmoid_val = jax.nn.sigmoid(pre_act)
    return sigmoid_val * (1.0 + pre_act * (1.0 - sigmoid_val))


def dot(left, right, left_dim, right_dim):
    return lax.dot_general(left, right, (((left_dim,), (right_dim,)), ((), ())), preferred_element_type=f32)


def feed_forward(residual, gain_row, up, down_t):
    saved = norm_rows(residual)
    normed = (saved[0] * gain_row).astype(bf16)
    pre_act = dot(normed, up, 1, 0)
    hidden = (pre_act * jax.nn.sigmoid(pre_act)).astype(bf16)
    return residual + 0.5 * dot(hidden, down_t, 1, 1), (saved, normed, pre_act, hidden)


def feed_backward(incoming, gain_row, up, down_t, stored):
    saved, normed, pre_act, hidden = stored
    grad_branch = (0.5 * incoming).astype(bf16)
    grad_down_t = dot(grad_branch, hidden, 0, 0)
    grad_pre = (dot(grad_branch, down_t, 1, 0) * swish_grad(pre_act)).astype(bf16)
    grad_up = dot(normed, grad_pre, 0, 0)
    grad_resid, gain_grad = norm_back(dot(grad_pre, up, 1, 1), gain_row, saved)
    return incoming + grad_resid, gain_grad, grad_up, grad_down_t


def angle_tables(frames, width):
    step = 32
    frequency = jnp.exp(jnp.arange(width // 2, dtype=f32) * (-2.0 * math.log(10000.0) / width))
    coarse = (jnp.arange(frames // step, dtype=f32) * step)[:, None] * frequency
    fine = jnp.arange(step, dtype=f32)[:, None] * frequency
    cs, cc = jnp.sin(coarse)[:, None], jnp.cos(coarse)[:, None]
    fs, fc = jnp.sin(fine)[None], jnp.cos(fine)[None]
    sines = (cs * fc + cc * fs).reshape(frames, width // 2)
    cosines = (cc * fc - cs * fs).reshape(frames, width // 2)
    return sines, cosines


def shifted(whole, taps, rows, reverse):
    total = None
    for tap in range(KERNEL):
        first = EDGE - HALF + (KERNEL - 1 - tap if reverse else tap)
        term = taps[tap] * whole[first:first + rows]
        total = term if total is None else total + term
    return total


def with_edges(block, edges, t, n_t):
    before = jnp.where(t > 0, edges[0], 0.0)
    after = jnp.where(t < n_t - 1, edges[1], 0.0)
    return jnp.concatenate([before, block, after], axis=0)


def per_device(n_dp, n_t, inputs, out_grad, norm_gains, first_up, first_down, attend_in, attend_out, position_bias,
               convolve_in, depth_kernel, batch_norm, convolve_out, second_up, second_down):
    d = lax.axis_index("dp")
    t = lax.axis_index("tensor")
    rows, D = inputs.shape
    w = attend_in.shape[2]
    R = attend_in.shape[1]
    F = first_up.shape[1]
    head_dim = position_bias.shape[2] * n_dp
    heads = D // head_dim
    local_heads = position_bias.shape[1]
    frames = rows * n_t
    n_gain = norm_gains.shape[1]
    n_bias = position_bias.shape[2]

    packed = jnp.stack([
        first_up, first_down.T, attend_in.transpose(1, 0, 2).reshape(R, 4 * w),
        jnp.concatenate([convolve_in.reshape(R, 2 * w), attend_out.T, convolve_out.T], axis=1),
        second_up, second_down.T])
    small = jnp.zeros((16, 128), f32)
    small = small.at[:n_gain, :5].set(norm_gains.T)
    small = small.at[:n_bias, 8:8 + 2 * local_heads].set(position_bias.astype(f32).reshape(2 * local_heads, n_bias).T)
    taps = jnp.concatenate([depth_kernel.T, batch_norm, jnp.zeros((7, w), f32)], axis=0)
    weights, small_all, taps_all = gather_weights(n_dp, n_t, packed, small, taps)
    small_all = small_all.reshape(n_t, n_dp, 16, 128)
    gains = small_all[:, :, :n_gain, :5].transpose(3, 1, 0, 2).reshape(5, D)
    bias = small_all[:, :, :n_bias, 8:8 + 2 * local_heads].reshape(n_t, n_dp, n_bias, 2, local_heads)
    bias = bias.transpose(3, 0, 4, 1, 2).reshape(2, D)
    taps_all = taps_all.transpose(1, 0, 2).reshape(40, D)
    tap_rows = taps_all[:KERNEL]
    bn_gain, bn_shift = taps_all[KERNEL], taps_all[KERNEL + 1]
    attend_w = weights[2].reshape(D, n_t, 4, w).transpose(2, 0, 1, 3).reshape(4, D, D)
    mixed_w = weights[3].reshape(D, n_t, 4, w).transpose(2, 0, 1, 3).reshape(4, D, D)

    x0 = inputs.astype(f32)
    x1, stored_one = feed_forward(x0, gains[0], weights[0], weights[1])

    saved_two = norm_rows(x1)
    a2 = (saved_two[0] * gains[1]).astype(bf16)
    a2_all = spread_frames(n_t, a2).reshape(frames, D)
    q = dot(a2, attend_w[0], 1, 0)
    content_q = (q + bias[0]).astype(bf16).reshape(rows, heads, head_dim)
    position_q = (q + bias[1]).astype(bf16).reshape(rows, heads, head_dim)
    keys = dot(a2_all, attend_w[1], 1, 0).astype(bf16).reshape(frames, heads, head_dim)
    values = dot(a2_all, attend_w[2], 1, 0).astype(bf16).reshape(frames, heads, head_dim)
    sines, cosines = angle_tables(frames, D)
    phases = jnp.concatenate([sines, cosines], axis=1).astype(bf16)
    own_sin = lax.dynamic_slice_in_dim(sines, t * rows, rows, 0)
    own_cos = lax.dynamic_slice_in_dim(cosines, t * rows, rows, 0)
    pos_w = attend_w[3].reshape(D, heads, head_dim)
    scale = head_dim ** -0.5
    turned = jnp.einsum("rhe,che->hrc", position_q, pos_w, preferred_element_type=f32)
    rs, rc = turned[..., :D // 2], turned[..., D // 2:]
    turned = jnp.concatenate([rc * own_sin - rs * own_cos, rs * own_sin + rc * own_cos], axis=-1).astype(bf16)
    scores = (jnp.einsum("rhe,fhe->hrf", content_q, keys, preferred_element_type=f32)
              + jnp.einsum("hrc,fc->hrf", turned, phases, preferred_element_type=f32)) * scale
    exponent = jnp.exp(scores - jnp.max(scores, axis=-1, keepdims=True))
    softmax_w = (exponent / jnp.sum(exponent, axis=-1, keepdims=True)).astype(bf16)
    mixture = jnp.einsum("hrf,fhe->rhe", softmax_w, values, preferred_element_type=f32).astype(bf16).reshape(rows, D)
    x2 = x1 + dot(mixture, mixed_w[2], 1, 1)

    saved_three = norm_rows(x2)
    a3 = (saved_three[0] * gains[2]).astype(bf16)
    value_half = dot(a3, mixed_w[0], 1, 0)
    sigmoid_gate = jax.nn.sigmoid(dot(a3, mixed_w[1], 1, 0))
    gated = value_half * sigmoid_gate
    edges = swap_edges(n_t, gated[None])
    gated_all = with_edges(gated, edges[:, 0], t, n_t)
    convolved = shifted(gated_all, tap_rows, rows, False)
    row_count = frames * n_dp
    sums = jnp.concatenate([jnp.stack([jnp.sum(convolved, axis=0), jnp.sum(convolved * convolved, axis=0)]),
                            jnp.zeros((6, D), f32)])
    sums, = whole_totals(n_dp, n_t, sums, 5)
    batch_mean = sums[0] / row_count
    inverse = lax.rsqrt(sums[1] / row_count - batch_mean * batch_mean + norm_eps)
    scaled = (convolved - batch_mean) * inverse
    normal_out = scaled * bn_gain + bn_shift
    activated = (normal_out * jax.nn.sigmoid(normal_out)).astype(bf16)
    x3 = x2 + dot(activated, mixed_w[3], 1, 1)

    x4, stored_four = feed_forward(x3, gains[3], weights[4], weights[5])
    saved_five = norm_rows(x4)
    output_rows = saved_five[0] * gains[4]

    dx4, gain_four = norm_back(out_grad.astype(f32), gains[4], saved_five)
    dx3, gain_three, grad_second_up, grad_second_down = feed_backward(dx4, gains[3], weights[4], weights[5],
                                                                      stored_four)
    dz3 = dx3.astype(bf16)
    grad_convolve_out = dot(dz3, activated, 0, 0)
    dbn = dot(dz3, mixed_w[3], 1, 0) * swish_grad(normal_out)
    sums = jnp.concatenate([jnp.stack([jnp.sum(dbn * scaled, axis=0), jnp.sum(dbn, axis=0)]), jnp.zeros((6, D), f32)])
    sums, edges = whole_totals(n_dp, n_t, sums, 6, jnp.stack([dbn, scaled]))
    grad_bn = sums[:2]
    norm_scale = bn_gain * inverse

    def conv_grad(dbn_rows, scaled_rows):
        return norm_scale * (dbn_rows - grad_bn[1] / row_count - scaled_rows * (grad_bn[0] / row_count))
    dcv = conv_grad(dbn, scaled)
    dcv_all = with_edges(dcv, conv_grad(edges[:, 0], edges[:, 1]), t, n_t)
    first = EDGE - HALF
    grad_taps = jnp.stack([jnp.sum(dcv * gated_all[first + tap:first + tap + rows], axis=0) for tap in range(KERNEL)])
    dglu = shifted(dcv_all, tap_rows, rows, True)
    de_value = (dglu * sigmoid_gate).astype(bf16)
    de_gate = (dglu * value_half * sigmoid_gate * (1.0 - sigmoid_gate)).astype(bf16)
    grad_value = dot(a3, de_value, 0, 0)
    grad_gate = dot(a3, de_gate, 0, 0)
    grad_normed = dot(de_value, mixed_w[0], 1, 1) + dot(de_gate, mixed_w[1], 1, 1)
    grad_resid, gain_two = norm_back(grad_normed, gains[2], saved_three)
    dx2 = dx3 + grad_resid

    dz2 = dx2.astype(bf16)
    grad_attend_out = dot(dz2, mixture, 0, 0)
    dmix = dot(dz2, mixed_w[2], 1, 0).astype(bf16).reshape(rows, heads, head_dim)
    dpl = jnp.einsum("rhe,fhe->hrf", dmix, values, preferred_element_type=f32)
    p = softmax_w.astype(f32)
    ds = (p * (dpl - jnp.sum(dpl * p, axis=-1, keepdims=True))).astype(bf16)
    dvalues = jnp.einsum("hrf,rhe->fhe", softmax_w, dmix, preferred_element_type=f32).astype(bf16).reshape(frames, D)
    dkeys = (jnp.einsum("hrf,rhe->fhe", ds, content_q, preferred_element_type=f32) * scale).astype(bf16)
    dkeys = dkeys.reshape(frames, D)
    dcq = jnp.einsum("hrf,fhe->rhe", ds, keys, preferred_element_type=f32).reshape(rows, D) * scale
    turned = jnp.einsum("hrf,fc->hrc", ds, phases, preferred_element_type=f32)
    ts, tc = turned[..., :D // 2], turned[..., D // 2:]
    turned = jnp.concatenate([tc * own_sin - ts * own_cos, ts * own_sin + tc * own_cos], axis=-1).astype(bf16)
    dpq = jnp.einsum("hrc,che->rhe", turned, pos_w, preferred_element_type=f32).reshape(rows, D) * scale
    grad_pos = (jnp.einsum("hrc,rhe->che", turned, position_q, preferred_element_type=f32) * scale).reshape(D, D)
    dq = (dcq + dpq).astype(bf16)
    grad_attend = jnp.stack([dot(a2, dq, 0, 0), dot(a2_all, dkeys, 0, 0), dot(a2_all, dvalues, 0, 0), grad_pos])
    part = dot(dkeys, attend_w[1], 1, 1) + dot(dvalues, attend_w[2], 1, 1)
    part = reduce_frames(n_t, part.astype(bf16).reshape(n_t, rows, D))
    grad_resid, gain_one = norm_back(part + dot(dq, attend_w[0], 1, 1), gains[1], saved_two)
    dx1 = dx2 + grad_resid
    dx0, gain_zero, grad_first_up, grad_first_down = feed_backward(dx1, gains[0], weights[0], weights[1], stored_one)

    def by_tensor(stacked):
        return stacked.reshape(4, D, n_t, w).transpose(1, 2, 0, 3).reshape(D, 4 * D)
    grads = jnp.stack([
        grad_first_up, grad_first_down, by_tensor(grad_attend),
        by_tensor(jnp.stack([grad_value, grad_gate, grad_attend_out, grad_convolve_out])),
        grad_second_up, grad_second_down]).astype(bf16)
    gain_rows = jnp.stack([gain_zero, gain_one, gain_two, gain_three, gain_four])
    gain_rows = gain_rows.reshape(5, n_dp, n_t, n_gain).transpose(2, 0, 1, 3).reshape(n_t, 5, w)
    wide_rows = jnp.concatenate([grad_taps, jnp.sum(dcq, axis=0)[None], jnp.sum(dpq, axis=0)[None],
                                 jnp.zeros((2, D), f32)])
    wide_rows = wide_rows.reshape(35, n_t, w).transpose(1, 0, 2)
    small = jnp.concatenate([wide_rows, gain_rows], axis=1)
    shards, small = fold_weights(n_dp, n_t, grads, small)
    grad_gains = lax.dynamic_slice_in_dim(small[35:], d * n_gain, n_gain, 1)
    grad_bias = small[KERNEL:KERNEL + 2].reshape(2, local_heads, head_dim)
    grad_bias = lax.dynamic_slice_in_dim(grad_bias, d * n_bias, n_bias, 2)
    return (
        output_rows, dx0, grad_gains,
        shards[0], shards[1].T, shards[2].reshape(R, 4, w).transpose(1, 0, 2), shards[3][:, 2 * w:3 * w].T, grad_bias,
        shards[3][:, :2 * w].reshape(R, 2, w), small[:KERNEL].T, lax.dynamic_slice_in_dim(grad_bn, t * w, w, 1),
        shards[3][:, 3 * w:].T, shards[4], shards[5].T)


def solution(mesh):
    n_dp, n_t = mesh.shape["dp"], mesh.shape["tensor"]
    row = P(("dp", "tensor"), None)
    gain = P(None, ("dp", "tensor"))
    up = P("dp", "tensor")
    down = P("tensor", "dp")
    weights = (up, down, P(None, "dp", "tensor"), down, P(None, "tensor", "dp"), P("dp", None, "tensor"),
               P("tensor", None), P(None, "tensor"), down, up, down)
    return jax.shard_map(
        functools.partial(per_device, n_dp, n_t), mesh=mesh,
        in_specs=(row, row, gain) + weights,
        out_specs=(row, row, gain) + weights,
        check_vma=False)
```

```python
import functools
import math

import jax
import jax.numpy as jnp
import numpy as np
from jax import lax
from jax.experimental import pallas as pl
from jax.experimental.pallas import tpu as pltpu
from jax.sharding import PartitionSpec as P

MESH = pl.DeviceIdType.MESH
CHUNKS = 6
CORE = 1


def flip(index, mask):
    result = index
    bit = 1
    while bit <= mask:
        if mask & bit:
            result = result + bit - 2 * bit * ((index // bit) % 2)
        bit *= 2
    return result


def span(bits):
    masks = [0]
    for bit in bits:
        masks = masks + [mask ^ bit for mask in masks]
    return masks


def link_orders(n_dp):
    bits = [1 << k for k in range(1, n_dp.bit_length() - 1)]
    return (bits, bits[::-1])


def greet(peers):
    barrier = pltpu.get_barrier_semaphore()
    for peer in peers:
        pl.semaphore_signal(barrier, inc=1, device_id=peer, device_id_type=MESH)
    pl.semaphore_wait(barrier, len(peers))


def tensor_peers(d, t, n_t):
    return [(d, lax.rem(t + step, n_t)) for step in range(1, n_t)]


def remote(src, dst, send_sem, recv_sem, peer):
    return pltpu.make_async_remote_copy(
        src_ref=src, dst_ref=dst, send_sem=send_sem, recv_sem=recv_sem,
        device_id=peer, device_id_type=MESH)


def gather_body(n_dp, n_t, p_ref, e_ref, f_ref, g_ref, ge_ref, gf_ref, local_sem, z_send, z_recv, d_send, d_recv,
                fz_send, fz_recv):
    d = lax.axis_index("dp")
    t = lax.axis_index("tensor")
    rows, width = p_ref.shape[1], p_ref.shape[2]
    e_rows = e_ref.shape[0]
    half = n_t * width // 2
    orders = [order + [CORE] for order in link_orders(n_dp)]
    stages = len(orders[0])
    z_peers = tensor_peers(d, t, n_t)
    greet(z_peers + [(flip(d, bit), t) for bit in orders[0]])

    def block(c, mask, start, size):
        if c == CHUNKS:
            return ge_ref.at[:, pl.ds(pl.multiple_of(flip(d, mask) * e_rows, e_rows), e_rows), :]
        first = pl.multiple_of(flip(d, mask) * rows, rows)
        return g_ref.at[c, pl.ds(first, rows), pl.ds(start, size)]

    def own(c):
        if c == CHUNKS:
            return ge_ref.at[t, pl.ds(pl.multiple_of(d * e_rows, e_rows), e_rows), :]
        return block(c, 0, pl.multiple_of(t * width, width), width)

    def source(c):
        return e_ref if c == CHUNKS else p_ref.at[c]

    def z_copy(c, step):
        return remote(source(c), own(c), z_send.at[c, step], z_recv.at[c, step], z_peers[step])

    def f_copy(step):
        return remote(f_ref, gf_ref.at[t], fz_send.at[step], fz_recv.at[step], z_peers[step])

    def local_copy(c):
        return pltpu.make_async_copy(source(c), own(c), local_sem.at[c])

    def dp_copies(c, stage):
        copies = []
        for h in range(1 if c == CHUNKS else 2):
            bit = orders[h][stage]
            masks = span(orders[h][:stage])
            for j, mask in enumerate(masks):
                slot = len(masks) - 1 + j
                window = block(c, mask, h * half, half)
                copies.append(remote(window, window, d_send.at[c, h, slot], d_recv.at[c, h, slot], (flip(d, bit), t)))
        return copies

    everything = [CHUNKS] + list(range(CHUNKS))
    own_f = pltpu.make_async_copy(f_ref, gf_ref.at[t], local_sem.at[CHUNKS + 1])
    own_f.start()
    for c in everything:
        local_copy(c).start()
        for step in range(n_t - 1):
            z_copy(c, step).start()
        if c == CHUNKS:
            for step in range(n_t - 1):
                f_copy(step).start()
    for tick in range(len(everything) + stages):
        for stage in range(stages + 1):
            place = tick - stage
            if 0 <= place < len(everything):
                c = everything[place]
                if stage == 0:
                    local_copy(c).wait()
                    for step in range(n_t - 1):
                        z_copy(c, step).wait_recv()
                else:
                    for copy in dp_copies(c, stage - 1):
                        copy.wait_recv()
                if stage < stages:
                    for copy in dp_copies(c, stage):
                        copy.start()
    for step in range(n_t - 1):
        f_copy(step).wait()
    own_f.wait()
    for c in everything:
        for step in range(n_t - 1):
            z_copy(c, step).wait_send()
        for stage in range(stages):
            for copy in dp_copies(c, stage):
                copy.wait_send()


def gather_weights(n_dp, n_t, packed, small, taps):
    _, rows, width = packed.shape
    e_rows = small.shape[0]
    dma = pltpu.SemaphoreType.DMA
    vmem = pl.BlockSpec(memory_space=pltpu.VMEM)
    hbm = pl.BlockSpec(memory_space=pl.ANY)
    return pl.pallas_call(
        functools.partial(gather_body, n_dp, n_t),
        name="gather_weights",
        out_shape=(
            jax.ShapeDtypeStruct((CHUNKS, n_dp * rows, n_t * width), packed.dtype),
            jax.ShapeDtypeStruct((n_t, n_dp * e_rows, 128), jnp.float32),
            jax.ShapeDtypeStruct((n_t,) + taps.shape, jnp.float32)),
        in_specs=[vmem, vmem, vmem],
        out_specs=(hbm, hbm, hbm),
        scratch_shapes=[
            dma((CHUNKS + 2,)), dma((CHUNKS + 1, n_t - 1)), dma((CHUNKS + 1, n_t - 1)),
            dma((CHUNKS + 1, 2, n_dp - 1)), dma((CHUNKS + 1, 2, n_dp - 1)),
            dma((n_t - 1,)), dma((n_t - 1,))],
        compiler_params=pltpu.CompilerParams(collective_id=0, has_side_effects=True, vmem_limit_bytes=16 << 20),
    )(packed, small, taps)


def fold_body(n_dp, n_t, x_ref, s_ref, o_ref, so_ref, acc, core_buf, dp_buf, z_buf, small_acc, small_buf, small_z,
              local_sem, core_send, core_recv, d_send, d_recv, z_send, z_recv, s_send, s_recv, sz_send, sz_recv):
    d = lax.axis_index("dp")
    t = lax.axis_index("tensor")
    rows, width = o_ref.shape[1], o_ref.shape[2]
    half = n_t * width // 2
    orders = [order[::-1] for order in link_orders(n_dp)]
    stages = len(orders[0])
    z_peers = tensor_peers(d, t, n_t)
    all_bits = [CORE] + orders[0]
    greet(z_peers + [(flip(d, bit), t) for bit in all_bits])
    groups = span(link_orders(n_dp)[0])

    def x_block(c, mask):
        return x_ref.at[c, pl.ds(pl.multiple_of(flip(d, mask) * rows, rows), rows), :]

    def local_copy(c, k):
        return pltpu.make_async_copy(x_block(c, groups[k]), acc.at[c, k], local_sem.at[c, k])

    def core_copy(c, k):
        return remote(x_block(c, groups[k] ^ CORE), core_buf.at[c, k], core_send.at[c, k], core_recv.at[c, k],
                      (flip(d, CORE), t))

    def dp_moves(c, stage):
        moves = []
        for h in range(2):
            bit = orders[h][stage]
            masks = span(orders[h][stage + 1:])
            base = len(groups) - 2 * len(masks)
            for j, mask in enumerate(masks):
                slot = base + j
                cols = pl.ds(h * half, half)
                copy = remote(acc.at[c, groups.index(mask ^ bit), :, cols], dp_buf.at[c, h, slot],
                              d_send.at[c, h, slot], d_recv.at[c, h, slot], (flip(d, bit), t))
                moves.append((copy, groups.index(mask), cols, h, slot))
        return moves

    def z_copy(c, step):
        target = lax.rem(t + step + 1, n_t)
        return remote(acc.at[c, 0, :, pl.ds(pl.multiple_of(target * width, width), width)], z_buf.at[c, step],
                      z_send.at[c, step], z_recv.at[c, step], z_peers[step])

    def small_copy(k):
        return remote(small_acc.at[k], small_buf.at[k], s_send.at[k], s_recv.at[k], (flip(d, all_bits[k]), t))

    def small_z_copy(step):
        target = lax.rem(t + step + 1, n_t)
        return remote(small_acc.at[len(all_bits), target], small_z.at[step], sz_send.at[step], sz_recv.at[step],
                      z_peers[step])

    for c in range(CHUNKS):
        for k in range(len(groups)):
            core_copy(c, k).start()
            local_copy(c, k).start()
    small_acc[0] = s_ref[...]
    small_copy(0).start()
    for k in range(1, len(all_bits) + 1):
        small_copy(k - 1).wait_recv()
        small_acc[k] = small_acc[k - 1] + small_buf[k - 1]
        if k < len(all_bits):
            small_copy(k).start()
    for step in range(n_t - 1):
        small_z_copy(step).start()

    def start_stage(c, stage):
        if stage < stages:
            for move in dp_moves(c, stage):
                move[0].start()
        else:
            for step in range(n_t - 1):
                z_copy(c, step).start()

    for tick in range(CHUNKS + stages + 1):
        for stage in range(stages + 2):
            c = tick - stage
            if not 0 <= c < CHUNKS:
                continue
            if stage == 0:
                for k in range(len(groups)):
                    local_copy(c, k).wait()
                    core_copy(c, k).wait_recv()

                def add_core(step, carry, c=c):
                    k = step // 4
                    part = pl.ds(pl.multiple_of(lax.rem(step, 4) * (rows // 4), rows // 4), rows // 4)
                    acc[c, k, part, :] = (acc[c, k, part, :].astype(jnp.float32)
                                          + core_buf[c, k, part, :].astype(jnp.float32)).astype(jnp.bfloat16)
                    return carry
                lax.fori_loop(0, 4 * len(groups), add_core, 0)
                start_stage(c, 0)
            elif stage <= stages:
                for copy, k, cols, h, slot in dp_moves(c, stage - 1):
                    copy.wait_recv()

                    def add_dp(step, carry, c=c, k=k, cols=cols, h=h, slot=slot):
                        part = pl.ds(pl.multiple_of(step * (rows // 4), rows // 4), rows // 4)
                        acc[c, k, part, cols] = (acc[c, k, part, cols].astype(jnp.float32)
                                                 + dp_buf[c, h, slot, part, :].astype(jnp.float32)).astype(jnp.bfloat16)
                        return carry
                    lax.fori_loop(0, 4, add_dp, 0)
                start_stage(c, stage)
            else:
                for step in range(n_t - 1):
                    z_copy(c, step).wait_recv()
                total = acc[c, 0, :, pl.ds(pl.multiple_of(t * width, width), width)].astype(jnp.float32)
                for step in range(n_t - 1):
                    total = total + z_buf[c, step].astype(jnp.float32)
                o_ref[c] = total
    total = small_acc[len(all_bits), t]
    for step in range(n_t - 1):
        small_z_copy(step).wait_recv()
        total = total + small_z[step]
    so_ref[...] = total
    for k in range(len(all_bits)):
        small_copy(k).wait_send()
    for step in range(n_t - 1):
        small_z_copy(step).wait_send()
    for c in range(CHUNKS):
        for k in range(len(groups)):
            core_copy(c, k).wait_send()
        for stage in range(stages):
            for move in dp_moves(c, stage):
                move[0].wait_send()
        for step in range(n_t - 1):
            z_copy(c, step).wait_send()


def fold_weights(n_dp, n_t, partial, small):
    rows, width = partial.shape[1] // n_dp, partial.shape[2] // n_t
    groups = n_dp // 2
    n_bits = n_dp.bit_length() - 1
    dma = pltpu.SemaphoreType.DMA
    vmem = pl.BlockSpec(memory_space=pltpu.VMEM)
    hbm = pl.BlockSpec(memory_space=pl.ANY)
    bf16 = jnp.bfloat16
    return pl.pallas_call(
        functools.partial(fold_body, n_dp, n_t),
        name="fold_weights",
        out_shape=(jax.ShapeDtypeStruct((CHUNKS, rows, width), jnp.float32),
                   jax.ShapeDtypeStruct(small.shape[1:], jnp.float32)),
        in_specs=[hbm, vmem],
        out_specs=(vmem, vmem),
        scratch_shapes=[
            pltpu.VMEM((CHUNKS, groups, rows, n_t * width), bf16),
            pltpu.VMEM((CHUNKS, groups, rows, n_t * width), bf16),
            pltpu.VMEM((CHUNKS, 2, groups - 1, rows, n_t * width // 2), bf16),
            pltpu.VMEM((CHUNKS, n_t - 1, rows, width), bf16),
            pltpu.VMEM((n_bits + 1,) + small.shape, jnp.float32),
            pltpu.VMEM((n_bits,) + small.shape, jnp.float32),
            pltpu.VMEM((n_t - 1,) + small.shape[1:], jnp.float32),
            dma((CHUNKS, groups)), dma((CHUNKS, groups)), dma((CHUNKS, groups)),
            dma((CHUNKS, 2, groups - 1)), dma((CHUNKS, 2, groups - 1)),
            dma((CHUNKS, n_t - 1)), dma((CHUNKS, n_t - 1)),
            dma((n_bits,)), dma((n_bits,)), dma((n_t - 1,)), dma((n_t - 1,))],
        compiler_params=pltpu.CompilerParams(collective_id=1, has_side_effects=True, vmem_limit_bytes=48 << 20),
    )(partial, small)


def spread_body(n_t, x_ref, y_ref, local_sem, send, recv):
    d = lax.axis_index("dp")
    t = lax.axis_index("tensor")
    peers = tensor_peers(d, t, n_t)
    greet(peers)
    local = pltpu.make_async_copy(x_ref, y_ref.at[t], local_sem.at[0])
    local.start()
    copies = [remote(x_ref, y_ref.at[t], send.at[k], recv.at[k], peers[k]) for k in range(n_t - 1)]
    for copy in copies:
        copy.start()
    local.wait()
    for copy in copies:
        copy.wait()


def spread_frames(n_t, rows_block):
    dma = pltpu.SemaphoreType.DMA
    vmem = pl.BlockSpec(memory_space=pltpu.VMEM)
    hbm = pl.BlockSpec(memory_space=pl.ANY)
    return pl.pallas_call(
        functools.partial(spread_body, n_t),
        name="spread_frames",
        out_shape=jax.ShapeDtypeStruct((n_t,) + rows_block.shape, rows_block.dtype),
        in_specs=[vmem],
        out_specs=hbm,
        scratch_shapes=[dma((1,)), dma((n_t - 1,)), dma((n_t - 1,))],
        compiler_params=pltpu.CompilerParams(collective_id=2, has_side_effects=True),
    )(rows_block)


def reduce_frames_body(n_t, x_ref, o_ref, buf, send, recv):
    d = lax.axis_index("dp")
    t = lax.axis_index("tensor")
    peers = tensor_peers(d, t, n_t)
    greet(peers)
    copies = [remote(x_ref.at[lax.rem(t + k + 1, n_t)], buf.at[k], send.at[k], recv.at[k], peers[k])
              for k in range(n_t - 1)]
    for copy in copies:
        copy.start()
    for copy in copies:
        copy.wait_recv()
    rows = o_ref.shape[0]
    size = rows // 8

    def add_part(step, carry):
        part = pl.ds(pl.multiple_of(step * size, size), size)
        total = x_ref[t, part, :].astype(jnp.float32)
        for k in range(n_t - 1):
            total = total + buf[k, part, :].astype(jnp.float32)
        o_ref[part, :] = total
        return carry
    lax.fori_loop(0, 8, add_part, 0)
    for copy in copies:
        copy.wait_send()


def reduce_frames(n_t, partial):
    dma = pltpu.SemaphoreType.DMA
    vmem = pl.BlockSpec(memory_space=pltpu.VMEM)
    return pl.pallas_call(
        functools.partial(reduce_frames_body, n_t),
        name="reduce_frames",
        out_shape=jax.ShapeDtypeStruct(partial.shape[1:], jnp.float32),
        in_specs=[vmem],
        out_specs=vmem,
        scratch_shapes=[pltpu.VMEM((n_t - 1,) + partial.shape[1:], partial.dtype), dma((n_t - 1,)), dma((n_t - 1,))],
        compiler_params=pltpu.CompilerParams(collective_id=3, has_side_effects=True),
    )(partial)


EDGE = 16


def edge_pieces(n_t, source, edges, send, recv):
    d = lax.axis_index("dp")
    t = lax.axis_index("tensor")
    before = (d, lax.rem(t + n_t - 1, n_t))
    after = (d, lax.rem(t + 1, n_t))
    rows = source.shape[1]
    return [remote(source.at[:, pl.ds(0, EDGE), :], edges.at[1], send.at[0], recv.at[0], before),
            remote(source.at[:, pl.ds(rows - EDGE, EDGE), :], edges.at[0], send.at[1], recv.at[1], after)]


def edges_body(n_t, x_ref, e_ref, send, recv):
    d = lax.axis_index("dp")
    t = lax.axis_index("tensor")
    greet([(d, lax.rem(t + n_t - 1, n_t)), (d, lax.rem(t + 1, n_t))])
    copies = edge_pieces(n_t, x_ref, e_ref, send, recv)
    for copy in copies:
        copy.start()
    for copy in copies:
        copy.wait()


def swap_edges(n_t, x):
    dma = pltpu.SemaphoreType.DMA
    vmem = pl.BlockSpec(memory_space=pltpu.VMEM)
    return pl.pallas_call(
        functools.partial(edges_body, n_t),
        name="swap_edges",
        out_shape=jax.ShapeDtypeStruct((2, x.shape[0], EDGE, x.shape[2]), x.dtype),
        in_specs=[vmem],
        out_specs=vmem,
        scratch_shapes=[dma((2,)), dma((2,))],
        compiler_params=pltpu.CompilerParams(collective_id=4, has_side_effects=True),
    )(x)


def totals_body(n_dp, n_t, with_edges, *refs):
    if with_edges:
        s_ref, x_ref, o_ref, e_ref, mine, dp_buf, mid, z_buf, d_send, d_recv, z_send, z_recv, e_send, e_recv = refs
    else:
        s_ref, o_ref, mine, dp_buf, mid, z_buf, d_send, d_recv, z_send, z_recv = refs
    d = lax.axis_index("dp")
    t = lax.axis_index("tensor")
    z_peers = tensor_peers(d, t, n_t)
    d_peers = [(flip(d, mask), t) for mask in range(1, n_dp)]
    greet(z_peers + d_peers)
    if with_edges:
        edge_copies = edge_pieces(n_t, x_ref, e_ref, e_send, e_recv)
    d_copies = [remote(s_ref, dp_buf.at[k], d_send.at[k], d_recv.at[k], d_peers[k]) for k in range(n_dp - 1)]
    for copy in d_copies:
        copy.start()
    if with_edges:
        for copy in edge_copies:
            copy.start()
    total = s_ref[...]
    for k in range(n_dp - 1):
        d_copies[k].wait_recv()
        total = total + dp_buf[k]
    mid[...] = total
    z_copies = [remote(mid, z_buf.at[k], z_send.at[k], z_recv.at[k], z_peers[k]) for k in range(n_t - 1)]
    for copy in z_copies:
        copy.start()
    for k in range(n_t - 1):
        z_copies[k].wait_recv()
        total = total + z_buf[k]
    o_ref[...] = total
    for copy in d_copies + z_copies:
        copy.wait_send()
    if with_edges:
        for copy in edge_copies:
            copy.wait()


def whole_totals(n_dp, n_t, sums, collective_id, edge_rows=None):
    dma = pltpu.SemaphoreType.DMA
    vmem = pl.BlockSpec(memory_space=pltpu.VMEM)
    shape = jax.ShapeDtypeStruct(sums.shape, jnp.float32)
    scratch = [pltpu.VMEM(sums.shape, jnp.float32), pltpu.VMEM((n_dp - 1,) + sums.shape, jnp.float32),
               pltpu.VMEM(sums.shape, jnp.float32), pltpu.VMEM((n_t - 1,) + sums.shape, jnp.float32),
               dma((n_dp - 1,)), dma((n_dp - 1,)), dma((n_t - 1,)), dma((n_t - 1,))]
    args = [sums]
    outs = [shape]
    if edge_rows is not None:
        args.append(edge_rows)
        outs.append(jax.ShapeDtypeStruct((2, edge_rows.shape[0], EDGE, edge_rows.shape[2]), jnp.float32))
        scratch += [dma((2,)), dma((2,))]
    return pl.pallas_call(
        functools.partial(totals_body, n_dp, n_t, edge_rows is not None),
        name="whole_totals",
        out_shape=tuple(outs),
        in_specs=[vmem] * len(args),
        out_specs=tuple([vmem] * len(outs)),
        scratch_shapes=scratch,
        compiler_params=pltpu.CompilerParams(collective_id=collective_id, has_side_effects=True),
    )(*args)


KERNEL = 31
HALF = KERNEL // 2
norm_eps = 1e-05
f32 = jnp.float32
bf16 = jnp.bfloat16


def norm_rows(values):
    centred = values - jnp.mean(values, axis=-1, keepdims=True)
    inverse = lax.rsqrt(jnp.mean(centred * centred, axis=-1, keepdims=True) + norm_eps)
    return centred * inverse, inverse


def norm_back(incoming, gain_row, saved):
    scaled, inverse = saved
    grad_scaled = incoming * gain_row
    inner = jnp.mean(grad_scaled * scaled, axis=-1, keepdims=True)
    grad_in = inverse * (grad_scaled - jnp.mean(grad_scaled, axis=-1, keepdims=True) - scaled * inner)
    return grad_in, jnp.sum(incoming * scaled, axis=0)


def swish_grad(pre_act):
    sigmoid_val = jax.nn.sigmoid(pre_act)
    return sigmoid_val * (1.0 + pre_act * (1.0 - sigmoid_val))


def dot(left, right, left_dim, right_dim):
    return lax.dot_general(left, right, (((left_dim,), (right_dim,)), ((), ())), preferred_element_type=f32)


def feed_forward(residual, gain_row, up, down_t):
    saved = norm_rows(residual)
    normed = (saved[0] * gain_row).astype(bf16)
    pre_act = dot(normed, up, 1, 0)
    hidden = (pre_act * jax.nn.sigmoid(pre_act)).astype(bf16)
    return residual + 0.5 * dot(hidden, down_t, 1, 1), (saved, normed, pre_act, hidden)


def feed_backward(incoming, gain_row, up, down_t, stored):
    saved, normed, pre_act, hidden = stored
    grad_branch = (0.5 * incoming).astype(bf16)
    grad_down_t = dot(grad_branch, hidden, 0, 0)
    grad_pre = (dot(grad_branch, down_t, 1, 0) * swish_grad(pre_act)).astype(bf16)
    grad_up = dot(normed, grad_pre, 0, 0)
    grad_resid, gain_grad = norm_back(dot(grad_pre, up, 1, 1), gain_row, saved)
    return incoming + grad_resid, gain_grad, grad_up, grad_down_t


def angle_tables(frames, width):
    step = 32
    frequency = np.exp(np.arange(width // 2) * (-2.0 * math.log(10000.0) / width))
    coarse = np.arange(frames // step)[:, None] * step * frequency
    fine = np.arange(step)[:, None] * frequency
    return jnp.asarray(np.stack([np.sin(coarse), np.cos(coarse), np.sin(fine), np.cos(fine)]), f32)


def shifted(whole, taps, rows, reverse):
    total = None
    for tap in range(KERNEL):
        first = EDGE - HALF + (KERNEL - 1 - tap if reverse else tap)
        term = taps[tap] * whole[first:first + rows]
        total = term if total is None else total + term
    return total


def with_edges(block, edges, t, n_t):
    before = jnp.where(t > 0, edges[0], 0.0)
    after = jnp.where(t < n_t - 1, edges[1], 0.0)
    return jnp.concatenate([before, block, after], axis=0)


def per_device(n_dp, n_t, inputs, out_grad, norm_gains, first_up, first_down, attend_in, attend_out, position_bias,
               convolve_in, depth_kernel, batch_norm, convolve_out, second_up, second_down):
    d = lax.axis_index("dp")
    t = lax.axis_index("tensor")
    rows, D = inputs.shape
    w = attend_in.shape[2]
    R = attend_in.shape[1]
    F = first_up.shape[1]
    head_dim = position_bias.shape[2] * n_dp
    heads = D // head_dim
    local_heads = position_bias.shape[1]
    frames = rows * n_t
    n_gain = norm_gains.shape[1]
    n_bias = position_bias.shape[2]

    gain_pack = jnp.concatenate([norm_gains, position_bias.astype(f32).reshape(2, local_heads * n_bias),
                                 jnp.zeros((1, n_gain), f32)])
    taps = jnp.concatenate([depth_kernel.T, batch_norm, jnp.zeros((7, w), f32)], axis=0)
    weights, gains, taps_all, x1, x2, a2_all, kv, content_q, position_q, softmax_w, mixture, phases, turns = forward_kernel(
        n_dp, n_t, head_dim,
        (first_up, first_down, attend_in, convolve_in.reshape(R, 2 * w), attend_out, convolve_out, second_up,
         second_down), gain_pack, taps, inputs, angle_tables(frames, D))
    a2_all = a2_all.reshape(frames, D)
    a2 = lax.dynamic_slice_in_dim(a2_all, t * rows, rows, 0)
    taps_all = taps_all.transpose(1, 0, 2).reshape(40, D)
    tap_rows = taps_all[:KERNEL]
    bn_gain, bn_shift = taps_all[KERNEL], taps_all[KERNEL + 1]
    attend_w = weights[2].reshape(D, n_t, 4, w).transpose(2, 0, 1, 3).reshape(4, D, D)
    mixed_w = weights[3].reshape(D, n_t, 4, w).transpose(2, 0, 1, 3).reshape(4, D, D)
    x0 = inputs.astype(f32)
    _, stored_one = feed_forward(x0, gains[0], weights[0], weights[1])
    saved_two = norm_rows(x1)
    pos_w = attend_w[3].reshape(D, heads, head_dim)
    scale = head_dim ** -0.5
    own_sin, own_cos = turns[0], turns[1]
    flat = lambda part: part.transpose(1, 0, 2).reshape(part.shape[1], D)
    keys = flat(kv[:, :, :w]).reshape(frames, heads, head_dim)
    values = flat(kv[:, :, w:]).reshape(frames, heads, head_dim)
    content_q = flat(content_q).reshape(rows, heads, head_dim)
    position_q = flat(position_q).reshape(rows, heads, head_dim)
    mixture = flat(mixture)

    saved_three = norm_rows(x2)
    a3 = (saved_three[0] * gains[2]).astype(bf16)
    value_half = dot(a3, mixed_w[0], 1, 0)
    sigmoid_gate = jax.nn.sigmoid(dot(a3, mixed_w[1], 1, 0))
    gated = value_half * sigmoid_gate
    edges = swap_edges(n_t, gated[None])
    gated_all = with_edges(gated, edges[:, 0], t, n_t)
    convolved = shifted(gated_all, tap_rows, rows, False)
    row_count = frames * n_dp
    sums = jnp.concatenate([jnp.stack([jnp.sum(convolved, axis=0), jnp.sum(convolved * convolved, axis=0)]),
                            jnp.zeros((6, D), f32)])
    sums, = whole_totals(n_dp, n_t, sums, 5)
    batch_mean = sums[0] / row_count
    inverse = lax.rsqrt(sums[1] / row_count - batch_mean * batch_mean + norm_eps)
    scaled = (convolved - batch_mean) * inverse
    normal_out = scaled * bn_gain + bn_shift
    activated = (normal_out * jax.nn.sigmoid(normal_out)).astype(bf16)
    x3 = x2 + dot(activated, mixed_w[3], 1, 1)

    x4, stored_four = feed_forward(x3, gains[3], weights[4], weights[5])
    saved_five = norm_rows(x4)
    output_rows = saved_five[0] * gains[4]

    dx4, gain_four = norm_back(out_grad.astype(f32), gains[4], saved_five)
    dx3, gain_three, grad_second_up, grad_second_down = feed_backward(dx4, gains[3], weights[4], weights[5],
                                                                      stored_four)
    dz3 = dx3.astype(bf16)
    grad_convolve_out = dot(dz3, activated, 0, 0)
    dbn = dot(dz3, mixed_w[3], 1, 0) * swish_grad(normal_out)
    sums = jnp.concatenate([jnp.stack([jnp.sum(dbn * scaled, axis=0), jnp.sum(dbn, axis=0)]), jnp.zeros((6, D), f32)])
    sums, edges = whole_totals(n_dp, n_t, sums, 6, jnp.stack([dbn, scaled]))
    grad_bn = sums[:2]
    norm_scale = bn_gain * inverse

    def conv_grad(dbn_rows, scaled_rows):
        return norm_scale * (dbn_rows - grad_bn[1] / row_count - scaled_rows * (grad_bn[0] / row_count))
    dcv = conv_grad(dbn, scaled)
    dcv_all = with_edges(dcv, conv_grad(edges[:, 0], edges[:, 1]), t, n_t)
    first = EDGE - HALF
    grad_taps = jnp.stack([jnp.sum(dcv * gated_all[first + tap:first + tap + rows], axis=0) for tap in range(KERNEL)])
    dglu = shifted(dcv_all, tap_rows, rows, True)
    de_value = (dglu * sigmoid_gate).astype(bf16)
    de_gate = (dglu * value_half * sigmoid_gate * (1.0 - sigmoid_gate)).astype(bf16)
    grad_value = dot(a3, de_value, 0, 0)
    grad_gate = dot(a3, de_gate, 0, 0)
    grad_normed = dot(de_value, mixed_w[0], 1, 1) + dot(de_gate, mixed_w[1], 1, 1)
    grad_resid, gain_two = norm_back(grad_normed, gains[2], saved_three)
    dx2 = dx3 + grad_resid

    dz2 = dx2.astype(bf16)
    grad_attend_out = dot(dz2, mixture, 0, 0)
    dmix = dot(dz2, mixed_w[2], 1, 0).astype(bf16).reshape(rows, heads, head_dim)
    dpl = jnp.einsum("rhe,fhe->hrf", dmix, values, preferred_element_type=f32)
    p = softmax_w.astype(f32)
    ds = (p * (dpl - jnp.sum(dpl * p, axis=-1, keepdims=True))).astype(bf16)
    dvalues = jnp.einsum("hrf,rhe->fhe", softmax_w, dmix, preferred_element_type=f32).astype(bf16).reshape(frames, D)
    dkeys = (jnp.einsum("hrf,rhe->fhe", ds, content_q, preferred_element_type=f32) * scale).astype(bf16)
    dkeys = dkeys.reshape(frames, D)
    dcq = jnp.einsum("hrf,fhe->rhe", ds, keys, preferred_element_type=f32).reshape(rows, D) * scale
    turned = jnp.einsum("hrf,fc->hrc", ds, phases, preferred_element_type=f32)
    ts, tc = turned[..., :D // 2], turned[..., D // 2:]
    turned = jnp.concatenate([tc * own_sin - ts * own_cos, ts * own_sin + tc * own_cos], axis=-1).astype(bf16)
    dpq = jnp.einsum("hrc,che->rhe", turned, pos_w, preferred_element_type=f32).reshape(rows, D) * scale
    grad_pos = (jnp.einsum("hrc,rhe->che", turned, position_q, preferred_element_type=f32) * scale).reshape(D, D)
    dq = (dcq + dpq).astype(bf16)
    grad_attend = jnp.stack([dot(a2, dq, 0, 0), dot(a2_all, dkeys, 0, 0), dot(a2_all, dvalues, 0, 0), grad_pos])
    part = dot(dkeys, attend_w[1], 1, 1) + dot(dvalues, attend_w[2], 1, 1)
    part = reduce_frames(n_t, part.astype(bf16).reshape(n_t, rows, D))
    grad_resid, gain_one = norm_back(part + dot(dq, attend_w[0], 1, 1), gains[1], saved_two)
    dx1 = dx2 + grad_resid
    dx0, gain_zero, grad_first_up, grad_first_down = feed_backward(dx1, gains[0], weights[0], weights[1], stored_one)

    def by_tensor(stacked):
        return stacked.reshape(4, D, n_t, w).transpose(1, 2, 0, 3).reshape(D, 4 * D)
    grads = jnp.stack([
        grad_first_up, grad_first_down, by_tensor(grad_attend),
        by_tensor(jnp.stack([grad_value, grad_gate, grad_attend_out, grad_convolve_out])),
        grad_second_up, grad_second_down]).astype(bf16)
    gain_rows = jnp.stack([gain_zero, gain_one, gain_two, gain_three, gain_four])
    gain_rows = gain_rows.reshape(5, n_dp, n_t, n_gain).transpose(2, 0, 1, 3).reshape(n_t, 5, w)
    wide_rows = jnp.concatenate([grad_taps, jnp.sum(dcq, axis=0)[None], jnp.sum(dpq, axis=0)[None],
                                 jnp.zeros((2, D), f32)])
    wide_rows = wide_rows.reshape(35, n_t, w).transpose(1, 0, 2)
    small = jnp.concatenate([wide_rows, gain_rows], axis=1)
    shards, small = fold_weights(n_dp, n_t, grads, small)
    grad_gains = lax.dynamic_slice_in_dim(small[35:], d * n_gain, n_gain, 1)
    grad_bias = small[KERNEL:KERNEL + 2].reshape(2, local_heads, head_dim)
    grad_bias = lax.dynamic_slice_in_dim(grad_bias, d * n_bias, n_bias, 2)
    return (
        output_rows, dx0, grad_gains,
        shards[0], shards[1].T, shards[2].reshape(R, 4, w).transpose(1, 0, 2), shards[3][:, 2 * w:3 * w].T, grad_bias,
        shards[3][:, :2 * w].reshape(R, 2, w), small[:KERNEL].T, lax.dynamic_slice_in_dim(grad_bn, t * w, w, 1),
        shards[3][:, 3 * w:].T, shards[4], shards[5].T)


def solution(mesh):
    n_dp, n_t = mesh.shape["dp"], mesh.shape["tensor"]
    row = P(("dp", "tensor"), None)
    gain = P(None, ("dp", "tensor"))
    up = P("dp", "tensor")
    down = P("tensor", "dp")
    weights = (up, down, P(None, "dp", "tensor"), down, P(None, "tensor", "dp"), P("dp", None, "tensor"),
               P("tensor", None), P(None, "tensor"), down, up, down)
    return jax.shard_map(
        functools.partial(per_device, n_dp, n_t), mesh=mesh,
        in_specs=(row, row, gain) + weights,
        out_specs=(row, row, gain) + weights,
        check_vma=False)


def lane_head(shape, head_dim, head):
    lanes = lax.broadcasted_iota(jnp.int32, shape, 1)
    return (lanes >= head * head_dim) & (lanes < (head + 1) * head_dim)


def row_head(shape, head_dim, head):
    lanes = lax.broadcasted_iota(jnp.int32, shape, 0)
    return (lanes >= head * head_dim) & (lanes < (head + 1) * head_dim)


def keep(mask, value):
    return jnp.where(mask, value, jnp.zeros_like(value))


def row_loop(rows, size, body):
    def step(k, carry):
        body(pl.ds(pl.multiple_of(k * size, size), size))
        return carry
    lax.fori_loop(0, rows // size, step, 0)


def sigmoid(values):
    return 1.0 / (1.0 + jnp.exp(-values))


def norm_parts(values):
    centred = values - jnp.mean(values, axis=-1, keepdims=True)
    inverse = lax.rsqrt(jnp.mean(centred * centred, axis=-1, keepdims=True) + norm_eps)
    return centred * inverse, inverse


def block_of(k, size):
    return pl.ds(pl.multiple_of(k * size, size), size)


def feed_rows(a_ref, up, down_t, z_ref):
    rows = a_ref.shape[0]
    width = 512

    def step(k, carry):
        cols = block_of(k, width)
        pre = dot(a_ref[...], up[:, cols], 1, 0)
        hidden = (pre * sigmoid(pre)).astype(bf16)
        z_ref[...] = z_ref[...] + dot(hidden, down_t[:, cols], 1, 1)
        return carry
    z_ref[...] = jnp.zeros_like(z_ref)
    lax.fori_loop(0, up.shape[1] // width, step, 0)


def forward_body(n_dp, n_t, head_dim, fu, fd, at, cw, ao, co, su, sd, gain_ref, f_ref, x_ref, tab_ref,
                 g_ref, gains_out, gf_ref, x1_ref, x2_ref, a2_ref, kv_ref, cq_ref, pq_ref, p_ref, mix_ref, phase_ref,
                 turn_ref,
                 pack, wbuf, a_s, z_s, s_s, u_s, e_acc, e_buf,
                 local_sem, z_send, z_recv, d_send, d_recv, fz_send, fz_recv, e_send, e_recv, a_send, a_recv):
    d = lax.axis_index("dp")
    t = lax.axis_index("tensor")
    rows_w, width = pack.shape[1], pack.shape[2]
    rows, D = x_ref.shape
    w = D // n_t
    half = n_t * width // 2
    frames = rows * n_t
    local_heads = w // head_dim
    n_gain = gain_ref.shape[1]
    n_bias = n_gain // local_heads
    orders = [order + [CORE] for order in link_orders(n_dp)]
    stages = len(orders[0])
    z_peers = tensor_peers(d, t, n_t)
    greet(z_peers + [(flip(d, bit), t) for bit in orders[0]])

    eye = (lax.broadcasted_iota(jnp.int32, (rows_w, rows_w), 0)
           == lax.broadcasted_iota(jnp.int32, (rows_w, rows_w), 1)).astype(bf16)

    def turn(ref):
        return dot(eye, ref[...], 1, 1).astype(bf16)

    def window(c, mask, start, size):
        first = pl.multiple_of(flip(d, mask) * rows_w, rows_w)
        return wbuf.at[c, pl.ds(first, rows_w), pl.ds(start, size)]

    def own(c):
        return window(c, 0, pl.multiple_of(t * width, width), width)

    def z_copy(c, step):
        return remote(pack.at[c], own(c), z_send.at[c, step], z_recv.at[c, step], z_peers[step])

    def local_copy(c):
        return pltpu.make_async_copy(pack.at[c], own(c), local_sem.at[c])

    def out_copy(c):
        return pltpu.make_async_copy(wbuf.at[c], g_ref.at[c], local_sem.at[CHUNKS + c])

    def f_copy(step):
        return remote(f_ref, gf_ref.at[t], fz_send.at[step], fz_recv.at[step], z_peers[step])

    def a_copy(step):
        return remote(a_s, a2_ref.at[t], a_send.at[step], a_recv.at[step], z_peers[step])

    def dp_copies(c, stage):
        copies = []
        for h in range(2):
            bit = orders[h][stage]
            masks = span(orders[h][:stage])
            for j, mask in enumerate(masks):
                slot = len(masks) - 1 + j
                part = window(c, mask, h * half, half)
                copies.append(remote(part, part, d_send.at[c, h, slot], d_recv.at[c, h, slot], (flip(d, bit), t)))
        return copies

    def send_own(c):
        local_copy(c).start()
        for step in range(n_t - 1):
            z_copy(c, step).start()

    def e_copy(k):
        if k < n_t - 1:
            return remote(e_acc.at[0], e_buf.at[k], e_send.at[k], e_recv.at[k], z_peers[k])
        return remote(e_acc.at[k - n_t + 2], e_buf.at[k], e_send.at[k], e_recv.at[k],
                      (flip(d, orders[0][k - n_t + 1]), t))

    pack[0] = fu[...]
    send_own(0)
    pack[1] = turn(fd)
    send_own(1)
    entry = lax.broadcasted_iota(jnp.int32, (n_gain, D), 0)
    lane = lax.broadcasted_iota(jnp.int32, (n_gain, D), 1)
    gain_spot = (lane == (d * n_t + t) * n_gain + entry).astype(f32)
    spot = lax.rem(entry, n_bias) + d * n_bias + (entry // n_bias + t * local_heads) * head_dim
    bias_spot = (lane == spot).astype(f32)
    high = lax.Precision.HIGHEST
    is_gain = lax.broadcasted_iota(jnp.int32, (8, D), 0) < 5
    e_acc[0] = jnp.where(is_gain, jnp.dot(gain_ref[...], gain_spot, precision=high, preferred_element_type=f32),
                         jnp.dot(gain_ref[...], bias_spot, precision=high, preferred_element_type=f32))
    for k in range(n_t - 1):
        e_copy(k).start()
    for k in range(4):
        pack[2, :, k * w:(k + 1) * w] = at[k]
    send_own(2)
    pack[3, :, 0:2 * w] = cw[...]
    pack[3, :, 2 * w:3 * w] = turn(ao)
    pack[3, :, 3 * w:4 * w] = turn(co)
    send_own(3)
    for step in range(n_t - 1):
        f_copy(step).start()
    own_f = pltpu.make_async_copy(f_ref, gf_ref.at[t], local_sem.at[2 * CHUNKS])
    own_f.start()
    pack[4] = su[...]
    send_own(4)
    pack[5] = turn(sd)
    send_own(5)
    total = e_acc[0]
    for k in range(n_t - 1):
        e_copy(k).wait_recv()
        total = total + e_buf[k]
    e_acc[1] = total

    def relay(stage, c):
        if stage == 0:
            local_copy(c).wait()
            for step in range(n_t - 1):
                z_copy(c, step).wait_recv()
        else:
            for copy in dp_copies(c, stage - 1):
                copy.wait_recv()
        if stage < stages:
            for copy in dp_copies(c, stage):
                copy.start()
        else:
            out_copy(c).start()

    def chain(number):
        if 0 < number <= len(orders[0]):
            e_copy(n_t - 2 + number).wait_recv()
            e_acc[number + 1] = e_acc[number] + e_buf[n_t - 2 + number]
        if number < len(orders[0]):
            e_copy(n_t - 1 + number).start()

    def step_all(number):
        chain(number)
        for stage in range(stages + 1):
            if 0 <= number - stage < CHUNKS:
                relay(stage, number - stage)

    step_t = tab_ref.shape[1]

    def table(k, carry):
        cs, cc = tab_ref[0, pl.ds(k, 1), :], tab_ref[1, pl.ds(k, 1), :]
        part = block_of(k, step_t)
        phase_ref[part, 0:D // 2] = (cs * tab_ref[3] + cc * tab_ref[2]).astype(bf16)
        phase_ref[part, D // 2:D] = (cc * tab_ref[3] - cs * tab_ref[2]).astype(bf16)
        return carry
    lax.fori_loop(0, frames // step_t, table, 0)

    def own_table(k, carry):
        at_k = t * (rows // step_t) + k
        cs, cc = tab_ref[0, pl.ds(at_k, 1), :], tab_ref[1, pl.ds(at_k, 1), :]
        part = block_of(k, step_t)
        turn_ref[0, part, :] = cs * tab_ref[3] + cc * tab_ref[2]
        turn_ref[1, part, :] = cc * tab_ref[3] - cs * tab_ref[2]
        return carry
    lax.fori_loop(0, rows // step_t, own_table, 0)

    last = len(orders[0]) + 1
    for number in range(stages + 2):
        step_all(number)
    gains_out[...] = e_acc[last]

    def norm_one(part):
        a_s[part, :] = (norm_parts(x_ref[part, :].astype(f32))[0] * gains_out[0:1, :]).astype(bf16)
    row_loop(rows, 64, norm_one)
    feed_rows(a_s, wbuf.at[0], wbuf.at[1], z_s)

    def norm_two(part):
        value = x_ref[part, :].astype(f32) + 0.5 * z_s[part, :]
        x1_ref[part, :] = value
        a_s[part, :] = (norm_parts(value)[0] * gains_out[1:2, :]).astype(bf16)
    row_loop(rows, 64, norm_two)
    for step in range(n_t - 1):
        a_copy(step).start()
    a2_ref[t] = a_s[...]
    for number in range(stages + 2, CHUNKS + stages):
        step_all(number)
    for step in range(n_t - 1):
        a_copy(step).wait_recv()

    scale = head_dim ** -0.5
    z_s[...] = jnp.zeros_like(z_s)

    def head_group(j, carry):
        cols = block_of(j, width)
        block = wbuf[2, :, cols]
        kv_cols = block[:, w:3 * w]
        for part in range(n_t):
            kv_ref[j, part * rows:(part + 1) * rows, :] = dot(a2_ref[part], kv_cols, 1, 0).astype(bf16)
        q = dot(a_s[...], block[:, 0:w], 1, 0)
        if w % 128 == 0:
            bias = gains_out[5:7, pl.ds(pl.multiple_of(j * w, w), w)]
        else:
            bias = keep(lax.broadcasted_iota(jnp.int32, (2, w), 0) >= 0, gains_out[5:7, 0:w])
            for other in range(1, n_t):
                bias = jnp.where(j == other, gains_out[5:7, other * w:(other + 1) * w], bias)
        cq = (q + bias[0:1]).astype(bf16)
        pq = (q + bias[1:2]).astype(bf16)
        cq_ref[j] = cq
        pq_ref[j] = pq
        for h in range(local_heads):
            mask = lane_head((rows, w), head_dim, h)
            turned = dot(keep(mask, pq), block[:, 3 * w:4 * w], 1, 1)
            rs, rc = turned[:, :D // 2], turned[:, D // 2:]
            u_s[:, 0:D // 2] = (rc * turn_ref[0] - rs * turn_ref[1]).astype(bf16)
            u_s[:, D // 2:D] = (rs * turn_ref[0] + rc * turn_ref[1]).astype(bf16)
            s_s[...] = (dot(u_s[...], phase_ref[...], 1, 1)
                        + dot(keep(mask, cq), kv_ref[j, :, 0:w], 1, 1))
            head = j * local_heads + h

            def soften(part):
                s = s_s[part, :] * scale
                e = jnp.exp(s - jnp.max(s, axis=-1, keepdims=True))
                p_ref[head, part, :] = (e * (1.0 / jnp.sum(e, axis=-1, keepdims=True))).astype(bf16)
            row_loop(rows, 32, soften)
            mixed = dot(p_ref[head], kv_ref[j, :, w:2 * w], 1, 0).astype(bf16)
            mixture = mixed if h == 0 else jnp.where(mask, mixed, mixture)
        mix_ref[j] = mixture
        block = wbuf[3, :, cols]
        z_s[...] = z_s[...] + dot(mixture, block[:, 2 * w:3 * w], 1, 1)
        return carry
    lax.fori_loop(0, n_t, head_group, 0)
    x2_ref[...] = x1_ref[...] + z_s[...]

    for step in range(n_t - 1):
        f_copy(step).wait()
        a_copy(step).wait_send()
    own_f.wait()
    for k in range(n_t - 1 + len(orders[0])):
        e_copy(k).wait_send()
    for c in range(CHUNKS):
        out_copy(c).wait()
        for step in range(n_t - 1):
            z_copy(c, step).wait_send()
        for stage in range(stages):
            for copy in dp_copies(c, stage):
                copy.wait_send()


def forward_kernel(n_dp, n_t, head_dim, args, gains, taps, x, tables):
    rows, D = x.shape
    rows_w, width = args[0].shape
    w = D // n_t
    frames = rows * n_t
    heads = D // head_dim
    n_e = n_t - 1 + n_dp.bit_length() - 1
    dma = pltpu.SemaphoreType.DMA
    vmem = pl.BlockSpec(memory_space=pltpu.VMEM)
    hbm = pl.BlockSpec(memory_space=pl.ANY)

    def shape(*dims, kind=bf16):
        return jax.ShapeDtypeStruct(dims, kind)
    inputs = list(args) + [gains, taps, x, tables]
    outs = (shape(CHUNKS, n_dp * rows_w, n_t * width), shape(8, D, kind=f32), shape(n_t, *taps.shape, kind=f32),
            shape(rows, D, kind=f32), shape(rows, D, kind=f32), shape(n_t, rows, D), shape(n_t, frames, 2 * w),
            shape(n_t, rows, w), shape(n_t, rows, w), shape(heads, rows, frames), shape(n_t, rows, w),
            shape(frames, D), shape(2, rows, D // 2, kind=f32))
    return pl.pallas_call(
        functools.partial(forward_body, n_dp, n_t, head_dim),
        name="forward",
        out_shape=outs,
        in_specs=[vmem] * len(inputs),
        out_specs=(hbm,) + (vmem,) * (len(outs) - 1),
        scratch_shapes=[
            pltpu.VMEM((CHUNKS, rows_w, width), bf16), pltpu.VMEM((CHUNKS, n_dp * rows_w, n_t * width), bf16),
            pltpu.VMEM((rows, D), bf16), pltpu.VMEM((rows, D), f32), pltpu.VMEM((rows, frames), f32),
            pltpu.VMEM((rows, D), bf16),
            pltpu.VMEM((n_dp.bit_length() + 1, 8, D), f32), pltpu.VMEM((n_e, 8, D), f32),
            dma((2 * CHUNKS + 1,)), dma((CHUNKS, n_t - 1)), dma((CHUNKS, n_t - 1)),
            dma((CHUNKS, 2, n_dp - 1)), dma((CHUNKS, 2, n_dp - 1)),
            dma((n_t - 1,)), dma((n_t - 1,)), dma((n_e,)), dma((n_e,)), dma((n_t - 1,)), dma((n_t - 1,))],
        compiler_params=pltpu.CompilerParams(collective_id=0, has_side_effects=True, vmem_limit_bytes=60 << 20),
    )(*inputs)
```

```python
import functools
import math
from types import SimpleNamespace

import jax
import jax.numpy as jnp
import numpy as np
from jax import lax
from jax.experimental import pallas as pl
from jax.experimental.pallas import tpu as pltpu
from jax.sharding import PartitionSpec as P

MESH = pl.DeviceIdType.MESH
CHUNKS = 6
CORE = 1
EDGE = 16
KERNEL = 31
HALF = KERNEL // 2
norm_eps = 1e-05
f32 = jnp.float32
bf16 = jnp.bfloat16
high = lax.Precision.HIGHEST


def flip(index, mask):
    result = index
    bit = 1
    while bit <= mask:
        if mask & bit:
            result = result + bit - 2 * bit * ((index // bit) % 2)
        bit *= 2
    return result


def span(bits):
    masks = [0]
    for bit in bits:
        masks = masks + [mask ^ bit for mask in masks]
    return masks


def link_orders(n_dp):
    bits = [1 << k for k in range(1, n_dp.bit_length() - 1)]
    return (bits, bits[::-1])


def greet(peers):
    barrier = pltpu.get_barrier_semaphore()
    for peer in peers:
        pl.semaphore_signal(barrier, inc=1, device_id=peer, device_id_type=MESH)
    pl.semaphore_wait(barrier, len(peers))


def remote(src, dst, send_sem, recv_sem, peer):
    return pltpu.make_async_remote_copy(
        src_ref=src, dst_ref=dst, send_sem=send_sem, recv_sem=recv_sem,
        device_id=peer, device_id_type=MESH)


def start_all(copies):
    for copy in copies:
        copy.start()


def arrive_all(copies):
    for copy in copies:
        copy.wait_recv()


def sent_all(copies):
    for copy in copies:
        copy.wait_send()


def dot(left, right, left_dim, right_dim):
    return lax.dot_general(left, right, (((left_dim,), (right_dim,)), ((), ())), preferred_element_type=f32)


def turned(value):
    return value.astype(f32).T.astype(bf16)


def head_mask(shape, axis, head_dim, head):
    place = lax.broadcasted_iota(jnp.int32, shape, axis)
    return (place >= head * head_dim) & (place < (head + 1) * head_dim)


def keep(mask, value):
    return jnp.where(mask, value, jnp.zeros_like(value))


def block_of(k, size):
    return pl.ds(pl.multiple_of(k * size, size), size)


def loop(count, body):
    def step(k, carry):
        body(k)
        return carry
    lax.fori_loop(0, count, step, 0)


def row_loop(rows, size, body):
    loop(rows // size, lambda k: body(block_of(k, size)))


def sigmoid(values):
    return 1.0 / (1.0 + jnp.exp(-values))


def norm_parts(values):
    centred = values - jnp.mean(values, axis=-1, keepdims=True)
    inverse = lax.rsqrt(jnp.mean(centred * centred, axis=-1, keepdims=True) + norm_eps)
    return centred * inverse, inverse


def norm_back(value, incoming, gain_row):
    scaled, inverse = norm_parts(value)
    grad_scaled = incoming * gain_row
    inner = jnp.mean(grad_scaled * scaled, axis=-1, keepdims=True)
    grad_in = inverse * (grad_scaled - jnp.mean(grad_scaled, axis=-1, keepdims=True) - scaled * inner)
    return scaled, grad_in, jnp.sum(incoming * scaled, axis=0, keepdims=True)


SLAB = 512


def feed_rows(a_ref, up, down_t, z_ref, hidden, slope):
    z_ref[...] = jnp.zeros_like(z_ref)

    def step(k):
        cols = block_of(k, SLAB)
        pre = dot(a_ref[...], up[:, cols], 1, 0)
        sig = sigmoid(pre)
        hidden[:, cols] = (pre * sig).astype(bf16)
        slope[:, cols] = (sig * (1.0 + pre * (1.0 - sig))).astype(bf16)
        z_ref[...] = z_ref[...] + dot(hidden[:, cols], down_t[:, cols], 1, 1)
    loop(up.shape[1] // SLAB, step)


def feed_back(dz_ref, dz_turn, a_turn, up, down_t, z_ref, hidden, slope, g_up, g_down):
    z_ref[...] = jnp.zeros_like(z_ref)

    def step(k):
        cols = block_of(k, SLAB)
        g_down[:, cols] = dot(dz_turn[...], hidden[:, cols], 1, 0).astype(bf16)
        grad_pre = (dot(dz_ref[...], down_t[:, cols], 1, 0) * slope[:, cols].astype(f32)).astype(bf16)
        g_up[:, cols] = dot(a_turn[...], grad_pre, 1, 0).astype(bf16)
        z_ref[...] = z_ref[...] + dot(grad_pre, up[:, cols], 1, 1)
    loop(up.shape[1] // SLAB, step)


def layer_body(names, n_dp, n_t, head_dim, *all_refs):
    r = SimpleNamespace(**dict(zip(names, all_refs)))
    d = lax.axis_index("dp")
    t = lax.axis_index("tensor")
    pack, wbuf, gbuf = r.pack, r.wbuf, r.gbuf
    x_ref, gains, taps = r.x, r.gains, r.taps
    rows_w, width = pack.shape[1], pack.shape[2]
    rows, D = x_ref.shape
    w = D // n_t
    half = n_t * width // 2
    frames = rows * n_t
    local_heads = w // head_dim
    n_gain = r.gain_in.shape[1]
    n_bias = n_gain // local_heads
    row_count = frames * n_dp
    scale = head_dim ** -0.5
    links = link_orders(n_dp)
    orders = [order + [CORE] for order in links]
    stages = len(orders[0])
    n_link = len(links[0])
    z_peers = [(d, lax.rem(t + step, n_t)) for step in range(1, n_t)]
    d_peers = [(flip(d, mask), t) for mask in range(1, n_dp)]
    before = (d, lax.rem(t + n_t - 1, n_t))
    after = (d, lax.rem(t + 1, n_t))
    z_range = range(n_t - 1)
    greet(z_peers + d_peers)

    eye = (lax.broadcasted_iota(jnp.int32, (rows_w, rows_w), 0)
           == lax.broadcasted_iota(jnp.int32, (rows_w, rows_w), 1)).astype(bf16)

    def turn(ref):
        return dot(eye, ref[...], 1, 1).astype(bf16)

    def window(c, mask, start, size):
        first = pl.multiple_of(flip(d, mask) * rows_w, rows_w)
        return wbuf.at[c, pl.ds(first, rows_w), pl.ds(start, size)]

    def own(c):
        return window(c, 0, pl.multiple_of(t * width, width), width)

    def z_copies(c):
        return [remote(pack.at[c], own(c), r.z_send.at[c, k], r.z_recv.at[c, k], z_peers[k]) for k in z_range]

    def local_copy(c):
        return pltpu.make_async_copy(pack.at[c], own(c), r.local_sem.at[c])

    def dp_copies(c, stage):
        copies = []
        for h in range(2):
            bit = orders[h][stage]
            masks = span(orders[h][:stage])
            for j, mask in enumerate(masks):
                slot = len(masks) - 1 + j
                part = window(c, mask, h * half, half)
                copies.append(remote(part, part, r.d_send.at[c, h, slot], r.d_recv.at[c, h, slot],
                                     (flip(d, bit), t)))
        return copies

    def send_own(c):
        local_copy(c).start()
        start_all(z_copies(c))

    e_acc, e_buf = r.e_acc, r.e_buf

    def e_copies(first, stop):
        copies = []
        for k in range(first, stop):
            if k < n_t - 1:
                source, peer = e_acc.at[0], z_peers[k]
            else:
                source, peer = e_acc.at[k - n_t + 2], (flip(d, orders[0][k - n_t + 1]), t)
            copies.append(remote(source, e_buf.at[k], r.e_send.at[k], r.e_recv.at[k], peer))
        return copies

    tap_copies = [remote(r.tap_in, taps.at[t], r.f_send.at[k], r.f_recv.at[k], z_peers[k]) for k in z_range]

    pack[0] = r.fu[...]
    send_own(0)
    pack[1] = turn(r.fd)
    send_own(1)
    entry = lax.broadcasted_iota(jnp.int32, (n_gain, D), 0)
    lane = lax.broadcasted_iota(jnp.int32, (n_gain, D), 1)
    gain_spot = (lane == (d * n_t + t) * n_gain + entry).astype(f32)
    bias_spot = (lane == lax.rem(entry, n_bias) + d * n_bias
                 + (entry // n_bias + t * local_heads) * head_dim).astype(f32)
    is_gain = lax.broadcasted_iota(jnp.int32, (8, D), 0) < 5
    e_acc[0] = jnp.where(is_gain, jnp.dot(r.gain_in[...], gain_spot, precision=high, preferred_element_type=f32),
                         jnp.dot(r.gain_in[...], bias_spot, precision=high, preferred_element_type=f32))
    start_all(e_copies(0, n_t - 1))
    for k in range(4):
        pack[2, :, k * w:(k + 1) * w] = r.at[k]
    send_own(2)
    pack[3, :, 0:2 * w] = r.cw[...]
    pack[3, :, 2 * w:3 * w] = turn(r.ao)
    pack[3, :, 3 * w:4 * w] = turn(r.co)
    send_own(3)
    start_all(tap_copies)
    taps[t] = r.tap_in[...]
    pack[4] = r.su[...]
    send_own(4)
    pack[5] = turn(r.sd)
    send_own(5)
    arrive_all(e_copies(0, n_t - 1))
    total = e_acc[0]
    for k in z_range:
        total = total + e_buf[k]
    e_acc[1] = total

    def tick(number):
        if 0 < number <= n_link + 1:
            arrive_all(e_copies(n_t - 2 + number, n_t - 1 + number))
            e_acc[number + 1] = e_acc[number] + e_buf[n_t - 2 + number]
        if number <= n_link:
            start_all(e_copies(n_t - 1 + number, n_t + number))
        for stage in range(stages + 1):
            c = number - stage
            if not 0 <= c < CHUNKS:
                continue
            if stage == 0:
                local_copy(c).wait()
                arrive_all(z_copies(c))
            else:
                arrive_all(dp_copies(c, stage - 1))
            if stage < stages:
                start_all(dp_copies(c, stage))

    tab, phase, spin = r.tab, r.phase, r.spin
    step_t = tab.shape[1]

    def table(k):
        cs, cc = tab[0, pl.ds(k, 1), :], tab[1, pl.ds(k, 1), :]
        part = block_of(k, step_t)
        phase[part, 0:D // 2] = (cs * tab[3] + cc * tab[2]).astype(bf16)
        phase[part, D // 2:D] = (cc * tab[3] - cs * tab[2]).astype(bf16)
    loop(frames // step_t, table)

    def own_table(k):
        place = t * (rows // step_t) + k
        cs, cc = tab[0, pl.ds(place, 1), :], tab[1, pl.ds(place, 1), :]
        part = block_of(k, step_t)
        spin[0, part, :] = cs * tab[3] + cc * tab[2]
        spin[1, part, :] = cc * tab[3] - cs * tab[2]
    loop(rows // step_t, own_table)

    def spun(sines, cosines):
        u_s = r.u_s
        u_s[:, 0:D // 2] = (cosines * spin[0] - sines * spin[1]).astype(bf16)
        u_s[:, D // 2:D] = (sines * spin[0] + cosines * spin[1]).astype(bf16)

    z_s, a1, a2, a2_all = r.z_s, r.a1, r.a2, r.a2_all
    x1, x2, x3 = r.x1, r.x2, r.x3
    for number in range(stages + 2):
        tick(number)
    gains[...] = e_acc[n_link + 2]

    def norm_one(part):
        a1[part, :] = (norm_parts(x_ref[part, :].astype(f32))[0] * gains[0:1, :]).astype(bf16)
    row_loop(rows, 64, norm_one)
    feed_rows(a1, wbuf.at[0], wbuf.at[1], z_s, r.hid1, r.slope1)

    def norm_two(part):
        value = x_ref[part, :].astype(f32) + 0.5 * z_s[part, :]
        x1[part, :] = value
        a2[part, :] = (norm_parts(value)[0] * gains[1:2, :]).astype(bf16)
    row_loop(rows, 64, norm_two)

    a_copies = [remote(a2, a2_all.at[t], r.a_send.at[k], r.a_recv.at[k], z_peers[k]) for k in z_range]
    start_all(a_copies)
    a2_all[t] = a2[...]
    for number in range(stages + 2, CHUNKS + stages):
        tick(number)
    arrive_all(a_copies)
    kv, cq, pq, probs, mix, s_s, u_s = r.kv, r.cq, r.pq, r.probs, r.mix, r.s_s, r.u_s
    z_s[...] = jnp.zeros_like(z_s)

    def head_group(j):
        cols = block_of(j, width)
        block = wbuf[2, :, cols]
        for part in range(n_t):
            kv[j, part * rows:(part + 1) * rows, :] = dot(a2_all[part], block[:, w:3 * w], 1, 0).astype(bf16)
        q = dot(a2[...], block[:, 0:w], 1, 0)
        if w % 128 == 0:
            bias = gains[5:7, block_of(j, w)]
        else:
            bias = gains[5:7, 0:w]
            for other in range(1, n_t):
                bias = jnp.where(j == other, gains[5:7, other * w:(other + 1) * w], bias)
        cq_j = (q + bias[0:1]).astype(bf16)
        pq_j = (q + bias[1:2]).astype(bf16)
        cq[j] = cq_j
        pq[j] = pq_j
        for h in range(local_heads):
            mask = head_mask((rows, w), 1, head_dim, h)
            spread = dot(keep(mask, pq_j), block[:, 3 * w:4 * w], 1, 1)
            spun(spread[:, :D // 2], spread[:, D // 2:])
            s_s[...] = dot(u_s[...], phase[...], 1, 1) + dot(keep(mask, cq_j), kv[j, :, 0:w], 1, 1)
            head = j * local_heads + h

            def soften(part):
                s = s_s[part, :] * scale
                e = jnp.exp(s - jnp.max(s, axis=-1, keepdims=True))
                probs[head, part, :] = (e * (1.0 / jnp.sum(e, axis=-1, keepdims=True))).astype(bf16)
            row_loop(rows, 32, soften)
            mixed = dot(probs[head], kv[j, :, w:2 * w], 1, 0).astype(bf16)
            mixture = mixed if h == 0 else jnp.where(mask, mixed, mixture)
        mix[j] = mixture
        z_s[...] = z_s[...] + dot(mixture, wbuf[3, :, cols][:, 2 * w:3 * w], 1, 1)
    loop(n_t, head_group)

    a3, glu, bhat, val, sig, act = r.a3, r.glu, r.bhat, r.val, r.sig, r.act
    dbn, sums, sum_buf, sum_mid, sum_z = r.dbn, r.sums, r.sum_buf, r.sum_mid, r.sum_z
    inner = pl.ds(EDGE, rows)

    def norm_three(part):
        value = x1[part, :] + z_s[part, :]
        x2[part, :] = value
        a3[part, :] = (norm_parts(value)[0] * gains[2:3, :]).astype(bf16)
    row_loop(rows, 64, norm_three)

    def gate(j):
        block = wbuf[3, :, block_of(j, width)]
        e = dot(a3[...], block[:, 0:2 * w], 1, 0)
        sig_j = sigmoid(e[:, w:2 * w])
        val[j] = e[:, 0:w]
        sig[j] = sig_j
        glu[j, inner, :] = e[:, 0:w] * sig_j
    loop(n_t, gate)

    def edge_copies(ref, k):
        first, last = pl.ds(EDGE, EDGE), pl.ds(rows, EDGE)
        return [remote(ref.at[:, first, :], ref.at[:, pl.ds(EDGE + rows, EDGE), :], r.edge_send.at[k, 0],
                       r.edge_recv.at[k, 0], before),
                remote(ref.at[:, last, :], ref.at[:, pl.ds(0, EDGE), :], r.edge_send.at[k, 1],
                       r.edge_recv.at[k, 1], after)]

    def close_edges(ref):
        ref[:, pl.ds(0, EDGE), :] = jnp.where(t > 0, ref[:, pl.ds(0, EDGE), :], 0.0)
        tail = pl.ds(EDGE + rows, EDGE)
        ref[:, tail, :] = jnp.where(t < n_t - 1, ref[:, tail, :], 0.0)

    def sum_copies(k):
        return [remote(sums.at[k], sum_buf.at[k, i], r.sum_send.at[k, i], r.sum_recv.at[k, i], d_peers[i])
                for i in range(n_dp - 1)]

    def sum_z_copies(k):
        return [remote(sum_mid.at[k], sum_z.at[k, i], r.sumz_send.at[k, i], r.sumz_recv.at[k, i], z_peers[i])
                for i in z_range]

    def sum_middle(k):
        arrive_all(sum_copies(k))
        total = sums[k]
        for i in range(n_dp - 1):
            total = total + sum_buf[k, i]
        sum_mid[k] = total
        start_all(sum_z_copies(k))

    def sum_end(k):
        arrive_all(sum_z_copies(k))
        total = sum_mid[k]
        for i in z_range:
            total = total + sum_z[k, i]
        sum_mid_out = r.sum_out
        sum_mid_out[k] = total

    start_all(edge_copies(glu, 0))
    arrive_all(tap_copies)
    arrive_all(edge_copies(glu, 0))
    sent_all(edge_copies(glu, 0))
    close_edges(glu)
    size = 64

    def sweep(ref, j, first, backward):
        total = None
        for k in range(KERNEL):
            offset = EDGE - HALF + (KERNEL - 1 - k if backward else k)
            term = taps[j, k:k + 1, :] * ref[j, pl.ds(first + offset, size), :]
            total = term if total is None else total + term
        return total

    def convolve(j):
        def part_step(k, carry):
            first = pl.multiple_of(k * size, size)
            value = sweep(glu, j, first, False)
            bhat[j, pl.ds(first + EDGE, size), :] = value
            return (carry[0] + jnp.sum(value, axis=0, keepdims=True),
                    carry[1] + jnp.sum(value * value, axis=0, keepdims=True))
        zero = jnp.zeros((1, w), f32)
        one, two = lax.fori_loop(0, rows // size, part_step, (zero, zero))
        sums[0, pl.ds(2 * j, 1), :] = one
        sums[0, pl.ds(2 * j + 1, 1), :] = two
    loop(n_t, convolve)
    start_all(sum_copies(0))
    sum_middle(0)
    sum_end(0)

    def bn_parts(j):
        mean = r.sum_out[0, pl.ds(2 * j, 1), :] / row_count
        square = r.sum_out[0, pl.ds(2 * j + 1, 1), :] / row_count
        return mean, lax.rsqrt(square - mean * mean + norm_eps), taps[j, KERNEL:KERNEL + 1, :], taps[
            j, KERNEL + 1:KERNEL + 2, :]

    z_s[...] = jnp.zeros_like(z_s)

    def activate(j):
        mean, inverse, bn_gain, bn_shift = bn_parts(j)
        scaled = (bhat[j, inner, :] - mean) * inverse
        bhat[j, inner, :] = scaled
        normal = scaled * bn_gain + bn_shift
        act[j] = (normal * sigmoid(normal)).astype(bf16)
        z_s[...] = z_s[...] + dot(act[j], wbuf[3, :, block_of(j, width)][:, 3 * w:4 * w], 1, 1)
    loop(n_t, activate)
    start_all(edge_copies(bhat, 1))

    a4, dx = r.a4, r.dx0

    def norm_four(part):
        value = x2[part, :] + z_s[part, :]
        x3[part, :] = value
        a4[part, :] = (norm_parts(value)[0] * gains[3:4, :]).astype(bf16)
    row_loop(rows, 64, norm_four)
    feed_rows(a4, wbuf.at[4], wbuf.at[5], z_s, r.hid2, r.slope2)
    gsum = r.gsum
    gsum[0] = jnp.zeros_like(gsum[0])
    dz, dz_turn, a_turn = r.dz, r.dz_turn, r.a_turn

    def add_gain(row, part_sum):
        gsum[0, row:row + 1, :] = gsum[0, row:row + 1, :] + part_sum

    def norm_five(part):
        value = x3[part, :] + 0.5 * z_s[part, :]
        scaled, grad_in, part_sum = norm_back(value, r.og[part, :].astype(f32), gains[4:5, :])
        r.out[part, :] = scaled * gains[4:5, :]
        dx[part, :] = grad_in
        dz[part, :] = (0.5 * grad_in).astype(bf16)
        add_gain(4, part_sum)
    row_loop(rows, 64, norm_five)

    def grad_chunk(c):
        return gbuf.at[c - 2] if c >= 2 else wbuf.at[c + 4]

    def join_norm(row, x_of, factor):
        def step(part):
            _, grad_in, part_sum = norm_back(x_of(part), z_s[part, :], gains[row:row + 1, :])
            value = dx[part, :] + grad_in
            dx[part, :] = value
            dz[part, :] = (factor * value).astype(bf16)
            add_gain(row, part_sum)
        row_loop(rows, 64, step)

    folds = [order[::-1] for order in links]
    groups = span(links[0])
    core_buf, dp_buf, z_buf = r.core_buf, r.dp_buf, r.z_buf

    def grad_rows(c, mask):
        return grad_chunk(c).at[pl.ds(pl.multiple_of(flip(d, mask) * rows_w, rows_w), rows_w), :]

    def core_copies(c):
        return [remote(grad_rows(c, mask ^ CORE), core_buf.at[c, k], r.core_send.at[c, k], r.core_recv.at[c, k],
                       (flip(d, CORE), t)) for k, mask in enumerate(groups)]

    def fold_moves(c, stage):
        moves = []
        for h in range(2):
            bit = folds[h][stage]
            masks = span(folds[h][stage + 1:])
            base = len(groups) - 2 * len(masks)
            for j, mask in enumerate(masks):
                slot = base + j
                copy = remote(grad_rows(c, mask ^ bit).at[:, pl.ds(h * half, half)], dp_buf.at[c, h, slot],
                              r.fd_send.at[c, h, slot], r.fd_recv.at[c, h, slot], (flip(d, bit), t))
                moves.append((copy, mask, h, slot))
        return moves

    def fold_copies(c, stage):
        return [move[0] for move in fold_moves(c, stage)]

    def fold_z_copies(c):
        copies = []
        for k in z_range:
            target = lax.rem(t + k + 1, n_t)
            source = grad_rows(c, 0).at[:, pl.ds(pl.multiple_of(target * width, width), width)]
            copies.append(remote(source, z_buf.at[c, k], r.fz_send.at[c, k], r.fz_recv.at[c, k], z_peers[k]))
        return copies

    piece = 16

    def fold_start(c):
        start_all(core_copies(c))

    def fold_next(c, stage):
        if stage < n_link:
            start_all(fold_copies(c, stage))
        else:
            start_all(fold_z_copies(c))

    def fold_step(c, stage):
        ref = grad_chunk(c)
        if stage == 0:
            arrive_all(core_copies(c))
            for k, mask in enumerate(groups):
                base = flip(d, mask) * rows_w

                def add_core(step, k=k, base=base):
                    part = pl.ds(pl.multiple_of(base + step * piece, piece), piece)
                    ref[part, :] = (ref[part, :].astype(f32)
                                    + core_buf[c, k, block_of(step, piece), :].astype(f32)).astype(bf16)
                loop(rows_w // piece, add_core)
            fold_next(c, 0)
        elif stage <= n_link:
            for copy, mask, h, slot in fold_moves(c, stage - 1):
                copy.wait_recv()
                base = flip(d, mask) * rows_w
                cols = pl.ds(h * half, half)

                def add_dp(step, base=base, cols=cols, h=h, slot=slot):
                    part = pl.ds(pl.multiple_of(base + step * piece, piece), piece)
                    ref[part, cols] = (ref[part, cols].astype(f32)
                                       + dp_buf[c, h, slot, block_of(step, piece), :].astype(f32)).astype(bf16)
                loop(rows_w // piece, add_dp)
            fold_next(c, stage)
        else:
            arrive_all(fold_z_copies(c))

            def finish(step):
                part = pl.ds(pl.multiple_of(d * rows_w + step * piece, piece), piece)
                total = ref[part, block_of(t, width)].astype(f32)
                for k in z_range:
                    total = total + z_buf[c, k, block_of(step, piece), :].astype(f32)
                r.shards[c, block_of(step, piece), :] = total
            loop(rows_w // piece, finish)

    final = n_link + 1

    dz_turn[...] = turned(dz[...])
    a_turn[...] = turned(a4[...])
    sent_all([copy for c in range(CHUNKS) for copy in z_copies(c)])
    sent_all([copy for c in range(CHUNKS) for stage in range(stages) for copy in dp_copies(c, stage)])
    feed_back(dz, dz_turn, a_turn, wbuf.at[4], wbuf.at[5], z_s, r.hid2, r.slope2, grad_chunk(4), grad_chunk(5))
    fold_start(4)
    fold_start(5)
    join_norm(3, lambda part: x3[part, :], 1.0)

    dz_turn[...] = turned(dz[...])

    def act_back(j):
        mean, inverse, bn_gain, bn_shift = bn_parts(j)
        grad_act = dot(dz[...], wbuf[3, :, block_of(j, width)][:, 3 * w:4 * w], 1, 0)
        scaled = bhat[j, inner, :]
        normal = scaled * bn_gain + bn_shift
        sig_n = sigmoid(normal)
        value = grad_act * (sig_n * (1.0 + normal * (1.0 - sig_n)))
        dbn[j, inner, :] = value
        sums[1, pl.ds(2 * j, 1), :] = jnp.sum(value * scaled, axis=0, keepdims=True)
        sums[1, pl.ds(2 * j + 1, 1), :] = jnp.sum(value, axis=0, keepdims=True)
    loop(n_t, act_back)
    start_all(sum_copies(1))
    start_all(edge_copies(dbn, 2))
    fold_step(4, 0)
    sum_middle(1)
    fold_step(5, 0)
    a_turn[...] = turned(a3[...])
    sum_end(1)
    for k, ref in ((1, bhat), (2, dbn)):
        arrive_all(edge_copies(ref, k))
        sent_all(edge_copies(ref, k))
    r.bn_out[...] = r.sum_out[1, pl.ds(2 * t, 2), :]
    small = r.small
    z_s[...] = jnp.zeros_like(z_s)

    def put_grad(c, j, first, value):
        if w % 128 == 0:
            grad_chunk(c)[:, pl.ds(pl.multiple_of(j * width + first, 128), value.shape[1])] = value
        else:
            old = grad_chunk(c)[:, block_of(j, width)]
            pieces = [old[:, :first], value, old[:, first + value.shape[1]:]]
            grad_chunk(c)[:, block_of(j, width)] = jnp.concatenate([p for p in pieces if p.shape[1] > 0], axis=1)

    def conv_back(j):
        mean, inverse, bn_gain, bn_shift = bn_parts(j)
        gamma = r.sum_out[1, pl.ds(2 * j, 1), :] / row_count
        beta = r.sum_out[1, pl.ds(2 * j + 1, 1), :] / row_count
        dbn[j] = bn_gain * inverse * (dbn[j] - beta - bhat[j] * gamma)
        dbn[j, pl.ds(0, EDGE), :] = jnp.where(t > 0, dbn[j, pl.ds(0, EDGE), :], 0.0)
        tail = pl.ds(EDGE + rows, EDGE)
        dbn[j, tail, :] = jnp.where(t < n_t - 1, dbn[j, tail, :], 0.0)

        def tap_step(k, carry):
            first = pl.multiple_of(k * size, size)
            own_part = dbn[j, pl.ds(first + EDGE, size), :]
            result = []
            for tap in range(KERNEL):
                term = own_part * glu[j, pl.ds(first + EDGE - HALF + tap, size), :]
                result.append(carry[tap] + jnp.sum(term.reshape(size // 8, 8, w), axis=0))
            return tuple(result)
        tap_sums = lax.fori_loop(0, rows // size, tap_step, tuple(jnp.zeros((8, w), f32) for _ in range(KERNEL)))
        for tap in range(KERNEL):
            small[0, j, tap:tap + 1, :] = jnp.sum(tap_sums[tap], axis=0, keepdims=True)

        def spread_step(k):
            first = pl.multiple_of(k * size, size)
            part = pl.ds(first, size)
            dglu = sweep(dbn, j, first, True)
            sig_p = sig[j, part, :]
            grad_val = dglu * sig_p
            r.de[part, 0:w] = grad_val.astype(bf16)
            r.de[part, w:2 * w] = (grad_val * val[j, part, :] * (1.0 - sig_p)).astype(bf16)
        loop(rows // size, spread_step)
        put_grad(3, j, 0, dot(a_turn[...], r.de[...], 1, 0).astype(bf16))
        put_grad(3, j, 3 * w, dot(dz_turn[...], act[j], 1, 0).astype(bf16))
        z_s[...] = z_s[...] + dot(r.de[...], wbuf[3, :, block_of(j, width)][:, 0:2 * w], 1, 1)
    loop(n_t, conv_back)
    fold_step(4, 1)
    fold_step(5, 1)
    join_norm(2, lambda part: x2[part, :], 1.0)

    dz_turn[...] = turned(dz[...])
    loop(n_t, lambda j: put_grad(3, j, 2 * w, dot(dz_turn[...], mix[j], 1, 0).astype(bf16)))
    fold_start(3)
    a2_turn, ds_s, rf_acc, rf_buf = r.a2_turn, r.ds_s, r.rf_acc, r.rf_buf
    for part in range(n_t):
        a2_turn[:, part * rows:(part + 1) * rows] = turned(a2_all[part])
    z_s[...] = jnp.zeros_like(z_s)
    rf_acc[...] = jnp.zeros_like(rf_acc)
    for stage in range(2, final + 1):
        fold_step(4, stage)
        fold_step(5, stage)

    def head_back(j):
        cols = block_of(j, width)
        block = wbuf[2, :, cols]
        dmix = dot(dz[...], wbuf[3, :, cols][:, 2 * w:3 * w], 1, 0)
        dmix_turn = dmix.T.astype(bf16)
        dmix = dmix.astype(bf16)
        cq_turn, pq_turn = turned(cq[j]), turned(pq[j])
        for h in range(local_heads):
            mask = head_mask((rows, w), 1, head_dim, h)
            turn_mask = head_mask((w, rows), 0, head_dim, h)
            head = j * local_heads + h
            s_s[...] = dot(keep(mask, dmix), kv[j, :, w:2 * w], 1, 1)

            def soft_back(part):
                p = probs[head, part, :].astype(f32)
                g = s_s[part, :]
                ds_s[part, :] = (p * (g - jnp.sum(p * g, axis=-1, keepdims=True))).astype(bf16)
            row_loop(rows, 32, soft_back)
            dv_h = dot(keep(turn_mask, dmix_turn), probs[head], 1, 0)
            dk_h = dot(keep(turn_mask, cq_turn), ds_s[...], 1, 0)
            dcq_h = keep(mask, dot(ds_s[...], kv[j, :, 0:w], 1, 0))
            back = dot(ds_s[...], phase[...], 1, 0)
            spun(back[:, :D // 2], back[:, D // 2:])
            dpq_h = keep(mask, dot(u_s[...], block[:, 3 * w:4 * w], 1, 0))
            pos_h = dot(keep(turn_mask, pq_turn), u_s[...], 1, 0)
            if h == 0:
                dv, dk, dcq, dpq, pos = dv_h, dk_h, dcq_h, dpq_h, pos_h
            else:
                dv, dk, dcq, dpq, pos = dv + dv_h, dk + dk_h, dcq + dcq_h, dpq + dpq_h, pos + pos_h
        dcq = dcq * scale
        dpq = dpq * scale
        small[0, j, KERNEL:KERNEL + 1, :] = jnp.sum(dcq, axis=0, keepdims=True)
        small[0, j, KERNEL + 1:KERNEL + 2, :] = jnp.sum(dpq, axis=0, keepdims=True)
        dq = (dcq + dpq).astype(bf16)
        dkv_turn = r.dkv_turn
        dkv_turn[0:w, :] = (dk * scale).astype(bf16)
        dkv_turn[w:2 * w, :] = dv.astype(bf16)
        for part in range(n_t):
            dkv = turned(dkv_turn[:, part * rows:(part + 1) * rows])
            rf_acc[part] = rf_acc[part] + dot(dkv, block[:, w:3 * w], 1, 1)
        z_s[...] = z_s[...] + dot(dq, block[:, 0:w], 1, 1)
        put_grad(2, j, 0, dot(a2_turn[:, block_of(t, rows)], dq, 1, 0).astype(bf16))
        put_grad(2, j, w, dot(a2_turn[...], dkv_turn[...], 1, 1).astype(bf16))
        put_grad(2, j, 3 * w, (pos.T * scale).astype(bf16))
    loop(n_t, head_back)

    for part in range(n_t):
        probs[part, :, 0:D] = rf_acc[part].astype(bf16)
    rf_copies = [remote(probs.at[lax.rem(t + k + 1, n_t), :, pl.ds(0, D)], rf_buf.at[k], r.rf_ss.at[k], r.rf_rs.at[k],
                        z_peers[k]) for k in z_range]
    start_all(rf_copies)
    fold_start(2)
    small_buf, small_z = r.small_buf, r.small_z
    all_bits = [CORE] + links[0]

    def small_copy(k):
        return remote(small.at[k], small_buf.at[k], r.s_send.at[k], r.s_recv.at[k], (flip(d, all_bits[k]), t))

    small_z_copies = [remote(small.at[len(all_bits), lax.rem(t + k + 1, n_t)], small_z.at[k], r.sz_send.at[k],
                             r.sz_recv.at[k], z_peers[k]) for k in z_range]
    small_copy(0).start()
    fold_step(3, 0)
    fold_step(2, 0)
    for k in range(1, len(all_bits) + 1):
        small_copy(k - 1).wait_recv()
        small[k] = small[k - 1] + small_buf[k - 1]
        if k < len(all_bits):
            small_copy(k).start()
    start_all(small_z_copies)
    a_turn[...] = turned(a1[...])
    fold_step(3, 1)
    fold_step(2, 1)
    arrive_all(rf_copies)

    def join_rows(part):
        total = z_s[part, :] + rf_acc[t, part, :]
        for k in z_range:
            total = total + rf_buf[k, part, :].astype(f32)
        z_s[part, :] = total
    row_loop(rows, 64, join_rows)
    join_norm(1, lambda part: x1[part, :], 0.5)

    dz_turn[...] = turned(dz[...])
    feed_back(dz, dz_turn, a_turn, wbuf.at[0], wbuf.at[1], z_s, r.hid1, r.slope1, grad_chunk(0), grad_chunk(1))
    fold_start(0)
    fold_start(1)
    join_norm(0, lambda part: x_ref[part, :].astype(f32), 1.0)

    def gsum_copy(k):
        return remote(gsum.at[k], r.gsum_buf.at[k], r.g_send.at[k], r.g_recv.at[k], (flip(d, all_bits[k]), t))

    gsum_z_copies = [remote(gsum.at[len(all_bits)], r.gsum_z.at[k], r.gz_send.at[k], r.gz_recv.at[k],
                            z_peers[k]) for k in z_range]
    gsum_copy(0).start()
    for stage in range(2, final + 1):
        fold_step(3, stage)
        fold_step(2, stage)
    for k in range(1, len(all_bits) + 1):
        gsum_copy(k - 1).wait_recv()
        gsum[k] = gsum[k - 1] + r.gsum_buf[k - 1]
        if k < len(all_bits):
            gsum_copy(k).start()
    start_all(gsum_z_copies)
    for stage in range(final + 1):
        fold_step(0, stage)
        fold_step(1, stage)
    arrive_all(small_z_copies)
    total = small[len(all_bits), t]
    for k in z_range:
        total = total + small_z[k]
    r.small_out[...] = total
    arrive_all(gsum_z_copies)
    total_g = gsum[len(all_bits)]
    for k in z_range:
        total_g = total_g + r.gsum_z[k]
    spot_g = lax.dot_general(total_g, gain_spot, (((1,), (1,)), ((), ())), precision=high, preferred_element_type=f32)
    r.gain_out[...] = spot_g

    sent_all(tap_copies + a_copies + rf_copies + small_z_copies + gsum_z_copies)
    sent_all(e_copies(0, n_t + n_link))
    for k in range(2):
        sent_all(sum_copies(k) + sum_z_copies(k))
    for k in range(len(all_bits)):
        small_copy(k).wait_send()
        gsum_copy(k).wait_send()
    for c in range(CHUNKS):
        sent_all(core_copies(c) + fold_z_copies(c))
        for stage in range(n_link):
            sent_all(fold_copies(c, stage))


def layer_kernel(n_dp, n_t, head_dim, inputs):
    given = SimpleNamespace(**inputs)
    rows, D = given.x.shape
    rows_w, width = given.fu.shape
    w = D // n_t
    frames = rows * n_t
    heads = D // head_dim
    hidden = n_t * width
    n_bits = n_dp.bit_length() - 1
    n_e = n_t - 1 + n_bits
    n_gain = given.gain_in.shape[1]
    tap_rows = given.tap_in.shape[0]
    groups = n_dp // 2
    z = n_t - 1
    sem = pltpu.SemaphoreType.DMA
    vm = pltpu.VMEM
    outs = dict(
        out=((rows, D), f32), dx0=((rows, D), f32), gain_out=((8, n_gain), f32),
        shards=((CHUNKS, rows_w, width), f32), small_out=((tap_rows, w), f32), bn_out=((2, w), f32))
    edge_shape = (n_t, rows + 2 * EDGE, w)
    scratch = dict(
        pack=vm((CHUNKS, rows_w, width), bf16), wbuf=vm((CHUNKS, n_dp * rows_w, hidden), bf16),
        gbuf=vm((CHUNKS - 2, n_dp * rows_w, hidden), bf16), gains=vm((8, D), f32),
        taps=vm((n_t, tap_rows, w), f32), e_acc=vm((n_bits + 2, 8, D), f32), e_buf=vm((n_e, 8, D), f32),
        phase=vm((frames, D), bf16), spin=vm((2, rows, D // 2), f32), u_s=vm((rows, D), bf16),
        z_s=vm((rows, D), f32), x1=vm((rows, D), f32), x2=vm((rows, D), f32),
        x3=vm((rows, D), f32), a1=vm((rows, D), bf16), a2=vm((rows, D), bf16), a3=vm((rows, D), bf16),
        a4=vm((rows, D), bf16), dz=vm((rows, D), bf16), dz_turn=vm((D, rows), bf16),
        a_turn=vm((D, rows), bf16), a2_all=vm((n_t, rows, D), bf16), a2_turn=vm((D, frames), bf16),
        hid1=vm((rows, hidden), bf16), slope1=vm((rows, hidden), bf16), hid2=vm((rows, hidden), bf16),
        slope2=vm((rows, hidden), bf16), kv=vm((n_t, frames, 2 * w), bf16), cq=vm((n_t, rows, w), bf16),
        pq=vm((n_t, rows, w), bf16), mix=vm((n_t, rows, w), bf16), probs=vm((heads, rows, frames), bf16),
        s_s=vm((rows, frames), f32), ds_s=vm((rows, frames), bf16), dkv_turn=vm((2 * w, frames), bf16),
        rf_acc=vm((n_t, rows, D), f32), rf_buf=vm((z, rows, D), bf16),
        glu=vm(edge_shape, f32), bhat=vm(edge_shape, f32), dbn=vm(edge_shape, f32),
        val=vm((n_t, rows, w), f32), sig=vm((n_t, rows, w), f32), act=vm((n_t, rows, w), bf16),
        de=vm((rows, 2 * w), bf16), sums=vm((2, 2 * n_t, w), f32), sum_mid=vm((2, 2 * n_t, w), f32),
        sum_out=vm((2, 2 * n_t, w), f32), sum_buf=vm((2, n_dp - 1, 2 * n_t, w), f32),
        sum_z=vm((2, z, 2 * n_t, w), f32), core_buf=vm((CHUNKS, groups, rows_w, hidden), bf16),
        dp_buf=vm((CHUNKS, 2, groups - 1, rows_w, hidden // 2), bf16), z_buf=vm((CHUNKS, z, rows_w, width), bf16),
        small=vm((n_bits + 1, n_t, tap_rows, w), f32), small_buf=vm((n_bits, n_t, tap_rows, w), f32),
        small_z=vm((z, tap_rows, w), f32), gsum=vm((n_bits + 1, 8, D), f32), gsum_buf=vm((n_bits, 8, D), f32),
        gsum_z=vm((z, 8, D), f32), local_sem=sem((CHUNKS,)))
    scratch.update(
        z_send=sem((CHUNKS, z)), z_recv=sem((CHUNKS, z)),
        d_send=sem((CHUNKS, 2, n_dp - 1)), d_recv=sem((CHUNKS, 2, n_dp - 1)),
        f_send=sem((z,)), f_recv=sem((z,)),
        e_send=sem((n_e,)), e_recv=sem((n_e,)),
        a_send=sem((z,)), a_recv=sem((z,)),
        edge_send=sem((3, 2)), edge_recv=sem((3, 2)),
        sum_send=sem((2, n_dp - 1)), sum_recv=sem((2, n_dp - 1)),
        sumz_send=sem((2, z)), sumz_recv=sem((2, z)),
        core_send=sem((CHUNKS, groups)), core_recv=sem((CHUNKS, groups)),
        fd_send=sem((CHUNKS, 2, groups - 1)), fd_recv=sem((CHUNKS, 2, groups - 1)),
        fz_send=sem((CHUNKS, z)), fz_recv=sem((CHUNKS, z)),
        rf_ss=sem((z,)), rf_rs=sem((z,)),
        s_send=sem((n_bits,)), s_recv=sem((n_bits,)),
        sz_send=sem((z,)), sz_recv=sem((z,)),
        g_send=sem((n_bits,)), g_recv=sem((n_bits,)),
        gz_send=sem((z,)), gz_recv=sem((z,)))
    names = list(inputs) + list(outs) + list(scratch)
    vmem = pl.BlockSpec(memory_space=pltpu.VMEM)
    result = pl.pallas_call(
        functools.partial(layer_body, names, n_dp, n_t, head_dim),
        name="layer",
        out_shape=tuple(jax.ShapeDtypeStruct(dims, kind) for dims, kind in outs.values()),
        in_specs=[vmem] * len(inputs),
        out_specs=(vmem,) * len(outs),
        scratch_shapes=list(scratch.values()),
        compiler_params=pltpu.CompilerParams(collective_id=0, has_side_effects=True, vmem_limit_bytes=67043328),
    )(*inputs.values())
    return SimpleNamespace(**dict(zip(outs, result)))


def angle_tables(frames, width):
    step = 32
    frequency = np.exp(np.arange(width // 2) * (-2.0 * math.log(10000.0) / width))
    coarse = np.arange(frames // step)[:, None] * step * frequency
    fine = np.arange(step)[:, None] * frequency
    return jnp.asarray(np.stack([np.sin(coarse), np.cos(coarse), np.sin(fine), np.cos(fine)]), f32)


def per_device(n_dp, n_t, inputs, out_grad, norm_gains, first_up, first_down, attend_in, attend_out, position_bias,
               convolve_in, depth_kernel, batch_norm, convolve_out, second_up, second_down):
    rows, D = inputs.shape
    w = attend_in.shape[2]
    R = attend_in.shape[1]
    n_bias = position_bias.shape[2]
    local_heads = position_bias.shape[1]
    head_dim = n_bias * n_dp
    n_gain = norm_gains.shape[1]
    d = lax.axis_index("dp")
    gain_in = jnp.concatenate([norm_gains, position_bias.astype(f32).reshape(2, local_heads * n_bias),
                               jnp.zeros((1, n_gain), f32)])
    tap_in = jnp.concatenate([depth_kernel.T, batch_norm, jnp.zeros((7, w), f32)], axis=0)
    got = layer_kernel(n_dp, n_t, head_dim, dict(
        fu=first_up, fd=first_down, at=attend_in, cw=convolve_in.reshape(R, 2 * w), ao=attend_out,
        co=convolve_out, su=second_up, sd=second_down, gain_in=gain_in, tap_in=tap_in, x=inputs,
        og=out_grad, tab=angle_tables(rows * n_t, D)))
    shards, small = got.shards, got.small_out
    grad_bias = small[KERNEL:KERNEL + 2].reshape(2, local_heads, head_dim)
    grad_bias = lax.dynamic_slice_in_dim(grad_bias, d * n_bias, n_bias, 2)
    return (
        got.out, got.dx0, got.gain_out[:5],
        shards[0], shards[1].T, shards[2].reshape(R, 4, w).transpose(1, 0, 2), shards[3][:, 2 * w:3 * w].T, grad_bias,
        shards[3][:, :2 * w].reshape(R, 2, w), small[:KERNEL].T, got.bn_out,
        shards[3][:, 3 * w:].T, shards[4], shards[5].T)


def solution(mesh):
    n_dp, n_t = mesh.shape["dp"], mesh.shape["tensor"]
    row = P(("dp", "tensor"), None)
    gain = P(None, ("dp", "tensor"))
    up = P("dp", "tensor")
    down = P("tensor", "dp")
    weights = (up, down, P(None, "dp", "tensor"), down, P(None, "tensor", "dp"), P("dp", None, "tensor"),
               P("tensor", None), P(None, "tensor"), down, up, down)
    return jax.shard_map(
        functools.partial(per_device, n_dp, n_t), mesh=mesh,
        in_specs=(row, row, gain) + weights,
        out_specs=(row, row, gain) + weights,
        check_vma=False)
```

```python
import functools
import math
from types import SimpleNamespace

import jax
import jax.numpy as jnp
import numpy as np
from jax import lax
from jax.experimental import pallas as pl
from jax.experimental.pallas import tpu as pltpu
from jax.sharding import PartitionSpec as P

MESH = pl.DeviceIdType.MESH
CHUNKS = 6
CUTS = 2
AHEAD = 2
CORE = 1
EDGE = 16
KERNEL = 31
HALF = KERNEL // 2
norm_eps = 1e-05
f32 = jnp.float32
bf16 = jnp.bfloat16
high = lax.Precision.HIGHEST


def flip(index, mask):
    result = index
    bit = 1
    while bit <= mask:
        if mask & bit:
            result = result + bit - 2 * bit * ((index // bit) % 2)
        bit *= 2
    return result


def span(bits):
    masks = [0]
    for bit in bits:
        masks = masks + [mask ^ bit for mask in masks]
    return masks


def link_orders(n_dp):
    bits = [1 << k for k in range(1, n_dp.bit_length() - 1)]
    return (bits, bits[::-1])


def greet(peers):
    barrier = pltpu.get_barrier_semaphore()
    for peer in peers:
        pl.semaphore_signal(barrier, inc=1, device_id=peer, device_id_type=MESH)
    pl.semaphore_wait(barrier, len(peers))


def remote(src, dst, send_sem, recv_sem, peer):
    return pltpu.make_async_remote_copy(
        src_ref=src, dst_ref=dst, send_sem=send_sem, recv_sem=recv_sem,
        device_id=peer, device_id_type=MESH)


def start_all(copies):
    for copy in copies:
        copy.start()


def settled(ref, sem, peer):
    remote(ref, ref, sem, sem, peer).wait_recv()


def arrive_all(copies):
    for copy in copies:
        copy.wait_recv()


def sent_all(copies):
    for copy in copies:
        copy.wait_send()


def dot(left, right, left_dim, right_dim):
    return lax.dot_general(left, right, (((left_dim,), (right_dim,)), ((), ())), preferred_element_type=f32)


def turned(value):
    return value.astype(f32).T.astype(bf16)


def head_mask(shape, axis, head_dim, head):
    place = lax.broadcasted_iota(jnp.int32, shape, axis)
    return (place >= head * head_dim) & (place < (head + 1) * head_dim)


def keep(mask, value):
    return jnp.where(mask, value, jnp.zeros_like(value))


def block_of(k, size):
    return pl.ds(pl.multiple_of(k * size, size), size)


def loop(count, body):
    def step(k, carry):
        body(k)
        return carry
    lax.fori_loop(0, count, step, 0)


def row_loop(rows, size, body):
    loop(rows // size, lambda k: body(block_of(k, size)))


def sigmoid(values):
    return 1.0 / (1.0 + jnp.exp(-values))


def norm_parts(values):
    centred = values - jnp.mean(values, axis=-1, keepdims=True)
    inverse = lax.rsqrt(jnp.mean(centred * centred, axis=-1, keepdims=True) + norm_eps)
    return centred * inverse, inverse


def norm_back(value, incoming, gain_row):
    scaled, inverse = norm_parts(value)
    grad_scaled = incoming * gain_row
    inner = jnp.mean(grad_scaled * scaled, axis=-1, keepdims=True)
    grad_in = inverse * (grad_scaled - jnp.mean(grad_scaled, axis=-1, keepdims=True) - scaled * inner)
    return scaled, grad_in, jnp.sum(incoming * scaled, axis=0, keepdims=True)


def tail_plan(final):
    parts = range(CUTS)
    plan = [((2, part), 1) for part in parts] + [((0, part), 0) for part in parts]
    for stage in range(1, final):
        plan += [((1, part), stage) for part in parts]
        if stage + 1 < final:
            plan += [((2, part), stage + 1) for part in parts]
        plan += [((0, part), stage) for part in parts]
    return plan + [((c, part), final) for c in (4, 5, 3, 2, 1, 0) for part in parts]


def relay_order(stages):
    hop, link_free, order = 1.5, 0.0, []
    units = [(c, part) for c in range(CHUNKS) for part in range(CUTS)]
    waiting = [(7.0 + 6.5 / CUTS * (k + 1), 0, u) for k, u in enumerate(units)]
    while waiting:
        waiting.sort()
        now, stage, u = waiting.pop(0)
        order.append((now, stage, u))
        if stage < stages - 1:
            link_free = max(now, link_free) + 3.1 / CUTS * 2 ** stage
            waiting.append((link_free + hop, stage + 1, u))
        elif stage == stages - 1:
            waiting.append((now + hop + 2.0 / CUTS, stages, u))
    return order


SLAB = 512
HBM = "_hbm"


def feed_rows(a_ref, up, down_t, z_ref, hidden, slope):
    z_ref[...] = jnp.zeros_like(z_ref)

    def step(k):
        cols = block_of(k, SLAB)
        pre = dot(a_ref[...], up[:, cols], 1, 0)
        sig = sigmoid(pre)
        hidden[:, cols] = (pre * sig).astype(bf16)
        slope[:, cols] = (sig * (1.0 + pre * (1.0 - sig))).astype(bf16)
        z_ref[...] = z_ref[...] + dot(hidden[:, cols], down_t[:, cols], 1, 1)
    loop(up.shape[1] // SLAB, step)


def feed_back(dz_ref, dz_turn, a_turn, up, down_t, z_ref, hidden, slope, g_up, g_down, start_down, middle):
    z_ref[...] = jnp.zeros_like(z_ref)

    def first_step(k):
        cols = block_of(k, SLAB)
        g_down[:, cols] = dot(dz_turn[...], hidden[:, cols], 1, 0).astype(bf16)
    loop(up.shape[1] // SLAB, first_step)
    start_down()
    slabs = up.shape[1] // SLAB

    def step(k):
        cols = block_of(k, SLAB)
        grad_pre = (dot(dz_ref[...], down_t[:, cols], 1, 0) * slope[:, cols].astype(f32)).astype(bf16)
        g_up[:, cols] = dot(a_turn[...], grad_pre, 1, 0).astype(bf16)
        z_ref[...] = z_ref[...] + dot(grad_pre, up[:, cols], 1, 1)
    loop(slabs - 1, step)
    middle()
    step(slabs - 1)


def layer_body(names, n_dp, n_t, head_dim, *all_refs):
    r = SimpleNamespace(**dict(zip(names, all_refs)))
    d = lax.axis_index("dp")
    t = lax.axis_index("tensor")
    pack, wbuf, gbuf = r.pack, r.wbuf, r.gbuf
    x_ref, gains, taps = r.x, r.gains, r.taps
    rows_w, width = pack.shape[1], pack.shape[2]
    rows, D = x_ref.shape
    w = D // n_t
    half = n_t * width // 2
    frames = rows * n_t
    local_heads = w // head_dim
    n_gain = r.gain_in.shape[1]
    n_bias = n_gain // local_heads
    row_count = frames * n_dp
    scale = head_dim ** -0.5
    links = link_orders(n_dp)
    orders = [order + [CORE] for order in links]
    stages = len(orders[0])
    n_link = len(links[0])
    z_peers = [(d, lax.rem(t + step, n_t)) for step in range(1, n_t)]
    d_peers = [(flip(d, mask), t) for mask in range(1, n_dp)]
    before = (d, lax.rem(t + n_t - 1, n_t))
    after = (d, lax.rem(t + 1, n_t))
    z_range = range(n_t - 1)
    leaving = [name for name in names if name.endswith(HBM)]

    def leave(*chosen):
        for ref in chosen:
            name = [one for one in leaving if getattr(r, one[:-len(HBM)]) is ref][0]
            k = leaving.index(name)
            pltpu.make_async_copy(ref, getattr(r, name), r.out_sem.at[k]).start()

    greet(z_peers + d_peers)

    def window(u, mask, start, size):
        c, part = u
        count = rows_w // CUTS
        first = pl.multiple_of(flip(d, mask) * rows_w + part * count, count)
        return wbuf.at[c, pl.ds(first, count), pl.ds(start, size)]

    def own(u):
        return window(u, 0, pl.multiple_of(t * width, width), width)

    def source(u):
        count = rows_w // CUTS
        return sources[u[0]].at[pl.ds(u[1] * count, count), :]

    sources = (r.fu, r.fd, pack.at[0], pack.at[1], r.su, r.sd)

    def z_copies(u):
        return [remote(source(u), own(u), r.z_send.at[0], r.z_recv.at[u[0], u[1]], z_peers[k])
                for k in z_range]

    def local_copy(u):
        return pltpu.make_async_copy(source(u), own(u), r.local_sem.at[u[0], u[1]])

    def dp_copies(u, stage):
        copies = []
        for h in range(2):
            bit = orders[h][stage]
            masks = span(orders[h][:stage])
            for mask in masks:
                part = window(u, mask, h * half, half)
                copies.append(remote(part, part, r.d_send.at[u[0]], r.d_recv.at[u[0], u[1], stage],
                                     (flip(d, bit), t)))
        return copies

    def send_unit(u):
        local_copy(u).start()
        start_all(z_copies(u))

    def allowed(done):
        return AHEAD + done + max(0, done - 3)

    queue = [(c, part) for c in range(CHUNKS) for part in range(CUTS)]

    e_acc, e_buf = r.e_acc, r.e_buf

    def e_copies(first, stop):
        copies = []
        for k in range(first, stop):
            if k < n_t - 1:
                source, peer = e_acc.at[0], z_peers[k]
            else:
                source, peer = e_acc.at[k - n_t + 2], (flip(d, orders[0][k - n_t + 1]), t)
            sem = max(0, k - n_t + 2)
            copies.append(remote(source, e_buf.at[k], r.e_send.at[sem], r.e_recv.at[sem], peer))
        return copies

    taps_own = r.taps_own
    tap_copies = [remote(taps_own, taps.at[t], r.f_send.at[0], r.f_recv.at[0], z_peers[k]) for k in z_range]

    entry = lax.broadcasted_iota(jnp.int32, (n_gain, D), 0)
    lane = lax.broadcasted_iota(jnp.int32, (n_gain, D), 1)
    gain_spot = (lane == (d * n_t + t) * n_gain + entry).astype(f32)
    e_acc[0] = jnp.zeros_like(e_acc[0])
    e_acc[0, 0:5, :] = jnp.dot(r.gain_in[...], gain_spot, precision=high, preferred_element_type=f32)
    entry_b = lax.broadcasted_iota(jnp.int32, (n_bias, D), 0)
    lane_b = lax.broadcasted_iota(jnp.int32, (n_bias, D), 1)
    bias_spots = [(lane_b == entry_b + d * n_bias + (h + t * local_heads) * head_dim).astype(f32)
                  for h in range(local_heads)]
    for pair in range(2):
        row = None
        for h in range(local_heads):
            term = jnp.dot(r.bias_in[pair, h:h + 1, :].astype(f32), bias_spots[h], precision=high,
                           preferred_element_type=f32)
            row = term if row is None else row + term
        e_acc[0, 5 + pair:6 + pair, :] = row
    start_all(e_copies(0, n_t - 1))
    for u in queue[:AHEAD]:
        send_unit(u)
    for k in range(4):
        pack[0, :, k * w:(k + 1) * w] = r.at[k]
    for k in range(2):
        pack[1, :, k * w:(k + 1) * w] = r.cw[:, k, :]
    pack[1, :, 2 * w:3 * w] = r.ao[...]
    pack[1, :, 3 * w:4 * w] = r.co[...]
    taps_own[...] = jnp.zeros_like(taps_own)
    taps_own[0:KERNEL, :] = r.tap_in[...]
    taps_own[KERNEL:KERNEL + 2, :] = r.bn_in[...]
    start_all(tap_copies)
    taps[t] = taps_own[...]

    def relay(stage, u):
        count = rows_w // CUTS
        if stage == 0:
            local_copy(u).wait()
            settled(wbuf.at[0, pl.ds(0, count), pl.ds(0, (n_t - 1) * width)], r.z_recv.at[u[0], u[1]], before)
            place = queue.index(u)
            for other in queue[allowed(place):allowed(place + 1)]:
                send_unit(other)
        else:
            settled(wbuf.at[0, pl.ds(0, count * 2 ** (stage - 1)), :], r.d_recv.at[u[0], u[1], stage - 1], before)
        if stage < stages:
            start_all(dp_copies(u, stage))

    def ready_after(order, chunks):
        places = [k + 1 for k, (_, stage, u) in enumerate(order) if stage == stages and u[0] in chunks]
        return max(places, default=0)

    e_step = [0]

    def e_next():
        k = e_step[0]
        if k == 0:
            settled(e_buf.at[pl.ds(0, n_t - 1)], r.e_recv.at[0], before)
            total = e_acc[0]
            for i in z_range:
                total = total + e_buf[i]
            e_acc[1] = total
        elif k <= n_link + 1:
            arrive_all(e_copies(n_t - 2 + k, n_t - 1 + k))
            e_acc[k + 1] = e_acc[k] + e_buf[n_t - 2 + k]
        if k <= n_link:
            start_all(e_copies(n_t - 1 + k, n_t + k))
        e_step[0] = k + 1

    tab, phase, spin = r.tab, r.phase, r.spin
    step_t = tab.shape[1]

    def table(k):
        cs, cc = tab[0, pl.ds(k, 1), :], tab[1, pl.ds(k, 1), :]
        part = block_of(k, step_t)
        phase[part, 0:D // 2] = (cs * tab[3] + cc * tab[2]).astype(bf16)
        phase[part, D // 2:D] = (cc * tab[3] - cs * tab[2]).astype(bf16)
    loop(frames // step_t, table)

    def own_table(k):
        place = t * (rows // step_t) + k
        cs, cc = tab[0, pl.ds(place, 1), :], tab[1, pl.ds(place, 1), :]
        part = block_of(k, step_t)
        spin[0, part, :] = cs * tab[3] + cc * tab[2]
        spin[1, part, :] = cc * tab[3] - cs * tab[2]
    loop(rows // step_t, own_table)

    def spun(sines, cosines):
        u_s = r.u_s
        u_s[:, 0:D // 2] = (cosines * spin[0] - sines * spin[1]).astype(bf16)
        u_s[:, D // 2:D] = (sines * spin[0] + cosines * spin[1]).astype(bf16)

    z_s, a1, a2, a2_all = r.z_s, r.a1, r.a2, r.a2_all
    x1, x2, x3 = r.x1, r.x2, r.x3
    events = relay_order(stages)
    ready = ready_after(events, (0, 1))
    for k, (_, stage, u) in enumerate(events[:ready]):
        relay(stage, u)
        if k % 4 == 3 and e_step[0] < n_link + 2:
            e_next()
    while e_step[0] < n_link + 2:
        e_next()
    gains[...] = e_acc[n_link + 2]

    def norm_one(part):
        a1[part, :] = (norm_parts(x_ref[part, :].astype(f32))[0] * gains[0:1, :]).astype(bf16)
    row_loop(rows, 64, norm_one)
    feed_rows(a1, wbuf.at[0], wbuf.at[1], z_s, r.hid1, r.slope1)

    def norm_two(part):
        value = x_ref[part, :].astype(f32) + 0.5 * z_s[part, :]
        x1[part, :] = value
        a2[part, :] = (norm_parts(value)[0] * gains[1:2, :]).astype(bf16)
    row_loop(rows, 64, norm_two)

    a_copies = [remote(a2, a2_all.at[t], r.a_send.at[0], r.a_recv.at[0], z_peers[k]) for k in z_range]
    start_all(a_copies)
    a2_all[t] = a2[...]
    for _, stage, u in events[ready:]:
        relay(stage, u)
    settled(a2_all.at[pl.ds(0, n_t - 1)], r.a_recv.at[0], before)
    kv, cq, pq, probs, mix, s_s, u_s = r.kv, r.cq, r.pq, r.probs, r.mix, r.s_s, r.u_s
    z_s[...] = jnp.zeros_like(z_s)
    inv_s = r.inv_s
    scale_low = jnp.asarray(scale, bf16)

    def head_group(j):
        cols = block_of(j, width)
        block = wbuf[2, :, cols]
        for part in range(n_t):
            kv[j, part * rows:(part + 1) * rows, :] = dot(a2_all[part], block[:, w:3 * w], 1, 0).astype(bf16)
        q = dot(a2[...], block[:, 0:w], 1, 0)
        if w % 128 == 0:
            bias = gains[5:7, block_of(j, w)]
        else:
            bias = gains[5:7, 0:w]
            for other in range(1, n_t):
                bias = jnp.where(j == other, gains[5:7, other * w:(other + 1) * w], bias)
        cq_j = (q + bias[0:1]).astype(bf16)
        pq_j = (q + bias[1:2]).astype(bf16)
        cq[j] = cq_j
        pq[j] = pq_j
        for h in range(local_heads):
            mask = head_mask((rows, w), 1, head_dim, h)
            spread = dot(keep(mask, pq_j), block[:, 3 * w:4 * w], 1, 1)
            spun(spread[:, :D // 2] * scale, spread[:, D // 2:] * scale)
            s_s[...] = dot(u_s[...], phase[...], 1, 1) + dot(keep(mask, cq_j) * scale_low, kv[j, :, 0:w], 1, 1)
            head = j * local_heads + h

            s = s_s[...]
            e = jnp.exp(s - jnp.max(s, axis=-1, keepdims=True))
            inv = 1.0 / jnp.sum(e, axis=-1, keepdims=True)
            probs[head] = e.astype(bf16)
            mixed = dot(probs[head], kv[j, :, w:2 * w], 1, 0) * inv
            inv = jnp.broadcast_to(inv, (rows, w))
            inverse = inv if h == 0 else jnp.where(mask, inv, inverse)
            mixture = mixed if h == 0 else jnp.where(mask, mixed, mixture)
        mix[j] = mixture
        inv_s[j] = inverse
        z_s[...] = z_s[...] + dot(mixture.astype(bf16), wbuf[3, :, cols][:, 2 * w:3 * w], 1, 1)
    loop(n_t, head_group)

    a3, glu, bhat, val, sig, act = r.a3, r.glu, r.bhat, r.val, r.sig, r.act
    dbn, sums, sum_buf, sum_mid, sum_z = r.dbn, r.sums, r.sum_buf, r.sum_mid, r.sum_z
    inner = pl.ds(EDGE, rows)

    def norm_three(part):
        value = x1[part, :] + z_s[part, :]
        x2[part, :] = value
        a3[part, :] = (norm_parts(value)[0] * gains[2:3, :]).astype(bf16)
    row_loop(rows, 64, norm_three)

    def gate(j):
        block = wbuf[3, :, block_of(j, width)]
        e = dot(a3[...], block[:, 0:2 * w], 1, 0)
        sig_j = sigmoid(e[:, w:2 * w])
        val[j] = e[:, 0:w]
        sig[j] = sig_j
        glu[j, inner, :] = e[:, 0:w] * sig_j
    loop(n_t, gate)

    def edge_copies(ref, k):
        first, last = pl.ds(EDGE, EDGE), pl.ds(rows, EDGE)
        return [remote(ref.at[:, first, :], ref.at[:, pl.ds(EDGE + rows, EDGE), :], r.edge_send.at[k, 0],
                       r.edge_recv.at[k, 0], before),
                remote(ref.at[:, last, :], ref.at[:, pl.ds(0, EDGE), :], r.edge_send.at[k, 1],
                       r.edge_recv.at[k, 1], after)]

    def edge_start(ref, k):
        back, ahead = edge_copies(ref, k)

        @pl.when(t > 0)
        def _():
            back.start()

        @pl.when(t < n_t - 1)
        def _():
            ahead.start()

        @pl.when(t == 0)
        def _():
            ref[:, pl.ds(0, EDGE), :] = jnp.zeros((n_t, EDGE, w), f32)

        @pl.when(t == n_t - 1)
        def _():
            ref[:, pl.ds(EDGE + rows, EDGE), :] = jnp.zeros((n_t, EDGE, w), f32)

    def edge_wait(ref, k):
        back, ahead = edge_copies(ref, k)

        @pl.when(t > 0)
        def _():
            ahead.wait_recv()
            back.wait_send()

        @pl.when(t < n_t - 1)
        def _():
            back.wait_recv()
            ahead.wait_send()

    def sum_copies(k):
        return [remote(sums.at[k], sum_buf.at[k, i], r.sum_send.at[k], r.sum_recv.at[k], d_peers[i])
                for i in range(n_dp - 1)]

    def sum_z_copies(k):
        return [remote(sum_mid.at[k], sum_z.at[k, i], r.sumz_send.at[k], r.sumz_recv.at[k], z_peers[i])
                for i in z_range]

    def sum_middle(k):
        settled(sum_buf.at[k], r.sum_recv.at[k], before)
        total = sums[k]
        for i in range(n_dp - 1):
            total = total + sum_buf[k, i]
        sum_mid[k] = total
        start_all(sum_z_copies(k))

    def sum_end(k):
        settled(sum_z.at[k], r.sumz_recv.at[k], before)
        total = sum_mid[k]
        for i in z_range:
            total = total + sum_z[k, i]
        sum_mid_out = r.sum_out
        sum_mid_out[k] = total

    edge_start(glu, 0)
    settled(taps.at[pl.ds(0, n_t - 1)], r.f_recv.at[0], before)
    edge_wait(glu, 0)
    size = 64

    def sweep(ref, j, first, backward):
        total = None
        for k in range(KERNEL):
            offset = EDGE - HALF + (KERNEL - 1 - k if backward else k)
            term = taps[j, k:k + 1, :] * ref[j, pl.ds(first + offset, size), :]
            total = term if total is None else total + term
        return total

    def convolve(j):
        def part_step(k, carry):
            first = pl.multiple_of(k * size, size)
            value = sweep(glu, j, first, False)
            bhat[j, pl.ds(first + EDGE, size), :] = value
            return (carry[0] + jnp.sum(value, axis=0, keepdims=True),
                    carry[1] + jnp.sum(value * value, axis=0, keepdims=True))
        zero = jnp.zeros((1, w), f32)
        one, two = lax.fori_loop(0, rows // size, part_step, (zero, zero))
        sums[0, pl.ds(2 * j, 1), :] = one
        sums[0, pl.ds(2 * j + 1, 1), :] = two
    loop(n_t, convolve)
    start_all(sum_copies(0))
    sum_middle(0)
    sum_end(0)

    def bn_parts(j):
        mean = r.sum_out[0, pl.ds(2 * j, 1), :] / row_count
        square = r.sum_out[0, pl.ds(2 * j + 1, 1), :] / row_count
        return mean, lax.rsqrt(square - mean * mean + norm_eps), taps[j, KERNEL:KERNEL + 1, :], taps[
            j, KERNEL + 1:KERNEL + 2, :]

    z_s[...] = jnp.zeros_like(z_s)

    def activate(j):
        mean, inverse, bn_gain, bn_shift = bn_parts(j)
        scaled = (bhat[j, inner, :] - mean) * inverse
        bhat[j, inner, :] = scaled
        normal = scaled * bn_gain + bn_shift
        act[j] = (normal * sigmoid(normal)).astype(bf16)
        z_s[...] = z_s[...] + dot(act[j], wbuf[3, :, block_of(j, width)][:, 3 * w:4 * w], 1, 1)
    loop(n_t, activate)
    edge_start(bhat, 1)

    a4, dx = r.a4, r.dx0

    def norm_four(part):
        value = x2[part, :] + z_s[part, :]
        x3[part, :] = value
        a4[part, :] = (norm_parts(value)[0] * gains[3:4, :]).astype(bf16)
    row_loop(rows, 64, norm_four)
    feed_rows(a4, wbuf.at[4], wbuf.at[5], z_s, r.hid2, r.slope2)
    gsum = r.gsum
    gsum[0] = jnp.zeros_like(gsum[0])
    dz, dz_turn, a_turn = r.dz, r.dz_turn, r.a_turn

    def add_gain(row, part_sum):
        gsum[0, row:row + 1, :] = gsum[0, row:row + 1, :] + part_sum

    def norm_five(part):
        value = x3[part, :] + 0.5 * z_s[part, :]
        scaled, grad_in, part_sum = norm_back(value, r.og[part, :].astype(f32), gains[4:5, :])
        r.out[part, :] = scaled * gains[4:5, :]
        dx[part, :] = grad_in
        dz[part, :] = (0.5 * grad_in).astype(bf16)
        add_gain(4, part_sum)
    row_loop(rows, 64, norm_five)
    leave(r.out)

    def grad_chunk(c):
        return gbuf.at[c - 2] if c >= 2 else wbuf.at[c + 4]

    def join_norm(row, x_of, factor):
        def step(part):
            _, grad_in, part_sum = norm_back(x_of(part), z_s[part, :], gains[row:row + 1, :])
            value = dx[part, :] + grad_in
            dx[part, :] = value
            dz[part, :] = (factor * value).astype(bf16)
            add_gain(row, part_sum)
        row_loop(rows, 64, step)

    folds = [order[::-1] for order in links]
    groups = span(links[0])
    core_buf, dp_buf, z_buf = r.core_buf, r.dp_buf, r.z_buf

    def grad_rows(u, mask):
        c, part = u
        count = rows_w // CUTS
        return grad_chunk(c).at[pl.ds(pl.multiple_of(flip(d, mask) * rows_w + part * count, count), count), :]

    def part_rows(part):
        return pl.ds(part * (rows_w // CUTS), rows_w // CUTS)

    def core_copies(u):
        return [remote(grad_rows(u, mask ^ CORE), core_buf.at[u[0], k, part_rows(u[1])],
                       r.core_send.at[0], r.core_recv.at[u[0], u[1]],
                       (flip(d, CORE), t)) for k, mask in enumerate(groups)]

    def fold_places(stage):
        places = []
        for h in range(2):
            masks = span(folds[h][stage + 1:])
            base = len(groups) - 2 * len(masks)
            places += [(mask, h, base + j) for j, mask in enumerate(masks)]
        return places

    def fold_copies(u, stage):
        c, part = u
        return [remote(grad_rows(u, mask ^ folds[h][stage]).at[:, pl.ds(h * half, half)],
                       dp_buf.at[c, h, slot, part_rows(part)],
                       r.fd_send.at[c], r.fd_recv.at[c, part, stage], (flip(d, folds[h][stage]), t))
                for mask, h, slot in fold_places(stage)]

    def fold_z_copies(u):
        c, part = u
        copies = []
        for k in z_range:
            target = lax.rem(t + k + 1, n_t)
            place = grad_rows(u, 0).at[:, pl.ds(pl.multiple_of(target * width, width), width)]
            copies.append(remote(place, z_buf.at[c, k, part_rows(part)], r.fz_send.at[0],
                                 r.fz_recv.at[c, part], z_peers[k]))
        return copies

    piece = 16
    per_part = rows_w // CUTS // piece

    def fold_start(c):
        for part in range(CUTS):
            start_all(core_copies((c, part)))

    def fold_step(c, stage, go=True):
        for part in range(CUTS):
            fold_unit((c, part), stage, go)

    def fold_send(c):
        for part in range(CUTS):
            start_all(fold_z_copies((c, part)))

    def fold_unit(u, stage, go=True):
        c, cut = u
        ref = grad_chunk(c)
        if stage == 0:
            settled(core_buf.at[c, :, part_rows(cut)], r.core_recv.at[c, cut], before)
            for k, mask in enumerate(groups):
                base = flip(d, mask) * rows_w

                def add_core(step, k=k, base=base):
                    step = step + cut * per_part
                    part = pl.ds(pl.multiple_of(base + step * piece, piece), piece)
                    ref[part, :] = (ref[part, :].astype(f32)
                                    + core_buf[c, k, block_of(step, piece), :].astype(f32)).astype(bf16)
                loop(per_part, add_core)
        elif stage <= n_link:
            places = fold_places(stage - 1)
            first_slot, count = places[0][2], len(places) // 2
            settled(dp_buf.at[c, :, pl.ds(first_slot, count), part_rows(cut)], r.fd_recv.at[c, cut, stage - 1], before)
            for mask, h, slot in places:
                base = flip(d, mask) * rows_w
                cols = pl.ds(h * half, half)

                def add_dp(step, base=base, cols=cols, h=h, slot=slot):
                    step = step + cut * per_part
                    part = pl.ds(pl.multiple_of(base + step * piece, piece), piece)
                    ref[part, cols] = (ref[part, cols].astype(f32)
                                       + dp_buf[c, h, slot, block_of(step, piece), :].astype(f32)).astype(bf16)
                loop(per_part, add_dp)
        else:
            settled(z_buf.at[c, :, part_rows(cut)], r.fz_recv.at[c, cut], before)

            def finish(step):
                step = step + cut * per_part
                part = pl.ds(pl.multiple_of(d * rows_w + step * piece, piece), piece)
                total = ref[part, block_of(t, width)].astype(f32)
                for k in z_range:
                    total = total + z_buf[c, k, block_of(step, piece), :].astype(f32)
                here = block_of(step, piece)
                if c == 2:
                    for k in range(4):
                        r.g_at[k, here, :] = total[:, k * w:(k + 1) * w]
                elif c == 3:
                    for k in range(2):
                        r.g_cw[here, k, :] = total[:, k * w:(k + 1) * w]
                    r.g_ao[here, :] = total[:, 2 * w:3 * w]
                    r.g_co[here, :] = total[:, 3 * w:4 * w]
                else:
                    grads[c][here, :] = total
            loop(per_part, finish)
            if cut == CUTS - 1:
                leave(*((r.g_at,) if c == 2 else (r.g_cw, r.g_ao, r.g_co) if c == 3 else (grads[c],)))
        if stage < n_link and go:
            start_all(fold_copies(u, stage))
        elif stage == n_link and go:
            start_all(fold_z_copies(u))

    grads = {0: r.g_fu, 1: r.g_fd, 4: r.g_su, 5: r.g_sd}
    final = n_link + 1
    fold_plan_one = [[(4, 1)], [], [(3, 0)]]
    fold_plan_two = []
    for stage in range(2, n_link + 1):
        fold_plan_two += [[(4, stage)], [(3, stage - 1)]]
    fold_plan_two += [[], [(3, n_link)]]

    dz_turn[...] = turned(dz[...])
    a_turn[...] = turned(a4[...])
    units = [(c, part) for c in range(CHUNKS) for part in range(CUTS)]
    settled(wbuf.at[0, pl.ds(0, CHUNKS * rows_w), pl.ds(0, (n_t - 1) * width)], r.z_send.at[0], before)
    for c in range(CHUNKS):
        settled(wbuf.at[0, pl.ds(0, (n_dp - 1) * rows_w), :], r.d_send.at[c], before)
    feed_back(dz, dz_turn, a_turn, wbuf.at[4], wbuf.at[5], z_s, r.hid2, r.slope2, grad_chunk(4), grad_chunk(5),
              lambda: fold_start(5), lambda: None)
    fold_start(4)
    join_norm(3, lambda part: x3[part, :], 1.0)

    dz_turn[...] = turned(dz[...])

    def act_back(j):
        mean, inverse, bn_gain, bn_shift = bn_parts(j)
        grad_act = dot(dz[...], wbuf[3, :, block_of(j, width)][:, 3 * w:4 * w], 1, 0)
        scaled = bhat[j, inner, :]
        normal = scaled * bn_gain + bn_shift
        sig_n = sigmoid(normal)
        value = grad_act * (sig_n * (1.0 + normal * (1.0 - sig_n)))
        dbn[j, inner, :] = value
        sums[1, pl.ds(2 * j, 1), :] = jnp.sum(value * scaled, axis=0, keepdims=True)
        sums[1, pl.ds(2 * j + 1, 1), :] = jnp.sum(value, axis=0, keepdims=True)
    loop(n_t, act_back)
    start_all(sum_copies(1))
    edge_start(dbn, 2)
    fold_step(5, 0)
    sum_middle(1)
    fold_step(4, 0, False)
    a_turn[...] = turned(a3[...])
    sum_end(1)
    for k, ref in ((1, bhat), (2, dbn)):
        edge_wait(ref, k)
    r.g_bn[...] = r.sum_out[1, pl.ds(2 * t, 2), :]
    leave(r.g_bn)
    small = r.small
    z_s[...] = jnp.zeros_like(z_s)

    def put_grad(c, j, first, value):
        if w % 128 == 0:
            grad_chunk(c)[:, pl.ds(pl.multiple_of(j * width + first, 128), value.shape[1])] = value
        else:
            old = grad_chunk(c)[:, block_of(j, width)]
            pieces = [old[:, :first], value, old[:, first + value.shape[1]:]]
            grad_chunk(c)[:, block_of(j, width)] = jnp.concatenate([p for p in pieces if p.shape[1] > 0], axis=1)

    def conv_back(j):
        mean, inverse, bn_gain, bn_shift = bn_parts(j)
        gamma = r.sum_out[1, pl.ds(2 * j, 1), :] / row_count
        beta = r.sum_out[1, pl.ds(2 * j + 1, 1), :] / row_count
        dbn[j] = bn_gain * inverse * (dbn[j] - beta - bhat[j] * gamma)
        dbn[j, pl.ds(0, EDGE), :] = jnp.where(t > 0, dbn[j, pl.ds(0, EDGE), :], 0.0)
        tail = pl.ds(EDGE + rows, EDGE)
        dbn[j, tail, :] = jnp.where(t < n_t - 1, dbn[j, tail, :], 0.0)

        def tap_step(k, carry):
            first = pl.multiple_of(k * size, size)
            own_part = dbn[j, pl.ds(first + EDGE, size), :]
            result = []
            for tap in range(KERNEL):
                term = own_part * glu[j, pl.ds(first + EDGE - HALF + tap, size), :]
                result.append(carry[tap] + jnp.sum(term.reshape(size // 8, 8, w), axis=0))
            return tuple(result)
        tap_sums = lax.fori_loop(0, rows // size, tap_step, tuple(jnp.zeros((8, w), f32) for _ in range(KERNEL)))
        for tap in range(KERNEL):
            small[0, j, tap:tap + 1, :] = jnp.sum(tap_sums[tap], axis=0, keepdims=True)

        def spread_step(k):
            first = pl.multiple_of(k * size, size)
            part = pl.ds(first, size)
            dglu = sweep(dbn, j, first, True)
            sig_p = sig[j, part, :]
            grad_val = dglu * sig_p
            r.de[part, 0:w] = grad_val.astype(bf16)
            r.de[part, w:2 * w] = (grad_val * val[j, part, :] * (1.0 - sig_p)).astype(bf16)
        loop(rows // size, spread_step)
        put_grad(3, j, 0, dot(a_turn[...], r.de[...], 1, 0).astype(bf16))
        put_grad(3, j, 3 * w, dot(dz_turn[...], act[j], 1, 0).astype(bf16))
        z_s[...] = z_s[...] + dot(r.de[...], wbuf[3, :, block_of(j, width)][:, 0:2 * w], 1, 1)

        @pl.when(j == n_t // 2)
        def _():
            fold_step(5, 1)
            for part in range(CUTS):
                start_all(fold_copies((4, part), 0))
    loop(n_t, conv_back)
    join_norm(2, lambda part: x2[part, :], 1.0)

    dz_turn[...] = turned(dz[...])
    dmix_s, dmix_turn, cq_turn, dcq_s = r.dmix_s, r.dmix_turn, r.cq_turn, r.dcq_s
    a2_turn, rf_out, rf_buf, rf_z = r.a2_turn, r.rf_out, r.rf_buf, r.rf_z

    def mix_back(j):
        put_grad(3, j, 2 * w, dot(dz_turn[...], mix[j].astype(bf16), 1, 0).astype(bf16))
        dmix = dot(dz[...], wbuf[3, :, block_of(j, width)][:, 2 * w:3 * w], 1, 0) * inv_s[j]
        dmix_s[j] = dmix.astype(bf16)
        dmix_turn[j] = dmix.T.astype(bf16)
        cq_turn[j] = turned(cq[j])
        dcq_s[j] = jnp.zeros_like(dcq_s[j])
    loop(n_t, mix_back)
    for stage in range(2, n_link + 1):
        fold_step(5, stage)
    fold_start(3)
    rf_copies = [remote(rf_out.at[k], rf_buf.at[k], r.rf_ss.at[k], r.rf_rs.at[k], z_peers[k]) for k in z_range]

    def keys_back(part, j):
        block = wbuf[2, :, block_of(j, width)]
        piece_rows = block_of(part, rows)
        k_p, v_p = kv[j, piece_rows, :][:, 0:w], kv[j, piece_rows, :][:, w:2 * w]
        product = dmix_s[j].astype(f32) * mix[j]
        for h in range(local_heads):
            mask = head_mask((rows, w), 1, head_dim, h)
            turn_mask = head_mask((w, rows), 0, head_dim, h)
            head = j * local_heads + h
            delta = jnp.sum(keep(mask, product), axis=-1, keepdims=True)
            p_h = probs[head, :, piece_rows]
            grad_p = dot(keep(mask, dmix_s[j]), v_p, 1, 1)
            ds = (p_h.astype(f32) * (grad_p - delta)).astype(bf16)
            probs[head, :, piece_rows] = ds
            dv_h = dot(keep(turn_mask, dmix_turn[j]), p_h, 1, 0)
            dk_h = dot(keep(turn_mask, cq_turn[j]), ds, 1, 0)
            dcq_h = keep(mask, dot(ds, k_p, 1, 0))
            if h == 0:
                dv, dk, dcq = dv_h, dk_h, dcq_h
            else:
                dv, dk, dcq = dv + dv_h, dk + dk_h, dcq + dcq_h
        dcq_s[j] = dcq_s[j] + dcq
        dkv = jnp.concatenate([(dk * scale).T, dv.T], axis=1).astype(bf16)
        kv[j, piece_rows, :] = dkv
        rf_z[...] = rf_z[...] + dot(dkv, block[:, w:3 * w], 1, 1)

    assert len(fold_plan_one) <= n_t
    for k in range(n_t):
        rf_z[...] = jnp.zeros_like(rf_z)
        part = lax.rem(t + 1 + k, n_t)
        loop(n_t, functools.partial(keys_back, part))
        if k < n_t - 1:
            rf_out[k] = rf_z[...].astype(bf16)
            rf_copies[k].start()
        for c, stage in fold_plan_one[k] if k < len(fold_plan_one) else ():
            fold_step(c, stage)
    for part in range(n_t):
        a2_turn[:, part * rows:(part + 1) * rows] = turned(a2_all[part])
    small[0, :, KERNEL:, :] = jnp.zeros_like(small[0, :, KERNEL:, :])

    z_s[...] = jnp.zeros_like(z_s)

    def queries_back(j):
        block = wbuf[2, :, block_of(j, width)]
        pq_turn = turned(pq[j])
        for h in range(local_heads):
            mask = head_mask((rows, w), 1, head_dim, h)
            turn_mask = head_mask((w, rows), 0, head_dim, h)
            back = dot(probs[j * local_heads + h], phase[...], 1, 0)
            spun(back[:, :D // 2], back[:, D // 2:])
            dpq_h = keep(mask, dot(u_s[...], block[:, 3 * w:4 * w], 1, 0))
            pos_h = dot(keep(turn_mask, pq_turn), u_s[...], 1, 0)
            if h == 0:
                dpq, pos = dpq_h, pos_h
            else:
                dpq, pos = dpq + dpq_h, pos + pos_h
        dcq = dcq_s[j] * scale
        dpq = dpq * scale
        small[0, j, KERNEL:KERNEL + 1, :] = jnp.sum(dcq, axis=0, keepdims=True)
        small[0, j, KERNEL + 1:KERNEL + 2, :] = jnp.sum(dpq, axis=0, keepdims=True)
        dq = (dcq + dpq).astype(bf16)
        z_s[...] = z_s[...] + dot(dq, block[:, 0:w], 1, 1)
        put_grad(2, j, 0, dot(a2_turn[:, block_of(t, rows)], dq, 1, 0).astype(bf16))
        put_grad(2, j, w, dot(a2_turn[...], kv[j], 1, 0).astype(bf16))
        put_grad(2, j, 3 * w, (pos.T * scale).astype(bf16))
        for turn in range(n_t):
            chosen = fold_plan_two[turn] if turn < len(fold_plan_two) else ()
            if chosen:
                @pl.when(j == turn)
                def _(chosen=chosen):
                    for c, stage in chosen:
                        fold_step(c, stage, stage < n_link)
    loop(n_t, queries_back)

    fold_start(2)
    small_buf, small_z = r.small_buf, r.small_z
    all_bits = [CORE] + links[0]

    def small_copy(k):
        return remote(small.at[k], small_buf.at[k], r.s_send.at[k], r.s_recv.at[k], (flip(d, all_bits[k]), t))

    small_z_copies = [remote(small.at[len(all_bits), lax.rem(t + k + 1, n_t)], small_z.at[k], r.sz_send.at[0],
                             r.sz_recv.at[0], z_peers[k]) for k in z_range]
    def small_next(k):
        small_copy(k - 1).wait_recv()
        small[k] = small[k - 1] + small_buf[k - 1]
        if k < len(all_bits):
            small_copy(k).start()
        else:
            start_all(small_z_copies)

    small_copy(0).start()
    a_turn[...] = turned(a1[...])
    arrive_all(rf_copies)
    small_next(1)

    def join_rows(part):
        total = z_s[part, :] + rf_z[part, :]
        for k in z_range:
            total = total + rf_buf[k, part, :].astype(f32)
        z_s[part, :] = total
    row_loop(rows, 64, join_rows)
    join_norm(1, lambda part: x1[part, :], 0.5)
    fold_step(2, 0)

    dz_turn[...] = turned(dz[...])
    def fold_middle():
        for c in (4, 3):
            fold_send(c)
        fold_step(1, 0)

    feed_back(dz, dz_turn, a_turn, wbuf.at[0], wbuf.at[1], z_s, r.hid1, r.slope1, grad_chunk(0), grad_chunk(1),
              lambda: fold_start(1), fold_middle)
    fold_start(0)
    join_norm(0, lambda part: x_ref[part, :].astype(f32), 1.0)
    leave(r.dx0)

    def gsum_copy(k):
        return remote(gsum.at[k], r.gsum_buf.at[k], r.g_send.at[k], r.g_recv.at[k], (flip(d, all_bits[k]), t))

    gsum_z_copies = [remote(gsum.at[len(all_bits)], r.gsum_z.at[k], r.gz_send.at[0], r.gz_recv.at[0],
                            z_peers[k]) for k in z_range]
    gsum_copy(0).start()

    def gsum_next(k):
        gsum_copy(k - 1).wait_recv()
        gsum[k] = gsum[k - 1] + r.gsum_buf[k - 1]
        if k < len(all_bits):
            gsum_copy(k).start()
        else:
            start_all(gsum_z_copies)

    chain = 1
    for u, stage in tail_plan(final):
        fold_unit(u, stage)
        if u == (0, CUTS - 1) and chain <= len(all_bits):
            if chain > 1:
                small_next(chain)
            gsum_next(chain)
            chain += 1
    for k in range(chain, len(all_bits) + 1):
        small_next(k)
        gsum_next(k)
    settled(small_z, r.sz_recv.at[0], before)
    total = small[len(all_bits), t]
    for k in z_range:
        total = total + small_z[k]
    r.g_taps[...] = total[0:KERNEL, :]
    for pair in range(2):
        row = total[KERNEL + pair:KERNEL + pair + 1, :]
        for h in range(local_heads):
            place = lax.broadcasted_iota(jnp.int32, (n_bias, w), 1)
            spot_h = (place == lax.broadcasted_iota(jnp.int32, (n_bias, w), 0) + d * n_bias + h * head_dim).astype(f32)
            r.g_bias[pair, h:h + 1, :] = lax.dot_general(row, spot_h, (((1,), (1,)), ((), ())), precision=high,
                                                         preferred_element_type=f32)
    settled(r.gsum_z, r.gz_recv.at[0], before)
    total_g = gsum[len(all_bits)]
    for k in z_range:
        total_g = total_g + r.gsum_z[k]
    spot_g = lax.dot_general(total_g, gain_spot, (((1,), (1,)), ((), ())), precision=high, preferred_element_type=f32)
    r.g_gains[...] = spot_g[0:5, :]

    leave(r.g_taps, r.g_bias, r.g_gains)
    for k, name in enumerate(leaving):
        pltpu.make_async_copy(getattr(r, name[:-len(HBM)]), getattr(r, name), r.out_sem.at[k]).wait()
    settled(taps.at[pl.ds(0, n_t - 1)], r.f_send.at[0], before)
    settled(a2_all.at[pl.ds(0, n_t - 1)], r.a_send.at[0], before)
    settled(small_z, r.sz_send.at[0], before)
    settled(r.gsum_z, r.gz_send.at[0], before)
    sent_all(rf_copies)
    settled(e_buf.at[pl.ds(0, n_t - 1)], r.e_send.at[0], before)
    sent_all(e_copies(n_t - 1, n_t + n_link))
    for k in range(2):
        settled(sum_buf.at[k], r.sum_send.at[k], before)
        settled(sum_z.at[k], r.sumz_send.at[k], before)
    for k in range(len(all_bits)):
        small_copy(k).wait_send()
        gsum_copy(k).wait_send()
    settled(gbuf.at[pl.ds(0, CHUNKS // 2)], r.core_send.at[0], before)
    settled(gbuf.at[0, pl.ds(0, CHUNKS * rows_w), pl.ds(0, (n_t - 1) * width)], r.fz_send.at[0], before)
    for c in range(CHUNKS):
        settled(gbuf.at[0, pl.ds(0, (len(groups) - 1) * rows_w), :], r.fd_send.at[c], before)


def layer_kernel(n_dp, n_t, head_dim, inputs):
    given = SimpleNamespace(**inputs)
    rows, D = given.x.shape
    rows_w, width = given.fu.shape
    w = D // n_t
    frames = rows * n_t
    heads = D // head_dim
    hidden = n_t * width
    n_bits = n_dp.bit_length() - 1
    n_e = n_t - 1 + n_bits
    n_gain = given.gain_in.shape[1]
    n_bias = given.bias_in.shape[2]
    tap_rows = 40
    groups = n_dp // 2
    z = n_t - 1
    sem = pltpu.SemaphoreType.DMA
    vm = pltpu.VMEM
    outs = dict(
        out=((rows, D), f32), dx0=((rows, D), f32), g_gains=((5, n_gain), f32), g_fu=((rows_w, width), f32),
        g_fd=((rows_w, width), f32), g_at=((4, rows_w, w), f32), g_ao=((rows_w, w), f32),
        g_bias=((2, w // head_dim, n_bias), f32), g_cw=((rows_w, 2, w), f32), g_taps=((KERNEL, w), f32),
        g_bn=((2, w), f32), g_co=((rows_w, w), f32), g_su=((rows_w, width), f32), g_sd=((rows_w, width), f32))
    edge_shape = (n_t, rows + 2 * EDGE, w)
    scratch = dict(
        pack=vm((2, rows_w, width), bf16), taps_own=vm((tap_rows, w), f32), wbuf=vm((CHUNKS, n_dp * rows_w, hidden), bf16),
        gbuf=vm((CHUNKS - 2, n_dp * rows_w, hidden), bf16), gains=vm((8, D), f32),
        taps=vm((n_t, tap_rows, w), f32), e_acc=vm((n_bits + 2, 8, D), f32), e_buf=vm((n_e, 8, D), f32),
        phase=vm((frames, D), bf16), spin=vm((2, rows, D // 2), f32), u_s=vm((rows, D), bf16),
        z_s=vm((rows, D), f32), x1=vm((rows, D), f32), x2=vm((rows, D), f32),
        x3=vm((rows, D), f32), a1=vm((rows, D), bf16), a2=vm((rows, D), bf16), a3=vm((rows, D), bf16),
        a4=vm((rows, D), bf16), dz=vm((rows, D), bf16), dz_turn=vm((D, rows), bf16),
        a_turn=vm((D, rows), bf16), a2_all=vm((n_t, rows, D), bf16), a2_turn=vm((D, frames), bf16),
        hid1=vm((rows, hidden), bf16), slope1=vm((rows, hidden), bf16), hid2=vm((rows, hidden), bf16),
        slope2=vm((rows, hidden), bf16), kv=vm((n_t, frames, 2 * w), bf16), cq=vm((n_t, rows, w), bf16),
        pq=vm((n_t, rows, w), bf16), mix=vm((n_t, rows, w), f32), inv_s=vm((n_t, rows, w), f32), probs=vm((heads, rows, frames), bf16),
        s_s=vm((rows, frames), f32), dmix_s=vm((n_t, rows, w), bf16), dmix_turn=vm((n_t, w, rows), bf16),
        cq_turn=vm((n_t, w, rows), bf16), dcq_s=vm((n_t, rows, w), f32),
        rf_z=vm((rows, D), f32), rf_out=vm((z, rows, D), bf16), rf_buf=vm((z, rows, D), bf16),
        glu=vm(edge_shape, f32), bhat=vm(edge_shape, f32), dbn=vm(edge_shape, f32),
        val=vm((n_t, rows, w), f32), sig=vm((n_t, rows, w), f32), act=vm((n_t, rows, w), bf16),
        de=vm((rows, 2 * w), bf16), sums=vm((2, 2 * n_t, w), f32), sum_mid=vm((2, 2 * n_t, w), f32),
        sum_out=vm((2, 2 * n_t, w), f32), sum_buf=vm((2, n_dp - 1, 2 * n_t, w), f32),
        sum_z=vm((2, z, 2 * n_t, w), f32), core_buf=vm((CHUNKS, groups, rows_w, hidden), bf16),
        dp_buf=vm((CHUNKS, 2, groups - 1, rows_w, hidden // 2), bf16), z_buf=vm((CHUNKS, z, rows_w, width), bf16),
        small=vm((n_bits + 1, n_t, tap_rows, w), f32), small_buf=vm((n_bits, n_t, tap_rows, w), f32),
        small_z=vm((z, tap_rows, w), f32), gsum=vm((n_bits + 1, 8, D), f32), gsum_buf=vm((n_bits, 8, D), f32),
        gsum_z=vm((z, 8, D), f32), local_sem=sem((CHUNKS, CUTS)))
    n_link = n_bits - 1
    scratch.update(
        z_send=sem((1,)), z_recv=sem((CHUNKS, CUTS)), d_send=sem((CHUNKS,)), d_recv=sem((CHUNKS, CUTS, n_bits)),
        f_send=sem((1,)), f_recv=sem((1,)), e_send=sem((n_bits + 1,)), e_recv=sem((n_bits + 1,)),
        a_send=sem((1,)), a_recv=sem((1,)), edge_send=sem((3, 2)), edge_recv=sem((3, 2)),
        sum_send=sem((2,)), sum_recv=sem((2,)), sumz_send=sem((2,)), sumz_recv=sem((2,)),
        core_send=sem((1,)), core_recv=sem((CHUNKS, CUTS)), fd_send=sem((CHUNKS,)),
        fd_recv=sem((CHUNKS, CUTS, n_link)), fz_send=sem((1,)), fz_recv=sem((CHUNKS, CUTS)),
        rf_ss=sem((z,)), rf_rs=sem((z,)), s_send=sem((n_bits,)), s_recv=sem((n_bits,)),
        sz_send=sem((1,)), sz_recv=sem((1,)), g_send=sem((n_bits,)), g_recv=sem((n_bits,)),
        gz_send=sem((1,)), gz_recv=sem((1,)))
    for name, (dims, kind) in outs.items():
        scratch[name] = vm(dims, kind)
    scratch.update(out_sem=sem((len(outs),)))
    names = list(inputs) + [name + HBM for name in outs] + list(scratch)
    vmem = pl.BlockSpec(memory_space=pltpu.VMEM)
    result = pl.pallas_call(
        functools.partial(layer_body, names, n_dp, n_t, head_dim),
        name="layer",
        out_shape=tuple(jax.ShapeDtypeStruct(dims, kind) for dims, kind in outs.values()),
        in_specs=[vmem] * len(inputs),
        out_specs=(pl.BlockSpec(memory_space=pl.ANY),) * len(outs),
        scratch_shapes=list(scratch.values()),
        compiler_params=pltpu.CompilerParams(collective_id=0, has_side_effects=True, vmem_limit_bytes=67043328),
    )(*inputs.values())
    return result


def settle_body(*refs):
    count = (len(refs) - 2) // 3
    sources, results, rooms = refs[:count], refs[count:2 * count], refs[2 * count:3 * count]
    sem_in, sem_out = refs[3 * count:]
    loads = [pltpu.make_async_copy(a, b, sem_in.at[k]) for k, (a, b) in enumerate(zip(sources, rooms))]
    stores = [pltpu.make_async_copy(a, b, sem_out.at[k]) for k, (a, b) in enumerate(zip(rooms, results))]
    for copy in loads:
        copy.start()
    for load, store in zip(loads, stores):
        load.wait()
        store.start()
    for copy in stores:
        copy.wait()


def settle(arrays):
    hbm = pl.BlockSpec(memory_space=pl.ANY)
    count = len(arrays)
    sem = pltpu.SemaphoreType.DMA
    return pl.pallas_call(
        settle_body,
        name="settle",
        out_shape=tuple(jax.ShapeDtypeStruct(a.shape, a.dtype) for a in arrays),
        in_specs=[hbm] * count,
        out_specs=(hbm,) * count,
        scratch_shapes=[pltpu.VMEM(a.shape, a.dtype) for a in arrays] + [sem((count,)), sem((count,))],
    )(*arrays)


def angle_tables(frames, width):
    step = 32
    frequency = np.exp(np.arange(width // 2) * (-2.0 * math.log(10000.0) / width))
    coarse = np.arange(frames // step)[:, None] * step * frequency
    fine = np.arange(step)[:, None] * frequency
    return jnp.asarray(np.stack([np.sin(coarse), np.cos(coarse), np.sin(fine), np.cos(fine)]), f32)


def per_device(n_dp, n_t, inputs, out_grad, norm_gains, first_up, first_down, attend_in, attend_out, position_bias,
               convolve_in, depth_kernel, batch_norm, convolve_out, second_up, second_down):
    rows, D = inputs.shape
    w = attend_in.shape[2]
    R = attend_in.shape[1]
    n_bias = position_bias.shape[2]
    head_dim = n_bias * n_dp
    got = layer_kernel(n_dp, n_t, head_dim, dict(
        fu=first_up, fd=first_down.T, at=attend_in, cw=convolve_in, ao=attend_out.T, co=convolve_out.T, su=second_up,
        sd=second_down.T, gain_in=norm_gains, bias_in=position_bias, tap_in=depth_kernel.T, bn_in=batch_norm, x=inputs,
        og=out_grad, tab=angle_tables(rows * n_t, D)))
    (out, dx0, g_gains, g_fu, g_fd, g_at, g_ao, g_bias, g_cw, g_taps, g_bn, g_co, g_su, g_sd) = settle(got)
    return (out, dx0, g_gains, g_fu, g_fd.T, g_at, g_ao.T, g_bias, g_cw, g_taps.T, g_bn, g_co.T, g_su, g_sd.T)


def solution(mesh):
    n_dp, n_t = mesh.shape["dp"], mesh.shape["tensor"]
    row = P(("dp", "tensor"), None)
    gain = P(None, ("dp", "tensor"))
    up = P("dp", "tensor")
    down = P("tensor", "dp")
    weights = (up, down, P(None, "dp", "tensor"), down, P(None, "tensor", "dp"), P("dp", None, "tensor"),
               P("tensor", None), P(None, "tensor"), down, up, down)
    return jax.shard_map(
        functools.partial(per_device, n_dp, n_t), mesh=mesh,
        in_specs=(row, row, gain) + weights,
        out_specs=(row, row, gain) + weights,
        check_vma=False)
```

```python
import functools
import math
from types import SimpleNamespace

import jax
import jax.numpy as jnp
import numpy as np
from jax import lax
from jax.experimental import pallas as pl
from jax.experimental.pallas import tpu as pltpu
from jax.sharding import PartitionSpec as P

MESH = pl.DeviceIdType.MESH
CHUNKS = 6
CUTS = 2
AHEAD = 2
CORE = 1
EDGE = 16
KERNEL = 31
HALF = KERNEL // 2
norm_eps = 1e-05
f32 = jnp.float32
bf16 = jnp.bfloat16
high = lax.Precision.HIGHEST


def flip(index, mask):
    result = index
    bit = 1
    while bit <= mask:
        if mask & bit:
            result = result + bit - 2 * bit * ((index // bit) % 2)
        bit *= 2
    return result


def span(bits):
    masks = [0]
    for bit in bits:
        masks = masks + [mask ^ bit for mask in masks]
    return masks


def link_orders(n_dp):
    bits = [1 << k for k in range(1, n_dp.bit_length() - 1)]
    return (bits, bits[::-1])


def greet(peers):
    barrier = pltpu.get_barrier_semaphore()
    for peer in peers:
        pl.semaphore_signal(barrier, inc=1, device_id=peer, device_id_type=MESH)
    pl.semaphore_wait(barrier, len(peers))


def remote(src, dst, send_sem, recv_sem, peer):
    return pltpu.make_async_remote_copy(
        src_ref=src, dst_ref=dst, send_sem=send_sem, recv_sem=recv_sem,
        device_id=peer, device_id_type=MESH)


def start_all(copies):
    for copy in copies:
        copy.start()


def settled(ref, sem, peer):
    remote(ref, ref, sem, sem, peer).wait_recv()


def arrive_all(copies):
    for copy in copies:
        copy.wait_recv()


def sent_all(copies):
    for copy in copies:
        copy.wait_send()


def dot(left, right, left_dim, right_dim):
    return lax.dot_general(left, right, (((left_dim,), (right_dim,)), ((), ())), preferred_element_type=f32)


def turned(value):
    return value.astype(f32).T.astype(bf16)


def head_mask(shape, axis, head_dim, head):
    place = lax.broadcasted_iota(jnp.int32, shape, axis)
    return (place >= head * head_dim) & (place < (head + 1) * head_dim)


def keep(mask, value):
    return jnp.where(mask, value, jnp.zeros_like(value))


def block_of(k, size):
    return pl.ds(pl.multiple_of(k * size, size), size)


def loop(count, body, unroll=1):
    def step(k, carry):
        body(k)
        return carry
    lax.fori_loop(0, count, step, 0, unroll=unroll)


def halves(count, body, between, unroll=1):
    loop(count // 2, body, unroll)
    between()
    loop(count - count // 2, lambda k: body(k + count // 2), unroll)


def row_loop(rows, size, body):
    loop(rows // size, lambda k: body(block_of(k, size)))


def sigmoid(values):
    return 1.0 / (1.0 + jnp.exp(-values))


def norm_parts(values):
    centred = values - jnp.mean(values, axis=-1, keepdims=True)
    inverse = lax.rsqrt(jnp.mean(centred * centred, axis=-1, keepdims=True) + norm_eps)
    return centred * inverse, inverse


def norm_back(value, incoming, gain_row):
    scaled, inverse = norm_parts(value)
    grad_scaled = incoming * gain_row
    inner = jnp.mean(grad_scaled * scaled, axis=-1, keepdims=True)
    grad_in = inverse * (grad_scaled - jnp.mean(grad_scaled, axis=-1, keepdims=True) - scaled * inner)
    return scaled, grad_in, jnp.sum(incoming * scaled, axis=0, keepdims=True)


def tail_plan(final):
    parts = range(CUTS)
    last = CUTS - 1
    plan = [((2, part), 1, True, None) for part in parts] + [((0, part), 0, False, None) for part in parts]
    plan += [((1, part), 1, True, (0, 0) if part == 0 else None) for part in parts]
    for stage in range(2, final):
        plan += [((2, part), stage, True, None) for part in parts]
    for stage in range(2, final):
        plan += [((1, part), stage, True, (0, last) if (stage, part) == (2, 0) else None) for part in parts]
    for stage in range(1, final):
        plan += [((0, part), stage, True, None) for part in parts]
    return plan + [((c, part), final, True, None) for c in (5, 4, 3, 2, 1, 0) for part in parts]


def relay_order(stages):
    hop, link_free, order = 1.5, 0.0, []
    units = [(c, part) for c in range(CHUNKS) for part in range(CUTS)]
    waiting = [(7.0 + 6.5 / CUTS * (k + 1), 0, u) for k, u in enumerate(units)]
    while waiting:
        waiting.sort()
        now, stage, u = waiting.pop(0)
        order.append((now, stage, u))
        if stage < stages - 1:
            link_free = max(now, link_free) + 3.1 / CUTS * 2 ** stage
            waiting.append((link_free + hop, stage + 1, u))
        elif stage == stages - 1:
            waiting.append((now + hop + 2.0 / CUTS, stages, u))
    return order


SLAB = 512
NORM_ROWS = 256
HBM = "_hbm"


def feed_rows(a_ref, up, down_t, z_ref, hidden, slope):
    z_ref[...] = jnp.zeros_like(z_ref)

    def step(k):
        cols = block_of(k, SLAB)
        pre = dot(a_ref[...], up[:, cols], 1, 0)
        sig = sigmoid(pre)
        hidden[:, cols] = (pre * sig).astype(bf16)
        slope[:, cols] = (sig * (1.0 + pre * (1.0 - sig))).astype(bf16)
        z_ref[...] = z_ref[...] + dot(hidden[:, cols], down_t[:, cols], 1, 1)
    loop(up.shape[1] // SLAB, step, 2)


def feed_back(dz_ref, dz_turn, a_turn, up, down_t, z_ref, hidden, slope, g_up, g_down, start_down, middle):
    z_ref[...] = jnp.zeros_like(z_ref)

    def first_step(k):
        cols = block_of(k, SLAB)
        g_down[:, cols] = dot(dz_turn[...], hidden[:, cols], 1, 0).astype(bf16)
    loop(up.shape[1] // SLAB, first_step)
    start_down()
    slabs = up.shape[1] // SLAB

    def step(k):
        cols = block_of(k, SLAB)
        grad_pre = (dot(dz_ref[...], down_t[:, cols], 1, 0) * slope[:, cols].astype(f32)).astype(bf16)
        g_up[:, cols] = dot(a_turn[...], grad_pre, 1, 0).astype(bf16)
        z_ref[...] = z_ref[...] + dot(grad_pre, up[:, cols], 1, 1)
    loop(slabs - 1, step, slabs - 1)
    middle()
    step(slabs - 1)


def layer_body(names, n_dp, n_t, head_dim, *all_refs):
    r = SimpleNamespace(**dict(zip(names, all_refs)))
    d = lax.axis_index("dp")
    t = lax.axis_index("tensor")
    pack, wbuf, gbuf = r.pack, r.wbuf, r.gbuf
    x_ref, gains, taps = r.x, r.gains, r.taps
    rows_w, width = pack.shape[1], pack.shape[2]
    rows, D = x_ref.shape
    w = D // n_t
    half = n_t * width // 2
    frames = rows * n_t
    local_heads = w // head_dim
    n_gain = r.gain_in.shape[1]
    n_bias = n_gain // local_heads
    row_count = frames * n_dp
    scale = head_dim ** -0.5
    links = link_orders(n_dp)
    orders = [order + [CORE] for order in links]
    stages = len(orders[0])
    n_link = len(links[0])
    z_peers = [(d, lax.rem(t + step, n_t)) for step in range(1, n_t)]
    d_peers = [(flip(d, mask), t) for mask in range(1, n_dp)]
    before = (d, lax.rem(t + n_t - 1, n_t))
    after = (d, lax.rem(t + 1, n_t))
    z_range = range(n_t - 1)
    leaving = [name for name in names if name.endswith(HBM)]

    def leave(*chosen):
        for ref in chosen:
            name = [one for one in leaving if getattr(r, one[:-len(HBM)]) is ref][0]
            k = leaving.index(name)
            pltpu.make_async_copy(ref, getattr(r, name), r.out_sem.at[k]).start()

    greet(z_peers + d_peers)

    def window(u, mask, start, size):
        c, part = u
        count = rows_w // CUTS
        first = pl.multiple_of(flip(d, mask) * rows_w + part * count, count)
        return wbuf.at[c, pl.ds(first, count), pl.ds(start, size)]

    def own(u):
        return window(u, 0, pl.multiple_of(t * width, width), width)

    def source(u):
        count = rows_w // CUTS
        return sources[u[0]].at[pl.ds(u[1] * count, count), :]

    sources = (r.fu, r.fd, pack.at[0], pack.at[1], r.su, r.sd)

    def z_copies(u):
        return [remote(source(u), own(u), r.z_send.at[0], r.z_recv.at[u[0], u[1]], z_peers[k])
                for k in z_range]

    def local_copy(u):
        return pltpu.make_async_copy(source(u), own(u), r.local_sem.at[u[0], u[1]])

    def dp_copies(u, stage):
        copies = []
        for h in range(2):
            bit = orders[h][stage]
            masks = span(orders[h][:stage])
            for mask in masks:
                part = window(u, mask, h * half, half)
                copies.append(remote(part, part, r.d_send.at[u[0]], r.d_recv.at[u[0], u[1], stage],
                                     (flip(d, bit), t)))
        return copies

    def send_unit(u):
        local_copy(u).start()
        start_all(z_copies(u))

    def allowed(done):
        return AHEAD + done + max(0, done - 3)

    queue = [(c, part) for c in range(CHUNKS) for part in range(CUTS)]

    e_acc, e_buf = r.e_acc, r.e_buf

    def e_copies(first, stop):
        copies = []
        for k in range(first, stop):
            if k < n_t - 1:
                source, peer = e_acc.at[0], z_peers[k]
            else:
                source, peer = e_acc.at[k - n_t + 2], (flip(d, orders[0][k - n_t + 1]), t)
            sem = max(0, k - n_t + 2)
            copies.append(remote(source, e_buf.at[k], r.e_send.at[sem], r.e_recv.at[sem], peer))
        return copies

    taps_own = r.taps_own
    tap_copies = [remote(taps_own, taps.at[t], r.f_send.at[0], r.f_recv.at[0], z_peers[k]) for k in z_range]

    entry = lax.broadcasted_iota(jnp.int32, (n_gain, D), 0)
    lane = lax.broadcasted_iota(jnp.int32, (n_gain, D), 1)
    gain_spot = (lane == (d * n_t + t) * n_gain + entry).astype(f32)
    e_acc[0] = jnp.zeros_like(e_acc[0])
    e_acc[0, 0:5, :] = jnp.dot(r.gain_in[...], gain_spot, precision=high, preferred_element_type=f32)
    entry_b = lax.broadcasted_iota(jnp.int32, (n_bias, D), 0)
    lane_b = lax.broadcasted_iota(jnp.int32, (n_bias, D), 1)
    bias_spots = [(lane_b == entry_b + d * n_bias + (h + t * local_heads) * head_dim).astype(f32)
                  for h in range(local_heads)]
    for pair in range(2):
        row = None
        for h in range(local_heads):
            term = jnp.dot(r.bias_in[pair, h:h + 1, :].astype(f32), bias_spots[h], precision=high,
                           preferred_element_type=f32)
            row = term if row is None else row + term
        e_acc[0, 5 + pair:6 + pair, :] = row
    start_all(e_copies(0, n_t - 1))
    for u in queue[:AHEAD]:
        send_unit(u)
    for k in range(4):
        pack[0, :, k * w:(k + 1) * w] = r.at[k]
    for k in range(2):
        pack[1, :, k * w:(k + 1) * w] = r.cw[:, k, :]
    pack[1, :, 2 * w:3 * w] = r.ao[...]
    pack[1, :, 3 * w:4 * w] = r.co[...]
    taps_own[...] = jnp.zeros_like(taps_own)
    taps_own[0:KERNEL, :] = r.tap_in[...]
    taps_own[KERNEL:KERNEL + 2, :] = r.bn_in[...]
    start_all(tap_copies)
    taps[t] = taps_own[...]

    def relay(stage, u):
        count = rows_w // CUTS
        if stage == 0:
            local_copy(u).wait()
            settled(wbuf.at[0, pl.ds(0, count), pl.ds(0, (n_t - 1) * width)], r.z_recv.at[u[0], u[1]], before)
            place = queue.index(u)
            for other in queue[allowed(place):allowed(place + 1)]:
                send_unit(other)
        else:
            settled(wbuf.at[0, pl.ds(0, count * 2 ** (stage - 1)), :], r.d_recv.at[u[0], u[1], stage - 1], before)
        if stage < stages:
            start_all(dp_copies(u, stage))

    def ready_after(order, chunks):
        places = [k + 1 for k, (_, stage, u) in enumerate(order) if stage == stages and u[0] in chunks]
        return max(places, default=0)

    e_step = [0]

    def e_next():
        k = e_step[0]
        if k == 0:
            settled(e_buf.at[pl.ds(0, n_t - 1)], r.e_recv.at[0], before)
            total = e_acc[0]
            for i in z_range:
                total = total + e_buf[i]
            e_acc[1] = total
        elif k <= n_link + 1:
            arrive_all(e_copies(n_t - 2 + k, n_t - 1 + k))
            e_acc[k + 1] = e_acc[k] + e_buf[n_t - 2 + k]
        if k <= n_link:
            start_all(e_copies(n_t - 1 + k, n_t + k))
        e_step[0] = k + 1

    tab, phase, spin = r.tab, r.phase, r.spin
    step_t = tab.shape[1]

    def table(k):
        cs, cc = tab[0, pl.ds(k, 1), :], tab[1, pl.ds(k, 1), :]
        part = block_of(k, step_t)
        phase[part, 0:D // 2] = (cs * tab[3] + cc * tab[2]).astype(bf16)
        phase[part, D // 2:D] = (cc * tab[3] - cs * tab[2]).astype(bf16)
    loop(frames // step_t, table)

    def own_table(k):
        place = t * (rows // step_t) + k
        cs, cc = tab[0, pl.ds(place, 1), :], tab[1, pl.ds(place, 1), :]
        part = block_of(k, step_t)
        spin[0, part, :] = cs * tab[3] + cc * tab[2]
        spin[1, part, :] = cc * tab[3] - cs * tab[2]
    loop(rows // step_t, own_table)

    def spun(sines, cosines):
        u_s = r.u_s
        u_s[:, 0:D // 2] = (cosines * spin[0] - sines * spin[1]).astype(bf16)
        u_s[:, D // 2:D] = (sines * spin[0] + cosines * spin[1]).astype(bf16)

    z_s, a1, a2, a2_all = r.z_s, r.a1, r.a2, r.a2_all
    x1, x2, x3 = r.x1, r.x2, r.x3
    events = relay_order(stages)
    ready = ready_after(events, (0, 1))
    for k, (_, stage, u) in enumerate(events[:ready]):
        relay(stage, u)
        if k % 4 == 3 and e_step[0] < n_link + 2:
            e_next()
    while e_step[0] < n_link + 2:
        e_next()
    gains[...] = e_acc[n_link + 2]

    def norm_one(part):
        a1[part, :] = (norm_parts(x_ref[part, :].astype(f32))[0] * gains[0:1, :]).astype(bf16)
    row_loop(rows, NORM_ROWS, norm_one)
    feed_rows(a1, wbuf.at[0], wbuf.at[1], z_s, r.hid1, r.slope1)

    def norm_two(part):
        value = x_ref[part, :].astype(f32) + 0.5 * z_s[part, :]
        x1[part, :] = value
        a2[part, :] = (norm_parts(value)[0] * gains[1:2, :]).astype(bf16)
    row_loop(rows, NORM_ROWS, norm_two)

    a_copies = [remote(a2, a2_all.at[t], r.a_send.at[0], r.a_recv.at[0], z_peers[k]) for k in z_range]
    start_all(a_copies)
    a2_all[t] = a2[...]
    for _, stage, u in events[ready:]:
        relay(stage, u)
    settled(a2_all.at[pl.ds(0, n_t - 1)], r.a_recv.at[0], before)
    kv, cq, pq, probs, mix, s_s, u_s = r.kv, r.cq, r.pq, r.probs, r.mix, r.s_s, r.u_s
    z_s[...] = jnp.zeros_like(z_s)
    inv_s = r.inv_s
    scale_low = jnp.asarray(scale, bf16)

    def head_group(j):
        cols = block_of(j, width)
        block = wbuf[2, :, cols]
        for part in range(n_t):
            kv[j, part * rows:(part + 1) * rows, :] = dot(a2_all[part], block[:, w:3 * w], 1, 0).astype(bf16)
        q = dot(a2[...], block[:, 0:w], 1, 0)
        if w % 128 == 0:
            bias = gains[5:7, block_of(j, w)]
        else:
            bias = gains[5:7, 0:w]
            for other in range(1, n_t):
                bias = jnp.where(j == other, gains[5:7, other * w:(other + 1) * w], bias)
        cq_j = (q + bias[0:1]).astype(bf16)
        pq_j = (q + bias[1:2]).astype(bf16)
        cq[j] = cq_j
        pq[j] = pq_j
        for h in range(local_heads):
            mask = head_mask((rows, w), 1, head_dim, h)
            spread = dot(keep(mask, pq_j), block[:, 3 * w:4 * w], 1, 1)
            spun(spread[:, :D // 2] * scale, spread[:, D // 2:] * scale)
            s_s[...] = dot(u_s[...], phase[...], 1, 1) + dot(keep(mask, cq_j) * scale_low, kv[j, :, 0:w], 1, 1)
            head = j * local_heads + h

            s = s_s[...]
            e = jnp.exp(s - jnp.max(s, axis=-1, keepdims=True))
            inv = 1.0 / jnp.sum(e, axis=-1, keepdims=True)
            probs[head] = e.astype(bf16)
            mixed = dot(probs[head], kv[j, :, w:2 * w], 1, 0) * inv
            inv = jnp.broadcast_to(inv, (rows, w))
            inverse = inv if h == 0 else jnp.where(mask, inv, inverse)
            mixture = mixed if h == 0 else jnp.where(mask, mixed, mixture)
        mix[j] = mixture
        inv_s[j] = inverse
        z_s[...] = z_s[...] + dot(mixture.astype(bf16), wbuf[3, :, cols][:, 2 * w:3 * w], 1, 1)
    loop(n_t, head_group, 2)

    a3, glu, bhat, val, sig, act = r.a3, r.glu, r.bhat, r.val, r.sig, r.act
    dbn, sums, sum_buf, sum_mid, sum_z = r.dbn, r.sums, r.sum_buf, r.sum_mid, r.sum_z
    inner = pl.ds(EDGE, rows)

    def norm_three(part):
        value = x1[part, :] + z_s[part, :]
        x2[part, :] = value
        a3[part, :] = (norm_parts(value)[0] * gains[2:3, :]).astype(bf16)
    row_loop(rows, NORM_ROWS, norm_three)

    def gate(j):
        block = wbuf[3, :, block_of(j, width)]
        e = dot(a3[...], block[:, 0:2 * w], 1, 0)
        sig_j = sigmoid(e[:, w:2 * w])
        val[j] = e[:, 0:w]
        sig[j] = sig_j
        glu[j, inner, :] = e[:, 0:w] * sig_j
    loop(n_t, gate)

    def edge_copies(ref, k):
        first, last = pl.ds(EDGE, EDGE), pl.ds(rows, EDGE)
        return [remote(ref.at[:, first, :], ref.at[:, pl.ds(EDGE + rows, EDGE), :], r.edge_send.at[k, 0],
                       r.edge_recv.at[k, 0], before),
                remote(ref.at[:, last, :], ref.at[:, pl.ds(0, EDGE), :], r.edge_send.at[k, 1],
                       r.edge_recv.at[k, 1], after)]

    def edge_start(ref, k):
        back, ahead = edge_copies(ref, k)

        @pl.when(t > 0)
        def _():
            back.start()

        @pl.when(t < n_t - 1)
        def _():
            ahead.start()

        @pl.when(t == 0)
        def _():
            ref[:, pl.ds(0, EDGE), :] = jnp.zeros((n_t, EDGE, w), f32)

        @pl.when(t == n_t - 1)
        def _():
            ref[:, pl.ds(EDGE + rows, EDGE), :] = jnp.zeros((n_t, EDGE, w), f32)

    def edge_wait(ref, k):
        back, ahead = edge_copies(ref, k)

        @pl.when(t > 0)
        def _():
            ahead.wait_recv()
            back.wait_send()

        @pl.when(t < n_t - 1)
        def _():
            back.wait_recv()
            ahead.wait_send()

    def sum_copies(k):
        return [remote(sums.at[k], sum_buf.at[k, i], r.sum_send.at[k], r.sum_recv.at[k], d_peers[i])
                for i in range(n_dp - 1)]

    def sum_z_copies(k):
        return [remote(sum_mid.at[k], sum_z.at[k, i], r.sumz_send.at[k], r.sumz_recv.at[k], z_peers[i])
                for i in z_range]

    def sum_middle(k):
        settled(sum_buf.at[k], r.sum_recv.at[k], before)
        total = sums[k]
        for i in range(n_dp - 1):
            total = total + sum_buf[k, i]
        sum_mid[k] = total
        start_all(sum_z_copies(k))

    def sum_end(k):
        settled(sum_z.at[k], r.sumz_recv.at[k], before)
        total = sum_mid[k]
        for i in z_range:
            total = total + sum_z[k, i]
        sum_mid_out = r.sum_out
        sum_mid_out[k] = total

    edge_start(glu, 0)
    settled(taps.at[pl.ds(0, n_t - 1)], r.f_recv.at[0], before)
    edge_wait(glu, 0)
    size = 64

    def sweep(ref, j, first, backward):
        total = None
        for k in range(KERNEL):
            offset = EDGE - HALF + (KERNEL - 1 - k if backward else k)
            term = taps[j, k:k + 1, :] * ref[j, pl.ds(first + offset, size), :]
            total = term if total is None else total + term
        return total

    def convolve(j):
        def part_step(k, carry):
            first = pl.multiple_of(k * size, size)
            value = sweep(glu, j, first, False)
            bhat[j, pl.ds(first + EDGE, size), :] = value
            return (carry[0] + jnp.sum(value, axis=0, keepdims=True),
                    carry[1] + jnp.sum(value * value, axis=0, keepdims=True))
        zero = jnp.zeros((1, w), f32)
        one, two = lax.fori_loop(0, rows // size, part_step, (zero, zero))
        sums[0, pl.ds(2 * j, 1), :] = one
        sums[0, pl.ds(2 * j + 1, 1), :] = two
    loop(n_t, convolve)
    start_all(sum_copies(0))
    sum_middle(0)
    sum_end(0)

    def bn_parts(j):
        mean = r.sum_out[0, pl.ds(2 * j, 1), :] / row_count
        square = r.sum_out[0, pl.ds(2 * j + 1, 1), :] / row_count
        return mean, lax.rsqrt(square - mean * mean + norm_eps), taps[j, KERNEL:KERNEL + 1, :], taps[
            j, KERNEL + 1:KERNEL + 2, :]

    z_s[...] = jnp.zeros_like(z_s)

    def activate(j):
        mean, inverse, bn_gain, bn_shift = bn_parts(j)
        scaled = (bhat[j, inner, :] - mean) * inverse
        bhat[j, inner, :] = scaled
        normal = scaled * bn_gain + bn_shift
        act[j] = (normal * sigmoid(normal)).astype(bf16)
        z_s[...] = z_s[...] + dot(act[j], wbuf[3, :, block_of(j, width)][:, 3 * w:4 * w], 1, 1)
    loop(n_t, activate)
    edge_start(bhat, 1)

    a4, dx = r.a4, r.dx0

    def norm_four(part):
        value = x2[part, :] + z_s[part, :]
        x3[part, :] = value
        a4[part, :] = (norm_parts(value)[0] * gains[3:4, :]).astype(bf16)
    row_loop(rows, NORM_ROWS, norm_four)
    feed_rows(a4, wbuf.at[4], wbuf.at[5], z_s, r.hid2, r.slope2)
    gsum = r.gsum
    gsum[...] = jnp.zeros_like(gsum)
    dz, dz_turn, a_turn = r.dz, r.dz_turn, r.a_turn

    def add_gain(row, part_sum):
        gsum[row:row + 1, :] = gsum[row:row + 1, :] + part_sum

    def norm_five(part):
        value = x3[part, :] + 0.5 * z_s[part, :]
        scaled, grad_in, part_sum = norm_back(value, r.og[part, :].astype(f32), gains[4:5, :])
        r.out[part, :] = scaled * gains[4:5, :]
        dx[part, :] = grad_in
        dz[part, :] = (0.5 * grad_in).astype(bf16)
        add_gain(4, part_sum)
    row_loop(rows, NORM_ROWS, norm_five)
    leave(r.out)

    def grad_chunk(c):
        return gbuf.at[c - 2] if c >= 2 else wbuf.at[c + 4]

    def join_norm(row, x_of, factor):
        def step(part):
            _, grad_in, part_sum = norm_back(x_of(part), z_s[part, :], gains[row:row + 1, :])
            value = dx[part, :] + grad_in
            dx[part, :] = value
            dz[part, :] = (factor * value).astype(bf16)
            add_gain(row, part_sum)
        row_loop(rows, NORM_ROWS, step)

    folds = [order[::-1] for order in links]
    groups = span(links[0])
    core_buf, dp_buf, z_buf = r.core_buf, r.dp_buf, r.z_buf

    def grad_rows(u, mask):
        c, part = u
        count = rows_w // CUTS
        return grad_chunk(c).at[pl.ds(pl.multiple_of(flip(d, mask) * rows_w + part * count, count), count), :]

    def part_rows(part):
        return pl.ds(part * (rows_w // CUTS), rows_w // CUTS)

    def core_copies(u):
        return [remote(grad_rows(u, mask ^ CORE), core_buf.at[u[0], k, part_rows(u[1])],
                       r.core_send.at[0], r.core_recv.at[u[0], u[1]],
                       (flip(d, CORE), t)) for k, mask in enumerate(groups)]

    def fold_places(stage):
        places = []
        for h in range(2):
            masks = span(folds[h][stage + 1:])
            base = len(groups) - 2 * len(masks)
            places += [(mask, h, base + j) for j, mask in enumerate(masks)]
        return places

    def fold_copies(u, stage):
        c, part = u
        return [remote(grad_rows(u, mask ^ folds[h][stage]).at[:, pl.ds(h * half, half)],
                       dp_buf.at[c, h, slot, part_rows(part)],
                       r.fd_send.at[c], r.fd_recv.at[c, part, stage], (flip(d, folds[h][stage]), t))
                for mask, h, slot in fold_places(stage)]

    def fold_z_copies(u):
        c, part = u
        copies = []
        for k in z_range:
            target = lax.rem(t + k + 1, n_t)
            place = grad_rows(u, 0).at[:, pl.ds(pl.multiple_of(target * width, width), width)]
            copies.append(remote(place, z_buf.at[c, k, part_rows(part)], r.fz_send.at[0],
                                 r.fz_recv.at[c, part], z_peers[k]))
        return copies

    piece = 16
    per_part = rows_w // CUTS // piece

    def fold_start(c):
        for part in range(CUTS):
            start_all(core_copies((c, part)))

    def fold_step(c, stage, go=True):
        for part in range(CUTS):
            fold_unit((c, part), stage, go)

    def fold_send(c):
        for part in range(CUTS):
            start_all(fold_z_copies((c, part)))

    def fold_unit(u, stage, go=True):
        c, cut = u
        ref = grad_chunk(c)
        if stage == 0:
            settled(core_buf.at[c, :, part_rows(cut)], r.core_recv.at[c, cut], before)
            for k, mask in enumerate(groups):
                base = flip(d, mask) * rows_w

                def add_core(step, k=k, base=base):
                    step = step + cut * per_part
                    part = pl.ds(pl.multiple_of(base + step * piece, piece), piece)
                    ref[part, :] = (ref[part, :].astype(f32)
                                    + core_buf[c, k, block_of(step, piece), :].astype(f32)).astype(bf16)
                loop(per_part, add_core)
        elif stage <= n_link:
            places = fold_places(stage - 1)
            first_slot, count = places[0][2], len(places) // 2
            settled(dp_buf.at[c, :, pl.ds(first_slot, count), part_rows(cut)], r.fd_recv.at[c, cut, stage - 1], before)
            for mask, h, slot in places:
                base = flip(d, mask) * rows_w
                cols = pl.ds(h * half, half)

                def add_dp(step, base=base, cols=cols, h=h, slot=slot):
                    step = step + cut * per_part
                    part = pl.ds(pl.multiple_of(base + step * piece, piece), piece)
                    ref[part, cols] = (ref[part, cols].astype(f32)
                                       + dp_buf[c, h, slot, block_of(step, piece), :].astype(f32)).astype(bf16)
                loop(per_part, add_dp)
        else:
            settled(z_buf.at[c, :, part_rows(cut)], r.fz_recv.at[c, cut], before)

            def finish(step):
                step = step + cut * per_part
                part = pl.ds(pl.multiple_of(d * rows_w + step * piece, piece), piece)
                total = ref[part, block_of(t, width)].astype(f32)
                for k in z_range:
                    total = total + z_buf[c, k, block_of(step, piece), :].astype(f32)
                here = block_of(step, piece)
                if c == 2:
                    for k in range(4):
                        r.g_at[k, here, :] = total[:, k * w:(k + 1) * w]
                elif c == 3:
                    for k in range(2):
                        r.g_cw[here, k, :] = total[:, k * w:(k + 1) * w]
                    r.g_ao[here, :] = total[:, 2 * w:3 * w]
                    r.g_co[here, :] = total[:, 3 * w:4 * w]
                else:
                    grads[c][here, :] = total
            loop(per_part, finish)
            if cut == CUTS - 1:
                leave(*((r.g_at,) if c == 2 else (r.g_cw, r.g_ao, r.g_co) if c == 3 else (grads[c],)))
        if stage < n_link and go:
            start_all(fold_copies(u, stage))
        elif stage == n_link and go:
            start_all(fold_z_copies(u))

    grads = {0: r.g_fu, 1: r.g_fd, 4: r.g_su, 5: r.g_sd}
    final = n_link + 1
    fold_plan_one = [[], [(5, stage) for stage in range(2, n_link + 1)], [(4, 1), (3, 0)]]

    dz_turn[...] = turned(dz[...])
    a_turn[...] = turned(a4[...])
    units = [(c, part) for c in range(CHUNKS) for part in range(CUTS)]
    settled(wbuf.at[0, pl.ds(0, CHUNKS * rows_w), pl.ds(0, (n_t - 1) * width)], r.z_send.at[0], before)
    for c in range(CHUNKS):
        settled(wbuf.at[0, pl.ds(0, (n_dp - 1) * rows_w), :], r.d_send.at[c], before)
    feed_back(dz, dz_turn, a_turn, wbuf.at[4], wbuf.at[5], z_s, r.hid2, r.slope2, grad_chunk(4), grad_chunk(5),
              lambda: fold_start(5), lambda: None)
    fold_start(4)
    join_norm(3, lambda part: x3[part, :], 1.0)

    dz_turn[...] = turned(dz[...])

    def act_back(j):
        mean, inverse, bn_gain, bn_shift = bn_parts(j)
        grad_act = dot(dz[...], wbuf[3, :, block_of(j, width)][:, 3 * w:4 * w], 1, 0)
        scaled = bhat[j, inner, :]
        normal = scaled * bn_gain + bn_shift
        sig_n = sigmoid(normal)
        value = grad_act * (sig_n * (1.0 + normal * (1.0 - sig_n)))
        dbn[j, inner, :] = value
        sums[1, pl.ds(2 * j, 1), :] = jnp.sum(value * scaled, axis=0, keepdims=True)
        sums[1, pl.ds(2 * j + 1, 1), :] = jnp.sum(value, axis=0, keepdims=True)
    loop(n_t, act_back)
    start_all(sum_copies(1))
    edge_start(dbn, 2)
    sum_middle(1)
    fold_step(5, 0)
    fold_step(4, 0, False)
    a_turn[...] = turned(a3[...])
    sum_end(1)
    for k, ref in ((1, bhat), (2, dbn)):
        edge_wait(ref, k)
    r.g_bn[...] = r.sum_out[1, pl.ds(2 * t, 2), :]
    leave(r.g_bn)
    small = r.small
    z_s[...] = jnp.zeros_like(z_s)

    def put_grad(c, j, first, value):
        if w % 128 == 0:
            grad_chunk(c)[:, pl.ds(pl.multiple_of(j * width + first, 128), value.shape[1])] = value
        else:
            old = grad_chunk(c)[:, block_of(j, width)]
            pieces = [old[:, :first], value, old[:, first + value.shape[1]:]]
            grad_chunk(c)[:, block_of(j, width)] = jnp.concatenate([p for p in pieces if p.shape[1] > 0], axis=1)

    def conv_back(j):
        mean, inverse, bn_gain, bn_shift = bn_parts(j)
        gamma = r.sum_out[1, pl.ds(2 * j, 1), :] / row_count
        beta = r.sum_out[1, pl.ds(2 * j + 1, 1), :] / row_count
        dbn[j] = bn_gain * inverse * (dbn[j] - beta - bhat[j] * gamma)
        dbn[j, pl.ds(0, EDGE), :] = jnp.where(t > 0, dbn[j, pl.ds(0, EDGE), :], 0.0)
        tail = pl.ds(EDGE + rows, EDGE)
        dbn[j, tail, :] = jnp.where(t < n_t - 1, dbn[j, tail, :], 0.0)

        def tap_step(k, carry):
            first = pl.multiple_of(k * size, size)
            own_part = dbn[j, pl.ds(first + EDGE, size), :]
            result = []
            for tap in range(KERNEL):
                term = own_part * glu[j, pl.ds(first + EDGE - HALF + tap, size), :]
                result.append(carry[tap] + jnp.sum(term.reshape(size // 8, 8, w), axis=0))
            return tuple(result)
        tap_sums = lax.fori_loop(0, rows // size, tap_step, tuple(jnp.zeros((8, w), f32) for _ in range(KERNEL)))
        for tap in range(KERNEL):
            small[j, tap:tap + 1, :] = jnp.sum(tap_sums[tap], axis=0, keepdims=True)

        def spread_step(k):
            first = pl.multiple_of(k * size, size)
            part = pl.ds(first, size)
            dglu = sweep(dbn, j, first, True)
            sig_p = sig[j, part, :]
            grad_val = dglu * sig_p
            r.de[part, 0:w] = grad_val.astype(bf16)
            r.de[part, w:2 * w] = (grad_val * val[j, part, :] * (1.0 - sig_p)).astype(bf16)
        loop(rows // size, spread_step)
        put_grad(3, j, 0, dot(a_turn[...], r.de[...], 1, 0).astype(bf16))
        put_grad(3, j, 3 * w, dot(dz_turn[...], act[j], 1, 0).astype(bf16))
        z_s[...] = z_s[...] + dot(r.de[...], wbuf[3, :, block_of(j, width)][:, 0:2 * w], 1, 1)

    def conv_middle():
        fold_step(5, 1)
        for part in range(CUTS):
            start_all(fold_copies((4, part), 0))
    loop(n_t, conv_back)
    conv_middle()
    join_norm(2, lambda part: x2[part, :], 1.0)

    dz_turn[...] = turned(dz[...])
    dmix_s, dmix_turn, cq_turn, dcq_s = r.dmix_s, r.dmix_turn, r.cq_turn, r.dcq_s
    a2_turn, rf_out, rf_buf = r.a2_turn, r.rf_out, r.rf_buf

    def mix_back(j):
        put_grad(3, j, 2 * w, dot(dz_turn[...], mix[j].astype(bf16), 1, 0).astype(bf16))
        dmix = dot(dz[...], wbuf[3, :, block_of(j, width)][:, 2 * w:3 * w], 1, 0) * inv_s[j]
        dmix_s[j] = dmix.astype(bf16)
        dmix_turn[j] = dmix.T.astype(bf16)
        cq_turn[j] = turned(cq[j])
        dcq_s[j] = jnp.zeros_like(dcq_s[j])
    loop(n_t, mix_back)
    fold_start(3)
    rf_copies = [remote(rf_out.at[k], rf_buf.at[k], r.rf_ss.at[k], r.rf_rs.at[k], z_peers[k]) for k in z_range]

    def keys_back(part, j):
        block = wbuf[2, :, block_of(j, width)]
        piece_rows = block_of(part, rows)
        k_p, v_p = kv[j, piece_rows, :][:, 0:w], kv[j, piece_rows, :][:, w:2 * w]
        product = dmix_s[j].astype(f32) * mix[j]
        for h in range(local_heads):
            mask = head_mask((rows, w), 1, head_dim, h)
            turn_mask = head_mask((w, rows), 0, head_dim, h)
            head = j * local_heads + h
            delta = jnp.sum(keep(mask, product), axis=-1, keepdims=True)
            p_h = probs[head, :, piece_rows]
            grad_p = dot(keep(mask, dmix_s[j]), v_p, 1, 1)
            ds = (p_h.astype(f32) * (grad_p - delta)).astype(bf16)
            probs[head, :, piece_rows] = ds
            dv_h = dot(keep(turn_mask, dmix_turn[j]), p_h, 1, 0)
            dk_h = dot(keep(turn_mask, cq_turn[j]), ds, 1, 0)
            dcq_h = keep(mask, dot(ds, k_p, 1, 0))
            if h == 0:
                dv, dk, dcq = dv_h, dk_h, dcq_h
            else:
                dv, dk, dcq = dv + dv_h, dk + dk_h, dcq + dcq_h
        dcq_s[j] = dcq_s[j] + dcq
        dkv = jnp.concatenate([(dk * scale).T, dv.T], axis=1).astype(bf16)
        kv[j, piece_rows, :] = dkv
        z_s[...] = z_s[...] + dot(dkv, block[:, w:3 * w], 1, 1)

    assert len(fold_plan_one) <= n_t
    for k in range(n_t):
        z_s[...] = jnp.zeros_like(z_s)
        part = lax.rem(t + 1 + k, n_t)
        loop(n_t, functools.partial(keys_back, part), 2)
        if k < n_t - 1:
            rf_out[k] = z_s[...].astype(bf16)
            rf_copies[k].start()
        for c, stage in fold_plan_one[k] if k < len(fold_plan_one) else ():
            fold_step(c, stage, stage < n_link)
    for part in range(n_t):
        a2_turn[:, part * rows:(part + 1) * rows] = turned(a2_all[part])
    small[:, KERNEL:, :] = jnp.zeros_like(small[:, KERNEL:, :])


    def queries_back(j):
        block = wbuf[2, :, block_of(j, width)]
        pq_turn = turned(pq[j])
        for h in range(local_heads):
            mask = head_mask((rows, w), 1, head_dim, h)
            turn_mask = head_mask((w, rows), 0, head_dim, h)
            back = dot(probs[j * local_heads + h], phase[...], 1, 0)
            spun(back[:, :D // 2], back[:, D // 2:])
            dpq_h = keep(mask, dot(u_s[...], block[:, 3 * w:4 * w], 1, 0))
            pos_h = dot(keep(turn_mask, pq_turn), u_s[...], 1, 0)
            if h == 0:
                dpq, pos = dpq_h, pos_h
            else:
                dpq, pos = dpq + dpq_h, pos + pos_h
        dcq = dcq_s[j] * scale
        dpq = dpq * scale
        small[j, KERNEL:KERNEL + 1, :] = jnp.sum(dcq, axis=0, keepdims=True)
        small[j, KERNEL + 1:KERNEL + 2, :] = jnp.sum(dpq, axis=0, keepdims=True)
        dq = (dcq + dpq).astype(bf16)
        z_s[...] = z_s[...] + dot(dq, block[:, 0:w], 1, 1)
        put_grad(2, j, 0, dot(a2_turn[:, block_of(t, rows)], dq, 1, 0).astype(bf16))
        put_grad(2, j, w, dot(a2_turn[...], kv[j], 1, 0).astype(bf16))
        put_grad(2, j, 3 * w, (pos.T * scale).astype(bf16))

    def fold_some(plan):
        for c, stage in plan:
            fold_step(c, stage, stage < n_link)
    middle_plan = [(4, stage) for stage in range(2, n_link + 1)]
    halves(n_t, queries_back, lambda: fold_some(middle_plan), 2)

    fold_start(2)
    small_z, small_mid, small_buf = r.small_z, r.small_mid, r.small_buf
    small_z_copies = [remote(small.at[lax.rem(t + k + 1, n_t)], small_z.at[k], r.sz_send.at[0], r.sz_recv.at[0],
                             z_peers[k]) for k in z_range]
    small_copies = [remote(small_mid, small_buf.at[k], r.s_send.at[0], r.s_recv.at[0], d_peers[k])
                    for k in range(n_dp - 1)]

    def small_middle():
        settled(small_z, r.sz_recv.at[0], before)
        total = small[t]
        for k in z_range:
            total = total + small_z[k]
        small_mid[...] = total
        start_all(small_copies)
    start_all(small_z_copies)
    a_turn[...] = turned(a1[...])
    fold_some([(3, 1)])
    fold_step(2, 0)
    fold_some([(3, stage) for stage in range(2, n_link + 1)])
    arrive_all(rf_copies)

    def join_rows(part):
        total = z_s[part, :]
        for k in z_range:
            total = total + rf_buf[k, part, :].astype(f32)
        z_s[part, :] = total
    row_loop(rows, NORM_ROWS, join_rows)
    join_norm(1, lambda part: x1[part, :], 0.5)
    for c in (5, 4, 3):
        fold_send(c)

    dz_turn[...] = turned(dz[...])
    def fold_middle():
        fold_step(1, 0)

    feed_back(dz, dz_turn, a_turn, wbuf.at[0], wbuf.at[1], z_s, r.hid1, r.slope1, grad_chunk(0), grad_chunk(1),
              lambda: fold_start(1), fold_middle)
    fold_start(0)
    join_norm(0, lambda part: x_ref[part, :].astype(f32), 1.0)
    leave(r.dx0)

    gsum_copies = [remote(gsum, r.gsum_buf.at[k], r.g_send.at[0], r.g_recv.at[0], d_peers[k])
                   for k in range(n_dp - 1)]
    gsum_z_copies = [remote(r.gsum_mid, r.gsum_z.at[k], r.gz_send.at[0], r.gz_recv.at[0], z_peers[k])
                     for k in z_range]
    start_all(gsum_copies)

    def gsum_middle():
        settled(r.gsum_buf, r.g_recv.at[0], before)
        total = gsum[...]
        for k in range(n_dp - 1):
            total = total + r.gsum_buf[k]
        r.gsum_mid[...] = total
        start_all(gsum_z_copies)
    small_middle()
    for u, stage, go, other in tail_plan(final):
        fold_unit(u, stage, go)
        if other is not None:
            start_all(fold_copies(other, 0))
        if (u, stage) == ((0, CUTS - 1), 1):
            gsum_middle()
    settled(small_buf, r.s_recv.at[0], before)
    total = small_mid[...]
    for k in range(n_dp - 1):
        total = total + small_buf[k]
    r.g_taps[...] = total[0:KERNEL, :]
    for pair in range(2):
        row = total[KERNEL + pair:KERNEL + pair + 1, :]
        for h in range(local_heads):
            place = lax.broadcasted_iota(jnp.int32, (n_bias, w), 1)
            spot_h = (place == lax.broadcasted_iota(jnp.int32, (n_bias, w), 0) + d * n_bias + h * head_dim).astype(f32)
            r.g_bias[pair, h:h + 1, :] = lax.dot_general(row, spot_h, (((1,), (1,)), ((), ())), precision=high,
                                                         preferred_element_type=f32)
    settled(r.gsum_z, r.gz_recv.at[0], before)
    total_g = r.gsum_mid[...]
    for k in z_range:
        total_g = total_g + r.gsum_z[k]
    spot_g = lax.dot_general(total_g, gain_spot, (((1,), (1,)), ((), ())), precision=high, preferred_element_type=f32)
    r.g_gains[...] = spot_g[0:5, :]

    leave(r.g_taps, r.g_bias, r.g_gains)
    for k, name in enumerate(leaving):
        pltpu.make_async_copy(getattr(r, name[:-len(HBM)]), getattr(r, name), r.out_sem.at[k]).wait()
    settled(taps.at[pl.ds(0, n_t - 1)], r.f_send.at[0], before)
    settled(a2_all.at[pl.ds(0, n_t - 1)], r.a_send.at[0], before)
    settled(small_z, r.sz_send.at[0], before)
    settled(r.gsum_z, r.gz_send.at[0], before)
    sent_all(rf_copies)
    settled(e_buf.at[pl.ds(0, n_t - 1)], r.e_send.at[0], before)
    sent_all(e_copies(n_t - 1, n_t + n_link))
    for k in range(2):
        settled(sum_buf.at[k], r.sum_send.at[k], before)
        settled(sum_z.at[k], r.sumz_send.at[k], before)
    settled(small_buf, r.s_send.at[0], before)
    settled(r.gsum_buf, r.g_send.at[0], before)
    settled(gbuf.at[pl.ds(0, CHUNKS // 2)], r.core_send.at[0], before)
    settled(gbuf.at[0, pl.ds(0, CHUNKS * rows_w), pl.ds(0, (n_t - 1) * width)], r.fz_send.at[0], before)
    for c in range(CHUNKS):
        settled(gbuf.at[0, pl.ds(0, (len(groups) - 1) * rows_w), :], r.fd_send.at[c], before)


def layer_kernel(n_dp, n_t, head_dim, inputs):
    given = SimpleNamespace(**inputs)
    rows, D = given.x.shape
    rows_w, width = given.fu.shape
    w = D // n_t
    frames = rows * n_t
    heads = D // head_dim
    hidden = n_t * width
    n_bits = n_dp.bit_length() - 1
    n_e = n_t - 1 + n_bits
    n_gain = given.gain_in.shape[1]
    n_bias = given.bias_in.shape[2]
    tap_rows = 40
    groups = n_dp // 2
    z = n_t - 1
    sem = pltpu.SemaphoreType.DMA
    vm = pltpu.VMEM
    outs = dict(
        out=((rows, D), f32), dx0=((rows, D), f32), g_gains=((5, n_gain), f32), g_fu=((rows_w, width), f32),
        g_fd=((rows_w, width), f32), g_at=((4, rows_w, w), f32), g_ao=((rows_w, w), f32),
        g_bias=((2, w // head_dim, n_bias), f32), g_cw=((rows_w, 2, w), f32), g_taps=((KERNEL, w), f32),
        g_bn=((2, w), f32), g_co=((rows_w, w), f32), g_su=((rows_w, width), f32), g_sd=((rows_w, width), f32))
    edge_shape = (n_t, rows + 2 * EDGE, w)
    scratch = dict(
        pack=vm((2, rows_w, width), bf16), taps_own=vm((tap_rows, w), f32), wbuf=vm((CHUNKS, n_dp * rows_w, hidden), bf16),
        gbuf=vm((CHUNKS - 2, n_dp * rows_w, hidden), bf16), gains=vm((8, D), f32),
        taps=vm((n_t, tap_rows, w), f32), e_acc=vm((n_bits + 2, 8, D), f32), e_buf=vm((n_e, 8, D), f32),
        phase=vm((frames, D), bf16), spin=vm((2, rows, D // 2), f32), u_s=vm((rows, D), bf16),
        z_s=vm((rows, D), f32), x1=vm((rows, D), f32), x2=vm((rows, D), f32),
        x3=vm((rows, D), f32), a1=vm((rows, D), bf16), a2=vm((rows, D), bf16), a3=vm((rows, D), bf16),
        a4=vm((rows, D), bf16), dz=vm((rows, D), bf16), dz_turn=vm((D, rows), bf16),
        a_turn=vm((D, rows), bf16), a2_all=vm((n_t, rows, D), bf16), a2_turn=vm((D, frames), bf16),
        hid1=vm((rows, hidden), bf16), slope1=vm((rows, hidden), bf16), hid2=vm((rows, hidden), bf16),
        slope2=vm((rows, hidden), bf16), kv=vm((n_t, frames, 2 * w), bf16), cq=vm((n_t, rows, w), bf16),
        pq=vm((n_t, rows, w), bf16), mix=vm((n_t, rows, w), f32), inv_s=vm((n_t, rows, w), f32), probs=vm((heads, rows, frames), bf16),
        s_s=vm((rows, frames), f32), dmix_s=vm((n_t, rows, w), bf16), dmix_turn=vm((n_t, w, rows), bf16),
        cq_turn=vm((n_t, w, rows), bf16), dcq_s=vm((n_t, rows, w), f32),
        rf_out=vm((z, rows, D), bf16), rf_buf=vm((z, rows, D), bf16),
        glu=vm(edge_shape, f32), bhat=vm(edge_shape, f32), dbn=vm(edge_shape, f32),
        val=vm((n_t, rows, w), f32), sig=vm((n_t, rows, w), f32), act=vm((n_t, rows, w), bf16),
        de=vm((rows, 2 * w), bf16), sums=vm((2, 2 * n_t, w), f32), sum_mid=vm((2, 2 * n_t, w), f32),
        sum_out=vm((2, 2 * n_t, w), f32), sum_buf=vm((2, n_dp - 1, 2 * n_t, w), f32),
        sum_z=vm((2, z, 2 * n_t, w), f32), core_buf=vm((CHUNKS, groups, rows_w, hidden), bf16),
        dp_buf=vm((CHUNKS, 2, groups - 1, rows_w, hidden // 2), bf16), z_buf=vm((CHUNKS, z, rows_w, width), bf16),
        small=vm((n_t, tap_rows, w), f32), small_buf=vm((n_dp - 1, tap_rows, w), f32),
        small_mid=vm((tap_rows, w), f32), small_z=vm((z, tap_rows, w), f32), gsum=vm((8, D), f32),
        gsum_buf=vm((n_dp - 1, 8, D), f32), gsum_mid=vm((8, D), f32), gsum_z=vm((z, 8, D), f32), local_sem=sem((CHUNKS, CUTS)))
    n_link = n_bits - 1
    scratch.update(
        z_send=sem((1,)), z_recv=sem((CHUNKS, CUTS)), d_send=sem((CHUNKS,)), d_recv=sem((CHUNKS, CUTS, n_bits)),
        f_send=sem((1,)), f_recv=sem((1,)), e_send=sem((n_bits + 1,)), e_recv=sem((n_bits + 1,)),
        a_send=sem((1,)), a_recv=sem((1,)), edge_send=sem((3, 2)), edge_recv=sem((3, 2)),
        sum_send=sem((2,)), sum_recv=sem((2,)), sumz_send=sem((2,)), sumz_recv=sem((2,)),
        core_send=sem((1,)), core_recv=sem((CHUNKS, CUTS)), fd_send=sem((CHUNKS,)),
        fd_recv=sem((CHUNKS, CUTS, n_link)), fz_send=sem((1,)), fz_recv=sem((CHUNKS, CUTS)),
        rf_ss=sem((z,)), rf_rs=sem((z,)), s_send=sem((1,)), s_recv=sem((1,)),
        sz_send=sem((1,)), sz_recv=sem((1,)), g_send=sem((1,)), g_recv=sem((1,)),
        gz_send=sem((1,)), gz_recv=sem((1,)))
    for name, (dims, kind) in outs.items():
        scratch[name] = vm(dims, kind)
    scratch.update(out_sem=sem((len(outs),)))
    names = list(inputs) + [name + HBM for name in outs] + list(scratch)
    vmem = pl.BlockSpec(memory_space=pltpu.VMEM)
    result = pl.pallas_call(
        functools.partial(layer_body, names, n_dp, n_t, head_dim),
        name="layer",
        out_shape=tuple(jax.ShapeDtypeStruct(dims, kind) for dims, kind in outs.values()),
        in_specs=[vmem] * len(inputs),
        out_specs=(pl.BlockSpec(memory_space=pl.ANY),) * len(outs),
        scratch_shapes=list(scratch.values()),
        compiler_params=pltpu.CompilerParams(collective_id=0, has_side_effects=True, vmem_limit_bytes=67043328),
    )(*inputs.values())
    return result


def settle_body(*refs):
    count = (len(refs) - 2) // 3
    sources, results, rooms = refs[:count], refs[count:2 * count], refs[2 * count:3 * count]
    sem_in, sem_out = refs[3 * count:]
    loads = [pltpu.make_async_copy(a, b, sem_in.at[k]) for k, (a, b) in enumerate(zip(sources, rooms))]
    stores = [pltpu.make_async_copy(a, b, sem_out.at[k]) for k, (a, b) in enumerate(zip(rooms, results))]
    for copy in loads:
        copy.start()
    for load, store in zip(loads, stores):
        load.wait()
        store.start()
    for copy in stores:
        copy.wait()


def settle(arrays):
    hbm = pl.BlockSpec(memory_space=pl.ANY)
    count = len(arrays)
    sem = pltpu.SemaphoreType.DMA
    return pl.pallas_call(
        settle_body,
        name="settle",
        out_shape=tuple(jax.ShapeDtypeStruct(a.shape, a.dtype) for a in arrays),
        in_specs=[hbm] * count,
        out_specs=(hbm,) * count,
        scratch_shapes=[pltpu.VMEM(a.shape, a.dtype) for a in arrays] + [sem((count,)), sem((count,))],
    )(*arrays)


def angle_tables(frames, width):
    step = 32
    frequency = np.exp(np.arange(width // 2) * (-2.0 * math.log(10000.0) / width))
    coarse = np.arange(frames // step)[:, None] * step * frequency
    fine = np.arange(step)[:, None] * frequency
    return jnp.asarray(np.stack([np.sin(coarse), np.cos(coarse), np.sin(fine), np.cos(fine)]), f32)


def per_device(n_dp, n_t, inputs, out_grad, norm_gains, first_up, first_down, attend_in, attend_out, position_bias,
               convolve_in, depth_kernel, batch_norm, convolve_out, second_up, second_down):
    rows, D = inputs.shape
    w = attend_in.shape[2]
    R = attend_in.shape[1]
    n_bias = position_bias.shape[2]
    head_dim = n_bias * n_dp
    got = layer_kernel(n_dp, n_t, head_dim, dict(
        fu=first_up, fd=first_down.T, at=attend_in, cw=convolve_in, ao=attend_out.T, co=convolve_out.T, su=second_up,
        sd=second_down.T, gain_in=norm_gains, bias_in=position_bias, tap_in=depth_kernel.T, bn_in=batch_norm, x=inputs,
        og=out_grad, tab=angle_tables(rows * n_t, D)))
    (out, dx0, g_gains, g_fu, g_fd, g_at, g_ao, g_bias, g_cw, g_taps, g_bn, g_co, g_su, g_sd) = settle(got)
    return (out, dx0, g_gains, g_fu, g_fd.T, g_at, g_ao.T, g_bias, g_cw, g_taps.T, g_bn, g_co.T, g_su, g_sd.T)


def solution(mesh):
    n_dp, n_t = mesh.shape["dp"], mesh.shape["tensor"]
    row = P(("dp", "tensor"), None)
    gain = P(None, ("dp", "tensor"))
    up = P("dp", "tensor")
    down = P("tensor", "dp")
    weights = (up, down, P(None, "dp", "tensor"), down, P(None, "tensor", "dp"), P("dp", None, "tensor"),
               P("tensor", None), P(None, "tensor"), down, up, down)
    return jax.shard_map(
        functools.partial(per_device, n_dp, n_t), mesh=mesh,
        in_specs=(row, row, gain) + weights,
        out_specs=(row, row, gain) + weights,
        check_vma=False)
```

```python
import functools
import math
from types import SimpleNamespace

import jax
import jax.numpy as jnp
import numpy as np
from jax import lax
from jax.experimental import pallas as pl
from jax.experimental.pallas import tpu as pltpu
from jax.sharding import PartitionSpec as P

MESH = pl.DeviceIdType.MESH
CHUNKS = 6
CUTS = 2
AHEAD = 2
CORE = 1
EDGE = 16
KERNEL = 31
HALF = KERNEL // 2
norm_eps = 1e-05
f32 = jnp.float32
bf16 = jnp.bfloat16
high = lax.Precision.HIGHEST


def flip(index, mask):
    result = index
    bit = 1
    while bit <= mask:
        if mask & bit:
            result = result + bit - 2 * bit * ((index // bit) % 2)
        bit *= 2
    return result


def span(bits):
    masks = [0]
    for bit in bits:
        masks = masks + [mask ^ bit for mask in masks]
    return masks


def link_orders(n_dp):
    bits = [1 << k for k in range(1, n_dp.bit_length() - 1)]
    return (bits, bits[::-1])


def greet(peers):
    barrier = pltpu.get_barrier_semaphore()
    for peer in peers:
        pl.semaphore_signal(barrier, inc=1, device_id=peer, device_id_type=MESH)
    pl.semaphore_wait(barrier, len(peers))


def remote(src, dst, send_sem, recv_sem, peer):
    return pltpu.make_async_remote_copy(
        src_ref=src, dst_ref=dst, send_sem=send_sem, recv_sem=recv_sem,
        device_id=peer, device_id_type=MESH)


def start_all(copies):
    for copy in copies:
        copy.start()


def settled(ref, sem, peer):
    remote(ref, ref, sem, sem, peer).wait_recv()


def arrive_all(copies):
    for copy in copies:
        copy.wait_recv()


def sent_all(copies):
    for copy in copies:
        copy.wait_send()


def dot(left, right, left_dim, right_dim):
    return lax.dot_general(left, right, (((left_dim,), (right_dim,)), ((), ())), preferred_element_type=f32)


def turned(value):
    return value.astype(f32).T.astype(bf16)


def head_mask(shape, axis, head_dim, head):
    place = lax.broadcasted_iota(jnp.int32, shape, axis)
    return (place >= head * head_dim) & (place < (head + 1) * head_dim)


def keep(mask, value):
    return jnp.where(mask, value, jnp.zeros_like(value))


def block_of(k, size):
    return pl.ds(pl.multiple_of(k * size, size), size)


def loop(count, body, unroll=1):
    def step(k, carry):
        body(k)
        return carry
    lax.fori_loop(0, count, step, 0, unroll=unroll)


def halves(count, body, between, unroll=1):
    loop(count // 2, body, unroll)
    between()
    loop(count - count // 2, lambda k: body(k + count // 2), unroll)


def row_loop(rows, size, body):
    loop(rows // size, lambda k: body(block_of(k, size)))


def sigmoid(values):
    return 1.0 / (1.0 + jnp.exp(-values))


def norm_parts(values):
    centred = values - jnp.mean(values, axis=-1, keepdims=True)
    inverse = lax.rsqrt(jnp.mean(centred * centred, axis=-1, keepdims=True) + norm_eps)
    return centred * inverse, inverse


def norm_back(value, incoming, gain_row):
    scaled, inverse = norm_parts(value)
    grad_scaled = incoming * gain_row
    inner = jnp.mean(grad_scaled * scaled, axis=-1, keepdims=True)
    grad_in = inverse * (grad_scaled - jnp.mean(grad_scaled, axis=-1, keepdims=True) - scaled * inner)
    return scaled, grad_in, jnp.sum(incoming * scaled, axis=0, keepdims=True)


def tail_plan(final):
    parts = range(CUTS)
    last = CUTS - 1
    plan = [((2, part), 1, True, None) for part in parts] + [((0, part), 0, False, None) for part in parts]
    plan += [((1, part), 1, True, (0, 0) if part == 0 else None) for part in parts]
    for stage in range(2, final):
        plan += [((2, part), stage, True, None) for part in parts]
    for stage in range(2, final):
        plan += [((1, part), stage, True, (0, last) if (stage, part) == (2, 0) else None) for part in parts]
    for stage in range(1, final):
        plan += [((0, part), stage, True, None) for part in parts]
    return plan + [((c, part), final, True, None) for c in (5, 4, 3, 2, 1, 0) for part in parts]


def relay_order(stages):
    hop, link_free, order = 1.5, 0.0, []
    units = [(c, part) for c in range(CHUNKS) for part in range(CUTS)]
    waiting = [(7.0 + 6.5 / CUTS * (k + 1), 0, u) for k, u in enumerate(units)]
    while waiting:
        waiting.sort()
        now, stage, u = waiting.pop(0)
        order.append((now, stage, u))
        if stage < stages - 1:
            link_free = max(now, link_free) + 3.1 / CUTS * 2 ** stage
            waiting.append((link_free + hop, stage + 1, u))
        elif stage == stages - 1:
            waiting.append((now + hop + 2.0 / CUTS, stages, u))
    return order


SLAB = 512
NORM_ROWS = 256
HBM = "_hbm"


def feed_rows(a_ref, up, down_t, z_ref, hidden, slope):
    z_ref[...] = jnp.zeros_like(z_ref)

    def step(k):
        cols = block_of(k, SLAB)
        pre = dot(a_ref[...], up[:, cols], 1, 0)
        sig = sigmoid(pre)
        hidden[:, cols] = (pre * sig).astype(bf16)
        slope[:, cols] = (sig * (1.0 + pre * (1.0 - sig))).astype(bf16)
        z_ref[...] = z_ref[...] + dot(hidden[:, cols], down_t[:, cols], 1, 1)
    loop(up.shape[1] // SLAB, step, 2)


def feed_back(dz_ref, dz_turn, a_turn, up, down_t, z_ref, hidden, slope, g_up, g_down, start_down, middle):
    z_ref[...] = jnp.zeros_like(z_ref)

    def first_step(k):
        cols = block_of(k, SLAB)
        g_down[:, cols] = dot(dz_turn[...], hidden[:, cols], 1, 0).astype(bf16)
    loop(up.shape[1] // SLAB, first_step)
    start_down()
    slabs = up.shape[1] // SLAB

    def step(k):
        cols = block_of(k, SLAB)
        grad_pre = (dot(dz_ref[...], down_t[:, cols], 1, 0) * slope[:, cols].astype(f32)).astype(bf16)
        g_up[:, cols] = dot(a_turn[...], grad_pre, 1, 0).astype(bf16)
        z_ref[...] = z_ref[...] + dot(grad_pre, up[:, cols], 1, 1)
    loop(slabs - 1, step, slabs - 1)
    middle()
    step(slabs - 1)


def layer_body(names, n_dp, n_t, head_dim, *all_refs):
    r = SimpleNamespace(**dict(zip(names, all_refs)))
    d = lax.axis_index("dp")
    t = lax.axis_index("tensor")
    pack, wbuf, gbuf = r.pack, r.wbuf, r.gbuf
    x_ref, gains, taps = r.x, r.gains, r.taps
    rows_w, width = pack.shape[1], pack.shape[2]
    rows, D = x_ref.shape
    w = D // n_t
    half = n_t * width // 2
    frames = rows * n_t
    local_heads = w // head_dim
    n_gain = r.gain_in.shape[1]
    n_bias = n_gain // local_heads
    row_count = frames * n_dp
    scale = head_dim ** -0.5
    links = link_orders(n_dp)
    orders = [order + [CORE] for order in links]
    stages = len(orders[0])
    n_link = len(links[0])
    z_peers = [(d, lax.rem(t + step, n_t)) for step in range(1, n_t)]
    d_peers = [(flip(d, mask), t) for mask in range(1, n_dp)]
    before = (d, lax.rem(t + n_t - 1, n_t))
    after = (d, lax.rem(t + 1, n_t))
    z_range = range(n_t - 1)
    leaving = [name for name in names if name.endswith(HBM)]

    def leave(*chosen):
        for ref in chosen:
            name = [one for one in leaving if getattr(r, one[:-len(HBM)]) is ref][0]
            k = leaving.index(name)
            pltpu.make_async_copy(ref, getattr(r, name), r.out_sem.at[k]).start()

    greet(z_peers + d_peers)

    def window(u, mask, start, size):
        c, part = u
        count = rows_w // CUTS
        first = pl.multiple_of(flip(d, mask) * rows_w + part * count, count)
        return wbuf.at[c, pl.ds(first, count), pl.ds(start, size)]

    def own(u):
        return window(u, 0, pl.multiple_of(t * width, width), width)

    def source(u):
        count = rows_w // CUTS
        return sources[u[0]].at[pl.ds(u[1] * count, count), :]

    sources = (r.fu, r.fd, pack.at[0], pack.at[1], r.su, r.sd)

    def z_copies(u):
        return [remote(source(u), own(u), r.z_send.at[0], r.z_recv.at[u[0], u[1]], z_peers[k])
                for k in z_range]

    def local_copy(u):
        return pltpu.make_async_copy(source(u), own(u), r.local_sem.at[u[0], u[1]])

    def dp_copies(u, stage):
        copies = []
        for h in range(2):
            bit = orders[h][stage]
            masks = span(orders[h][:stage])
            for mask in masks:
                part = window(u, mask, h * half, half)
                copies.append(remote(part, part, r.d_send.at[u[0]], r.d_recv.at[u[0], u[1], stage],
                                     (flip(d, bit), t)))
        return copies

    def send_unit(u):
        local_copy(u).start()
        start_all(z_copies(u))

    def allowed(done):
        return AHEAD + done + max(0, done - 3)

    queue = [(c, part) for c in range(CHUNKS) for part in range(CUTS)]

    e_acc, e_buf = r.e_acc, r.e_buf

    def e_copies(first, stop):
        copies = []
        for k in range(first, stop):
            if k < n_t - 1:
                source, peer = e_acc.at[0], z_peers[k]
            else:
                source, peer = e_acc.at[k - n_t + 2], (flip(d, orders[0][k - n_t + 1]), t)
            sem = max(0, k - n_t + 2)
            copies.append(remote(source, e_buf.at[k], r.e_send.at[sem], r.e_recv.at[sem], peer))
        return copies

    taps_own = r.taps_own
    tap_copies = [remote(taps_own, taps.at[t], r.f_send.at[0], r.f_recv.at[0], z_peers[k]) for k in z_range]

    entry = lax.broadcasted_iota(jnp.int32, (n_gain, D), 0)
    lane = lax.broadcasted_iota(jnp.int32, (n_gain, D), 1)
    gain_spot = (lane == (d * n_t + t) * n_gain + entry).astype(f32)
    e_acc[0] = jnp.zeros_like(e_acc[0])
    e_acc[0, 0:5, :] = jnp.dot(r.gain_in[...], gain_spot, precision=high, preferred_element_type=f32)
    entry_b = lax.broadcasted_iota(jnp.int32, (n_bias, D), 0)
    lane_b = lax.broadcasted_iota(jnp.int32, (n_bias, D), 1)
    bias_spots = [(lane_b == entry_b + d * n_bias + (h + t * local_heads) * head_dim).astype(f32)
                  for h in range(local_heads)]
    for pair in range(2):
        row = None
        for h in range(local_heads):
            term = jnp.dot(r.bias_in[pair, h:h + 1, :].astype(f32), bias_spots[h], precision=high,
                           preferred_element_type=f32)
            row = term if row is None else row + term
        e_acc[0, 5 + pair:6 + pair, :] = row
    start_all(e_copies(0, n_t - 1))
    for u in queue[:AHEAD]:
        send_unit(u)
    for k in range(4):
        pack[0, :, k * w:(k + 1) * w] = r.at[k]
    for k in range(2):
        pack[1, :, k * w:(k + 1) * w] = r.cw[:, k, :]
    pack[1, :, 2 * w:3 * w] = r.ao[...]
    pack[1, :, 3 * w:4 * w] = r.co[...]
    taps_own[...] = jnp.zeros_like(taps_own)
    taps_own[0:KERNEL, :] = r.tap_in[...]
    taps_own[KERNEL:KERNEL + 2, :] = r.bn_in[...]
    start_all(tap_copies)
    taps[t] = taps_own[...]

    def relay(stage, u):
        count = rows_w // CUTS
        if stage == 0:
            local_copy(u).wait()
            settled(wbuf.at[0, pl.ds(0, count), pl.ds(0, (n_t - 1) * width)], r.z_recv.at[u[0], u[1]], before)
            place = queue.index(u)
            for other in queue[allowed(place):allowed(place + 1)]:
                send_unit(other)
        else:
            settled(wbuf.at[0, pl.ds(0, count * 2 ** (stage - 1)), :], r.d_recv.at[u[0], u[1], stage - 1], before)
        if stage < stages:
            start_all(dp_copies(u, stage))

    def ready_after(order, chunks):
        places = [k + 1 for k, (_, stage, u) in enumerate(order) if stage == stages and u[0] in chunks]
        return max(places, default=0)

    e_step = [0]

    def e_next():
        k = e_step[0]
        if k == 0:
            settled(e_buf.at[pl.ds(0, n_t - 1)], r.e_recv.at[0], before)
            total = e_acc[0]
            for i in z_range:
                total = total + e_buf[i]
            e_acc[1] = total
        elif k <= n_link + 1:
            arrive_all(e_copies(n_t - 2 + k, n_t - 1 + k))
            e_acc[k + 1] = e_acc[k] + e_buf[n_t - 2 + k]
        if k <= n_link:
            start_all(e_copies(n_t - 1 + k, n_t + k))
        e_step[0] = k + 1

    tab, phase, spin = r.tab, r.phase, r.spin
    step_t = tab.shape[1]

    def table(k):
        cs, cc = tab[0, pl.ds(k, 1), :], tab[1, pl.ds(k, 1), :]
        part = block_of(k, step_t)
        phase[part, 0:D // 2] = (cs * tab[3] + cc * tab[2]).astype(bf16)
        phase[part, D // 2:D] = (cc * tab[3] - cs * tab[2]).astype(bf16)
    loop(frames // step_t, table)

    def own_table(k):
        place = t * (rows // step_t) + k
        cs, cc = tab[0, pl.ds(place, 1), :], tab[1, pl.ds(place, 1), :]
        part = block_of(k, step_t)
        spin[0, part, :] = cs * tab[3] + cc * tab[2]
        spin[1, part, :] = cc * tab[3] - cs * tab[2]
    loop(rows // step_t, own_table)

    def spun(sines, cosines):
        u_s = r.u_s
        u_s[:, 0:D // 2] = (cosines * spin[0] - sines * spin[1]).astype(bf16)
        u_s[:, D // 2:D] = (sines * spin[0] + cosines * spin[1]).astype(bf16)

    z_s, a1, a2, a2_all = r.z_s, r.a1, r.a2, r.a2_all
    x1, x2, x3 = r.x1, r.x2, r.x3
    events = relay_order(stages)
    ready = ready_after(events, (0, 1))
    for k, (_, stage, u) in enumerate(events[:ready]):
        relay(stage, u)
        if k % 4 == 3 and e_step[0] < n_link + 2:
            e_next()
    while e_step[0] < n_link + 2:
        e_next()
    gains[...] = e_acc[n_link + 2]

    def norm_one(part):
        a1[part, :] = (norm_parts(x_ref[part, :].astype(f32))[0] * gains[0:1, :]).astype(bf16)
    row_loop(rows, NORM_ROWS, norm_one)
    feed_rows(a1, wbuf.at[0], wbuf.at[1], z_s, r.hid1, r.slope1)

    def norm_two(part):
        value = x_ref[part, :].astype(f32) + 0.5 * z_s[part, :]
        x1[part, :] = value
        a2[part, :] = (norm_parts(value)[0] * gains[1:2, :]).astype(bf16)
    row_loop(rows, NORM_ROWS, norm_two)

    a_copies = [remote(a2, a2_all.at[t], r.a_send.at[0], r.a_recv.at[0], z_peers[k]) for k in z_range]
    start_all(a_copies)
    a2_all[t] = a2[...]
    for _, stage, u in events[ready:]:
        relay(stage, u)
    settled(a2_all.at[pl.ds(0, n_t - 1)], r.a_recv.at[0], before)
    kv, cq, pq, probs, mix, s_s, u_s = r.kv, r.cq, r.pq, r.probs, r.mix, r.s_s, r.u_s
    z_s[...] = jnp.zeros_like(z_s)
    inv_s = r.inv_s
    scale_low = jnp.asarray(scale, bf16)

    def head_group(j):
        cols = block_of(j, width)
        block = wbuf[2, :, cols]
        for part in range(n_t):
            kv[j, part * rows:(part + 1) * rows, :] = dot(a2_all[part], block[:, w:3 * w], 1, 0).astype(bf16)
        q = dot(a2[...], block[:, 0:w], 1, 0)
        if w % 128 == 0:
            bias = gains[5:7, block_of(j, w)]
        else:
            bias = gains[5:7, 0:w]
            for other in range(1, n_t):
                bias = jnp.where(j == other, gains[5:7, other * w:(other + 1) * w], bias)
        cq_j = (q + bias[0:1]).astype(bf16)
        pq_j = (q + bias[1:2]).astype(bf16)
        cq[j] = cq_j
        pq[j] = pq_j
        for h in range(local_heads):
            mask = head_mask((rows, w), 1, head_dim, h)
            spread = dot(keep(mask, pq_j), block[:, 3 * w:4 * w], 1, 1)
            spun(spread[:, :D // 2] * scale, spread[:, D // 2:] * scale)
            s_s[...] = dot(u_s[...], phase[...], 1, 1) + dot(keep(mask, cq_j) * scale_low, kv[j, :, 0:w], 1, 1)
            head = j * local_heads + h

            s = s_s[...]
            e = jnp.exp(s - jnp.max(s, axis=-1, keepdims=True))
            inv = 1.0 / jnp.sum(e, axis=-1, keepdims=True)
            probs[head] = e.astype(bf16)
            mixed = dot(probs[head], kv[j, :, w:2 * w], 1, 0) * inv
            inv = jnp.broadcast_to(inv, (rows, w))
            inverse = inv if h == 0 else jnp.where(mask, inv, inverse)
            mixture = mixed if h == 0 else jnp.where(mask, mixed, mixture)
        mix[j] = mixture
        inv_s[j] = inverse
        z_s[...] = z_s[...] + dot(mixture.astype(bf16), wbuf[3, :, cols][:, 2 * w:3 * w], 1, 1)
    loop(n_t, head_group, 2)

    a3, glu, bhat, val, sig, act = r.a3, r.glu, r.bhat, r.val, r.sig, r.act
    dbn, sums, sum_buf, sum_mid, sum_z = r.dbn, r.sums, r.sum_buf, r.sum_mid, r.sum_z
    inner = pl.ds(EDGE, rows)

    def norm_three(part):
        value = x1[part, :] + z_s[part, :]
        x2[part, :] = value
        a3[part, :] = (norm_parts(value)[0] * gains[2:3, :]).astype(bf16)
    row_loop(rows, NORM_ROWS, norm_three)

    def gate(j):
        block = wbuf[3, :, block_of(j, width)]
        e = dot(a3[...], block[:, 0:2 * w], 1, 0)
        sig_j = sigmoid(e[:, w:2 * w])
        val[j] = e[:, 0:w]
        sig[j] = sig_j
        glu[j, inner, :] = e[:, 0:w] * sig_j
    loop(n_t, gate)

    def edge_copies(ref, k):
        first, last = pl.ds(EDGE, EDGE), pl.ds(rows, EDGE)
        return [remote(ref.at[:, first, :], ref.at[:, pl.ds(EDGE + rows, EDGE), :], r.edge_send.at[k, 0],
                       r.edge_recv.at[k, 0], before),
                remote(ref.at[:, last, :], ref.at[:, pl.ds(0, EDGE), :], r.edge_send.at[k, 1],
                       r.edge_recv.at[k, 1], after)]

    def edge_start(ref, k):
        back, ahead = edge_copies(ref, k)

        @pl.when(t > 0)
        def _():
            back.start()

        @pl.when(t < n_t - 1)
        def _():
            ahead.start()

        @pl.when(t == 0)
        def _():
            ref[:, pl.ds(0, EDGE), :] = jnp.zeros((n_t, EDGE, w), f32)

        @pl.when(t == n_t - 1)
        def _():
            ref[:, pl.ds(EDGE + rows, EDGE), :] = jnp.zeros((n_t, EDGE, w), f32)

    def edge_wait(ref, k):
        back, ahead = edge_copies(ref, k)

        @pl.when(t > 0)
        def _():
            ahead.wait_recv()
            back.wait_send()

        @pl.when(t < n_t - 1)
        def _():
            back.wait_recv()
            ahead.wait_send()

    def sum_copies(k):
        return [remote(sums.at[k], sum_buf.at[k, i], r.sum_send.at[k], r.sum_recv.at[k], d_peers[i])
                for i in range(n_dp - 1)]

    def sum_z_copies(k):
        return [remote(sum_mid.at[k], sum_z.at[k, i], r.sumz_send.at[k], r.sumz_recv.at[k], z_peers[i])
                for i in z_range]

    def sum_middle(k):
        settled(sum_buf.at[k], r.sum_recv.at[k], before)
        total = sums[k]
        for i in range(n_dp - 1):
            total = total + sum_buf[k, i]
        sum_mid[k] = total
        start_all(sum_z_copies(k))

    def sum_end(k):
        settled(sum_z.at[k], r.sumz_recv.at[k], before)
        total = sum_mid[k]
        for i in z_range:
            total = total + sum_z[k, i]
        sum_mid_out = r.sum_out
        sum_mid_out[k] = total

    edge_start(glu, 0)
    settled(taps.at[pl.ds(0, n_t - 1)], r.f_recv.at[0], before)
    edge_wait(glu, 0)
    size = 64

    def sweep(ref, j, first, backward):
        total = None
        for k in range(KERNEL):
            offset = EDGE - HALF + (KERNEL - 1 - k if backward else k)
            term = taps[j, k:k + 1, :] * ref[j, pl.ds(first + offset, size), :]
            total = term if total is None else total + term
        return total

    def convolve(j):
        def part_step(k, carry):
            first = pl.multiple_of(k * size, size)
            value = sweep(glu, j, first, False)
            bhat[j, pl.ds(first + EDGE, size), :] = value
            return (carry[0] + jnp.sum(value, axis=0, keepdims=True),
                    carry[1] + jnp.sum(value * value, axis=0, keepdims=True))
        zero = jnp.zeros((1, w), f32)
        one, two = lax.fori_loop(0, rows // size, part_step, (zero, zero))
        sums[0, pl.ds(2 * j, 1), :] = one
        sums[0, pl.ds(2 * j + 1, 1), :] = two
    loop(n_t, convolve)
    start_all(sum_copies(0))
    sum_middle(0)
    sum_end(0)

    def bn_parts(j):
        mean = r.sum_out[0, pl.ds(2 * j, 1), :] / row_count
        square = r.sum_out[0, pl.ds(2 * j + 1, 1), :] / row_count
        return mean, lax.rsqrt(square - mean * mean + norm_eps), taps[j, KERNEL:KERNEL + 1, :], taps[
            j, KERNEL + 1:KERNEL + 2, :]

    z_s[...] = jnp.zeros_like(z_s)

    def activate(j):
        mean, inverse, bn_gain, bn_shift = bn_parts(j)
        scaled = (bhat[j, inner, :] - mean) * inverse
        bhat[j, inner, :] = scaled
        normal = scaled * bn_gain + bn_shift
        act[j] = (normal * sigmoid(normal)).astype(bf16)
        z_s[...] = z_s[...] + dot(act[j], wbuf[3, :, block_of(j, width)][:, 3 * w:4 * w], 1, 1)
    loop(n_t, activate)
    edge_start(bhat, 1)

    a4, dx = r.a4, r.dx0

    def norm_four(part):
        value = x2[part, :] + z_s[part, :]
        x3[part, :] = value
        a4[part, :] = (norm_parts(value)[0] * gains[3:4, :]).astype(bf16)
    row_loop(rows, NORM_ROWS, norm_four)
    feed_rows(a4, wbuf.at[4], wbuf.at[5], z_s, r.hid2, r.slope2)
    gsum = r.gsum
    gsum[...] = jnp.zeros_like(gsum)
    dz, dz_turn, a_turn = r.dz, r.dz_turn, r.a_turn

    def add_gain(row, part_sum):
        gsum[row:row + 1, :] = gsum[row:row + 1, :] + part_sum

    def norm_five(part):
        value = x3[part, :] + 0.5 * z_s[part, :]
        scaled, grad_in, part_sum = norm_back(value, r.og[part, :].astype(f32), gains[4:5, :])
        r.out[part, :] = scaled * gains[4:5, :]
        dx[part, :] = grad_in
        dz[part, :] = (0.5 * grad_in).astype(bf16)
        add_gain(4, part_sum)
    row_loop(rows, NORM_ROWS, norm_five)
    leave(r.out)

    def grad_chunk(c):
        return gbuf.at[c - 2] if c >= 2 else wbuf.at[c + 4]

    def join_norm(row, x_of, factor):
        def step(part):
            _, grad_in, part_sum = norm_back(x_of(part), z_s[part, :], gains[row:row + 1, :])
            value = dx[part, :] + grad_in
            dx[part, :] = value
            dz[part, :] = (factor * value).astype(bf16)
            add_gain(row, part_sum)
        row_loop(rows, NORM_ROWS, step)

    folds = [order[::-1] for order in links]
    groups = span(links[0])
    core_buf, dp_buf, z_buf = r.core_buf, r.dp_buf, r.z_buf

    def grad_rows(u, mask):
        c, part = u
        count = rows_w // CUTS
        return grad_chunk(c).at[pl.ds(pl.multiple_of(flip(d, mask) * rows_w + part * count, count), count), :]

    def part_rows(part):
        return pl.ds(part * (rows_w // CUTS), rows_w // CUTS)

    def core_copies(u):
        return [remote(grad_rows(u, mask ^ CORE), core_buf.at[u[0], k, part_rows(u[1])],
                       r.core_send.at[0], r.core_recv.at[u[0], u[1]],
                       (flip(d, CORE), t)) for k, mask in enumerate(groups)]

    def fold_places(stage):
        places = []
        for h in range(2):
            masks = span(folds[h][stage + 1:])
            base = len(groups) - 2 * len(masks)
            places += [(mask, h, base + j) for j, mask in enumerate(masks)]
        return places

    def fold_copies(u, stage):
        c, part = u
        return [remote(grad_rows(u, mask ^ folds[h][stage]).at[:, pl.ds(h * half, half)],
                       dp_buf.at[c, h, slot, part_rows(part)],
                       r.fd_send.at[c], r.fd_recv.at[c, part, stage], (flip(d, folds[h][stage]), t))
                for mask, h, slot in fold_places(stage)]

    def fold_z_copies(u):
        c, part = u
        copies = []
        for k in z_range:
            target = lax.rem(t + k + 1, n_t)
            place = grad_rows(u, 0).at[:, pl.ds(pl.multiple_of(target * width, width), width)]
            copies.append(remote(place, z_buf.at[c, k, part_rows(part)], r.fz_send.at[0],
                                 r.fz_recv.at[c, part], z_peers[k]))
        return copies

    piece = 16
    per_part = rows_w // CUTS // piece

    def fold_start(c):
        for part in range(CUTS):
            start_all(core_copies((c, part)))

    def fold_step(c, stage, go=True):
        for part in range(CUTS):
            fold_unit((c, part), stage, go)

    def fold_send(c):
        for part in range(CUTS):
            start_all(fold_z_copies((c, part)))

    def fold_unit(u, stage, go=True):
        c, cut = u
        ref = grad_chunk(c)
        if stage == 0:
            settled(core_buf.at[c, :, part_rows(cut)], r.core_recv.at[c, cut], before)
            for k, mask in enumerate(groups):
                base = flip(d, mask) * rows_w

                def add_core(step, k=k, base=base):
                    step = step + cut * per_part
                    part = pl.ds(pl.multiple_of(base + step * piece, piece), piece)
                    ref[part, :] = (ref[part, :].astype(f32)
                                    + core_buf[c, k, block_of(step, piece), :].astype(f32)).astype(bf16)
                loop(per_part, add_core)
        elif stage <= n_link:
            places = fold_places(stage - 1)
            first_slot, count = places[0][2], len(places) // 2
            settled(dp_buf.at[c, :, pl.ds(first_slot, count), part_rows(cut)], r.fd_recv.at[c, cut, stage - 1], before)
            for mask, h, slot in places:
                base = flip(d, mask) * rows_w
                cols = pl.ds(h * half, half)

                def add_dp(step, base=base, cols=cols, h=h, slot=slot):
                    step = step + cut * per_part
                    part = pl.ds(pl.multiple_of(base + step * piece, piece), piece)
                    ref[part, cols] = (ref[part, cols].astype(f32)
                                       + dp_buf[c, h, slot, block_of(step, piece), :].astype(f32)).astype(bf16)
                loop(per_part, add_dp)
        else:
            settled(z_buf.at[c, :, part_rows(cut)], r.fz_recv.at[c, cut], before)

            def finish(step):
                step = step + cut * per_part
                part = pl.ds(pl.multiple_of(d * rows_w + step * piece, piece), piece)
                total = ref[part, block_of(t, width)].astype(f32)
                for k in z_range:
                    total = total + z_buf[c, k, block_of(step, piece), :].astype(f32)
                here = block_of(step, piece)
                if c == 2:
                    for k in range(4):
                        r.g_at[k, here, :] = total[:, k * w:(k + 1) * w]
                elif c == 3:
                    for k in range(2):
                        r.g_cw[here, k, :] = total[:, k * w:(k + 1) * w]
                    r.g_ao[here, :] = total[:, 2 * w:3 * w]
                    r.g_co[here, :] = total[:, 3 * w:4 * w]
                else:
                    grads[c][here, :] = total
            loop(per_part, finish)
            if cut == CUTS - 1:
                leave(*((r.g_at,) if c == 2 else (r.g_cw, r.g_ao, r.g_co) if c == 3 else (grads[c],)))
        if stage < n_link and go:
            start_all(fold_copies(u, stage))
        elif stage == n_link and go:
            start_all(fold_z_copies(u))

    grads = {0: r.g_fu, 1: r.g_fd, 4: r.g_su, 5: r.g_sd}
    final = n_link + 1
    fold_plan_one = [[], [(5, stage) for stage in range(2, n_link + 1)], [(4, 1), (3, 0)]]

    dz_turn[...] = turned(dz[...])
    a_turn[...] = turned(a4[...])
    units = [(c, part) for c in range(CHUNKS) for part in range(CUTS)]
    settled(wbuf.at[0, pl.ds(0, CHUNKS * rows_w), pl.ds(0, (n_t - 1) * width)], r.z_send.at[0], before)
    for c in range(CHUNKS):
        settled(wbuf.at[0, pl.ds(0, (n_dp - 1) * rows_w), :], r.d_send.at[c], before)
    feed_back(dz, dz_turn, a_turn, wbuf.at[4], wbuf.at[5], z_s, r.hid2, r.slope2, grad_chunk(4), grad_chunk(5),
              lambda: fold_start(5), lambda: None)
    fold_start(4)
    join_norm(3, lambda part: x3[part, :], 1.0)

    dz_turn[...] = turned(dz[...])

    def act_back(j):
        mean, inverse, bn_gain, bn_shift = bn_parts(j)
        grad_act = dot(dz[...], wbuf[3, :, block_of(j, width)][:, 3 * w:4 * w], 1, 0)
        scaled = bhat[j, inner, :]
        normal = scaled * bn_gain + bn_shift
        sig_n = sigmoid(normal)
        value = grad_act * (sig_n * (1.0 + normal * (1.0 - sig_n)))
        dbn[j, inner, :] = value
        sums[1, pl.ds(2 * j, 1), :] = jnp.sum(value * scaled, axis=0, keepdims=True)
        sums[1, pl.ds(2 * j + 1, 1), :] = jnp.sum(value, axis=0, keepdims=True)
    loop(n_t, act_back)
    start_all(sum_copies(1))
    edge_start(dbn, 2)
    sum_middle(1)
    fold_step(5, 0)
    fold_step(4, 0, False)
    a_turn[...] = turned(a3[...])
    sum_end(1)
    for k, ref in ((1, bhat), (2, dbn)):
        edge_wait(ref, k)
    r.g_bn[...] = r.sum_out[1, pl.ds(2 * t, 2), :]
    leave(r.g_bn)
    small = r.small
    z_s[...] = jnp.zeros_like(z_s)

    def put_grad(c, j, first, value):
        if w % 128 == 0:
            grad_chunk(c)[:, pl.ds(pl.multiple_of(j * width + first, 128), value.shape[1])] = value
        else:
            old = grad_chunk(c)[:, block_of(j, width)]
            pieces = [old[:, :first], value, old[:, first + value.shape[1]:]]
            grad_chunk(c)[:, block_of(j, width)] = jnp.concatenate([p for p in pieces if p.shape[1] > 0], axis=1)

    def conv_back(j):
        mean, inverse, bn_gain, bn_shift = bn_parts(j)
        gamma = r.sum_out[1, pl.ds(2 * j, 1), :] / row_count
        beta = r.sum_out[1, pl.ds(2 * j + 1, 1), :] / row_count
        dbn[j] = bn_gain * inverse * (dbn[j] - beta - bhat[j] * gamma)
        dbn[j, pl.ds(0, EDGE), :] = jnp.where(t > 0, dbn[j, pl.ds(0, EDGE), :], 0.0)
        tail = pl.ds(EDGE + rows, EDGE)
        dbn[j, tail, :] = jnp.where(t < n_t - 1, dbn[j, tail, :], 0.0)

        def tap_step(k, carry):
            first = pl.multiple_of(k * size, size)
            own_part = dbn[j, pl.ds(first + EDGE, size), :]
            result = []
            for tap in range(KERNEL):
                term = own_part * glu[j, pl.ds(first + EDGE - HALF + tap, size), :]
                result.append(carry[tap] + jnp.sum(term.reshape(size // 8, 8, w), axis=0))
            return tuple(result)
        tap_sums = lax.fori_loop(0, rows // size, tap_step, tuple(jnp.zeros((8, w), f32) for _ in range(KERNEL)))
        for tap in range(KERNEL):
            small[j, tap:tap + 1, :] = jnp.sum(tap_sums[tap], axis=0, keepdims=True)

        def spread_step(k):
            first = pl.multiple_of(k * size, size)
            part = pl.ds(first, size)
            dglu = sweep(dbn, j, first, True)
            sig_p = sig[j, part, :]
            grad_val = dglu * sig_p
            r.de[part, 0:w] = grad_val.astype(bf16)
            r.de[part, w:2 * w] = (grad_val * val[j, part, :] * (1.0 - sig_p)).astype(bf16)
        loop(rows // size, spread_step)
        put_grad(3, j, 0, dot(a_turn[...], r.de[...], 1, 0).astype(bf16))
        put_grad(3, j, 3 * w, dot(dz_turn[...], act[j], 1, 0).astype(bf16))
        z_s[...] = z_s[...] + dot(r.de[...], wbuf[3, :, block_of(j, width)][:, 0:2 * w], 1, 1)

    def conv_middle():
        fold_step(5, 1)
        for part in range(CUTS):
            start_all(fold_copies((4, part), 0))
    loop(n_t, conv_back)
    conv_middle()
    join_norm(2, lambda part: x2[part, :], 1.0)

    dz_turn[...] = turned(dz[...])
    dmix_s, dmix_turn, cq_turn, dcq_s = r.dmix_s, r.dmix_turn, r.cq_turn, r.dcq_s
    a2_turn, rf_out, rf_buf = r.a2_turn, r.rf_out, r.rf_buf

    def mix_back(j):
        put_grad(3, j, 2 * w, dot(dz_turn[...], mix[j].astype(bf16), 1, 0).astype(bf16))
        dmix = dot(dz[...], wbuf[3, :, block_of(j, width)][:, 2 * w:3 * w], 1, 0) * inv_s[j]
        dmix_s[j] = dmix.astype(bf16)
        dmix_turn[j] = dmix.T.astype(bf16)
        cq_turn[j] = turned(cq[j])
        dcq_s[j] = jnp.zeros_like(dcq_s[j])
    loop(n_t, mix_back)
    fold_start(3)
    rf_copies = [remote(rf_out.at[k], rf_buf.at[k], r.rf_ss.at[k], r.rf_rs.at[k], z_peers[k]) for k in z_range]

    def keys_back(part, j):
        block = wbuf[2, :, block_of(j, width)]
        piece_rows = block_of(part, rows)
        k_p, v_p = kv[j, piece_rows, :][:, 0:w], kv[j, piece_rows, :][:, w:2 * w]
        product = dmix_s[j].astype(f32) * mix[j]
        for h in range(local_heads):
            mask = head_mask((rows, w), 1, head_dim, h)
            turn_mask = head_mask((w, rows), 0, head_dim, h)
            head = j * local_heads + h
            delta = jnp.sum(keep(mask, product), axis=-1, keepdims=True)
            p_h = probs[head, :, piece_rows]
            grad_p = dot(keep(mask, dmix_s[j]), v_p, 1, 1)
            ds = (p_h.astype(f32) * (grad_p - delta)).astype(bf16)
            probs[head, :, piece_rows] = ds
            dv_h = dot(keep(turn_mask, dmix_turn[j]), p_h, 1, 0)
            dk_h = dot(keep(turn_mask, cq_turn[j]), ds, 1, 0)
            dcq_h = keep(mask, dot(ds, k_p, 1, 0))
            if h == 0:
                dv, dk, dcq = dv_h, dk_h, dcq_h
            else:
                dv, dk, dcq = dv + dv_h, dk + dk_h, dcq + dcq_h
        dcq_s[j] = dcq_s[j] + dcq
        dkv = jnp.concatenate([(dk * scale).T, dv.T], axis=1).astype(bf16)
        kv[j, piece_rows, :] = dkv
        z_s[...] = z_s[...] + dot(dkv, block[:, w:3 * w], 1, 1)

    assert len(fold_plan_one) <= n_t
    for k in range(n_t):
        z_s[...] = jnp.zeros_like(z_s)
        part = lax.rem(t + 1 + k, n_t)
        loop(n_t, functools.partial(keys_back, part), 2)
        if k < n_t - 1:
            rf_out[k] = z_s[...].astype(bf16)
            rf_copies[k].start()
        for c, stage in fold_plan_one[k] if k < len(fold_plan_one) else ():
            fold_step(c, stage, stage < n_link)
    for part in range(n_t):
        a2_turn[:, part * rows:(part + 1) * rows] = turned(a2_all[part])
    small[:, KERNEL:, :] = jnp.zeros_like(small[:, KERNEL:, :])


    def queries_back(j):
        block = wbuf[2, :, block_of(j, width)]
        pq_turn = turned(pq[j])
        for h in range(local_heads):
            mask = head_mask((rows, w), 1, head_dim, h)
            turn_mask = head_mask((w, rows), 0, head_dim, h)
            back = dot(probs[j * local_heads + h], phase[...], 1, 0)
            spun(back[:, :D // 2], back[:, D // 2:])
            dpq_h = keep(mask, dot(u_s[...], block[:, 3 * w:4 * w], 1, 0))
            pos_h = dot(keep(turn_mask, pq_turn), u_s[...], 1, 0)
            if h == 0:
                dpq, pos = dpq_h, pos_h
            else:
                dpq, pos = dpq + dpq_h, pos + pos_h
        dcq = dcq_s[j] * scale
        dpq = dpq * scale
        small[j, KERNEL:KERNEL + 1, :] = jnp.sum(dcq, axis=0, keepdims=True)
        small[j, KERNEL + 1:KERNEL + 2, :] = jnp.sum(dpq, axis=0, keepdims=True)
        dq = (dcq + dpq).astype(bf16)
        z_s[...] = z_s[...] + dot(dq, block[:, 0:w], 1, 1)
        put_grad(2, j, 0, dot(a2_turn[:, block_of(t, rows)], dq, 1, 0).astype(bf16))
        put_grad(2, j, w, dot(a2_turn[...], kv[j], 1, 0).astype(bf16))
        put_grad(2, j, 3 * w, (pos.T * scale).astype(bf16))

    def fold_some(plan):
        for c, stage in plan:
            fold_step(c, stage, stage < n_link)
    middle_plan = [(4, stage) for stage in range(2, n_link + 1)]
    halves(n_t, queries_back, lambda: fold_some(middle_plan), 2)

    fold_start(2)
    small_z, small_mid, small_buf = r.small_z, r.small_mid, r.small_buf
    small_z_copies = [remote(small.at[lax.rem(t + k + 1, n_t)], small_z.at[k], r.sz_send.at[0], r.sz_recv.at[0],
                             z_peers[k]) for k in z_range]
    small_copies = [remote(small_mid, small_buf.at[k], r.s_send.at[0], r.s_recv.at[0], d_peers[k])
                    for k in range(n_dp - 1)]

    def small_middle():
        settled(small_z, r.sz_recv.at[0], before)
        total = small[t]
        for k in z_range:
            total = total + small_z[k]
        small_mid[...] = total
        start_all(small_copies)
    start_all(small_z_copies)
    a_turn[...] = turned(a1[...])
    fold_some([(3, 1)])
    fold_step(2, 0)
    arrive_all(rf_copies)

    def join_rows(part):
        total = z_s[part, :]
        for k in z_range:
            total = total + rf_buf[k, part, :].astype(f32)
        z_s[part, :] = total
    row_loop(rows, NORM_ROWS, join_rows)
    join_norm(1, lambda part: x1[part, :], 0.5)
    fold_some([(3, stage) for stage in range(2, n_link + 1)])
    for c in (5, 4, 3):
        fold_send(c)

    dz_turn[...] = turned(dz[...])
    def fold_middle():
        fold_step(1, 0)

    feed_back(dz, dz_turn, a_turn, wbuf.at[0], wbuf.at[1], z_s, r.hid1, r.slope1, grad_chunk(0), grad_chunk(1),
              lambda: fold_start(1), fold_middle)
    fold_start(0)
    join_norm(0, lambda part: x_ref[part, :].astype(f32), 1.0)
    leave(r.dx0)

    gsum_copies = [remote(gsum, r.gsum_buf.at[k], r.g_send.at[0], r.g_recv.at[0], d_peers[k])
                   for k in range(n_dp - 1)]
    gsum_z_copies = [remote(r.gsum_mid, r.gsum_z.at[k], r.gz_send.at[0], r.gz_recv.at[0], z_peers[k])
                     for k in z_range]
    start_all(gsum_copies)

    def gsum_middle():
        settled(r.gsum_buf, r.g_recv.at[0], before)
        total = gsum[...]
        for k in range(n_dp - 1):
            total = total + r.gsum_buf[k]
        r.gsum_mid[...] = total
        start_all(gsum_z_copies)
    small_middle()
    for u, stage, go, other in tail_plan(final):
        fold_unit(u, stage, go)
        if other is not None:
            start_all(fold_copies(other, 0))
        if (u, stage) == ((0, CUTS - 1), 1):
            gsum_middle()
    settled(small_buf, r.s_recv.at[0], before)
    total = small_mid[...]
    for k in range(n_dp - 1):
        total = total + small_buf[k]
    r.g_taps[...] = total[0:KERNEL, :]
    for pair in range(2):
        row = total[KERNEL + pair:KERNEL + pair + 1, :]
        for h in range(local_heads):
            place = lax.broadcasted_iota(jnp.int32, (n_bias, w), 1)
            spot_h = (place == lax.broadcasted_iota(jnp.int32, (n_bias, w), 0) + d * n_bias + h * head_dim).astype(f32)
            r.g_bias[pair, h:h + 1, :] = lax.dot_general(row, spot_h, (((1,), (1,)), ((), ())), precision=high,
                                                         preferred_element_type=f32)
    settled(r.gsum_z, r.gz_recv.at[0], before)
    total_g = r.gsum_mid[...]
    for k in z_range:
        total_g = total_g + r.gsum_z[k]
    spot_g = lax.dot_general(total_g, gain_spot, (((1,), (1,)), ((), ())), precision=high, preferred_element_type=f32)
    r.g_gains[...] = spot_g[0:5, :]

    leave(r.g_taps, r.g_bias, r.g_gains)
    for k, name in enumerate(leaving):
        pltpu.make_async_copy(getattr(r, name[:-len(HBM)]), getattr(r, name), r.out_sem.at[k]).wait()
    settled(taps.at[pl.ds(0, n_t - 1)], r.f_send.at[0], before)
    settled(a2_all.at[pl.ds(0, n_t - 1)], r.a_send.at[0], before)
    settled(small_z, r.sz_send.at[0], before)
    settled(r.gsum_z, r.gz_send.at[0], before)
    sent_all(rf_copies)
    settled(e_buf.at[pl.ds(0, n_t - 1)], r.e_send.at[0], before)
    sent_all(e_copies(n_t - 1, n_t + n_link))
    for k in range(2):
        settled(sum_buf.at[k], r.sum_send.at[k], before)
        settled(sum_z.at[k], r.sumz_send.at[k], before)
    settled(small_buf, r.s_send.at[0], before)
    settled(r.gsum_buf, r.g_send.at[0], before)
    settled(gbuf.at[pl.ds(0, CHUNKS // 2)], r.core_send.at[0], before)
    settled(gbuf.at[0, pl.ds(0, CHUNKS * rows_w), pl.ds(0, (n_t - 1) * width)], r.fz_send.at[0], before)
    for c in range(CHUNKS):
        settled(gbuf.at[0, pl.ds(0, (len(groups) - 1) * rows_w), :], r.fd_send.at[c], before)


def layer_kernel(n_dp, n_t, head_dim, inputs):
    given = SimpleNamespace(**inputs)
    rows, D = given.x.shape
    rows_w, width = given.fu.shape
    w = D // n_t
    frames = rows * n_t
    heads = D // head_dim
    hidden = n_t * width
    n_bits = n_dp.bit_length() - 1
    n_e = n_t - 1 + n_bits
    n_gain = given.gain_in.shape[1]
    n_bias = given.bias_in.shape[2]
    tap_rows = 40
    groups = n_dp // 2
    z = n_t - 1
    sem = pltpu.SemaphoreType.DMA
    vm = pltpu.VMEM
    outs = dict(
        out=((rows, D), f32), dx0=((rows, D), f32), g_gains=((5, n_gain), f32), g_fu=((rows_w, width), f32),
        g_fd=((rows_w, width), f32), g_at=((4, rows_w, w), f32), g_ao=((rows_w, w), f32),
        g_bias=((2, w // head_dim, n_bias), f32), g_cw=((rows_w, 2, w), f32), g_taps=((KERNEL, w), f32),
        g_bn=((2, w), f32), g_co=((rows_w, w), f32), g_su=((rows_w, width), f32), g_sd=((rows_w, width), f32))
    edge_shape = (n_t, rows + 2 * EDGE, w)
    scratch = dict(
        pack=vm((2, rows_w, width), bf16), taps_own=vm((tap_rows, w), f32), wbuf=vm((CHUNKS, n_dp * rows_w, hidden), bf16),
        gbuf=vm((CHUNKS - 2, n_dp * rows_w, hidden), bf16), gains=vm((8, D), f32),
        taps=vm((n_t, tap_rows, w), f32), e_acc=vm((n_bits + 2, 8, D), f32), e_buf=vm((n_e, 8, D), f32),
        phase=vm((frames, D), bf16), spin=vm((2, rows, D // 2), f32), u_s=vm((rows, D), bf16),
        z_s=vm((rows, D), f32), x1=vm((rows, D), f32), x2=vm((rows, D), f32),
        x3=vm((rows, D), f32), a1=vm((rows, D), bf16), a2=vm((rows, D), bf16), a3=vm((rows, D), bf16),
        a4=vm((rows, D), bf16), dz=vm((rows, D), bf16), dz_turn=vm((D, rows), bf16),
        a_turn=vm((D, rows), bf16), a2_all=vm((n_t, rows, D), bf16), a2_turn=vm((D, frames), bf16),
        hid1=vm((rows, hidden), bf16), slope1=vm((rows, hidden), bf16), hid2=vm((rows, hidden), bf16),
        slope2=vm((rows, hidden), bf16), kv=vm((n_t, frames, 2 * w), bf16), cq=vm((n_t, rows, w), bf16),
        pq=vm((n_t, rows, w), bf16), mix=vm((n_t, rows, w), f32), inv_s=vm((n_t, rows, w), f32), probs=vm((heads, rows, frames), bf16),
        s_s=vm((rows, frames), f32), dmix_s=vm((n_t, rows, w), bf16), dmix_turn=vm((n_t, w, rows), bf16),
        cq_turn=vm((n_t, w, rows), bf16), dcq_s=vm((n_t, rows, w), f32),
        rf_out=vm((z, rows, D), bf16), rf_buf=vm((z, rows, D), bf16),
        glu=vm(edge_shape, f32), bhat=vm(edge_shape, f32), dbn=vm(edge_shape, f32),
        val=vm((n_t, rows, w), f32), sig=vm((n_t, rows, w), f32), act=vm((n_t, rows, w), bf16),
        de=vm((rows, 2 * w), bf16), sums=vm((2, 2 * n_t, w), f32), sum_mid=vm((2, 2 * n_t, w), f32),
        sum_out=vm((2, 2 * n_t, w), f32), sum_buf=vm((2, n_dp - 1, 2 * n_t, w), f32),
        sum_z=vm((2, z, 2 * n_t, w), f32), core_buf=vm((CHUNKS, groups, rows_w, hidden), bf16),
        dp_buf=vm((CHUNKS, 2, groups - 1, rows_w, hidden // 2), bf16), z_buf=vm((CHUNKS, z, rows_w, width), bf16),
        small=vm((n_t, tap_rows, w), f32), small_buf=vm((n_dp - 1, tap_rows, w), f32),
        small_mid=vm((tap_rows, w), f32), small_z=vm((z, tap_rows, w), f32), gsum=vm((8, D), f32),
        gsum_buf=vm((n_dp - 1, 8, D), f32), gsum_mid=vm((8, D), f32), gsum_z=vm((z, 8, D), f32), local_sem=sem((CHUNKS, CUTS)))
    n_link = n_bits - 1
    scratch.update(
        z_send=sem((1,)), z_recv=sem((CHUNKS, CUTS)), d_send=sem((CHUNKS,)), d_recv=sem((CHUNKS, CUTS, n_bits)),
        f_send=sem((1,)), f_recv=sem((1,)), e_send=sem((n_bits + 1,)), e_recv=sem((n_bits + 1,)),
        a_send=sem((1,)), a_recv=sem((1,)), edge_send=sem((3, 2)), edge_recv=sem((3, 2)),
        sum_send=sem((2,)), sum_recv=sem((2,)), sumz_send=sem((2,)), sumz_recv=sem((2,)),
        core_send=sem((1,)), core_recv=sem((CHUNKS, CUTS)), fd_send=sem((CHUNKS,)),
        fd_recv=sem((CHUNKS, CUTS, n_link)), fz_send=sem((1,)), fz_recv=sem((CHUNKS, CUTS)),
        rf_ss=sem((z,)), rf_rs=sem((z,)), s_send=sem((1,)), s_recv=sem((1,)),
        sz_send=sem((1,)), sz_recv=sem((1,)), g_send=sem((1,)), g_recv=sem((1,)),
        gz_send=sem((1,)), gz_recv=sem((1,)))
    for name, (dims, kind) in outs.items():
        scratch[name] = vm(dims, kind)
    scratch.update(out_sem=sem((len(outs),)))
    names = list(inputs) + [name + HBM for name in outs] + list(scratch)
    vmem = pl.BlockSpec(memory_space=pltpu.VMEM)
    result = pl.pallas_call(
        functools.partial(layer_body, names, n_dp, n_t, head_dim),
        name="layer",
        out_shape=tuple(jax.ShapeDtypeStruct(dims, kind) for dims, kind in outs.values()),
        in_specs=[vmem] * len(inputs),
        out_specs=(pl.BlockSpec(memory_space=pl.ANY),) * len(outs),
        scratch_shapes=list(scratch.values()),
        compiler_params=pltpu.CompilerParams(collective_id=0, has_side_effects=True, vmem_limit_bytes=67043328),
    )(*inputs.values())
    return result


def settle_body(*refs):
    count = (len(refs) - 2) // 3
    sources, results, rooms = refs[:count], refs[count:2 * count], refs[2 * count:3 * count]
    sem_in, sem_out = refs[3 * count:]
    loads = [pltpu.make_async_copy(a, b, sem_in.at[k]) for k, (a, b) in enumerate(zip(sources, rooms))]
    stores = [pltpu.make_async_copy(a, b, sem_out.at[k]) for k, (a, b) in enumerate(zip(rooms, results))]
    for copy in loads:
        copy.start()
    for load, store in zip(loads, stores):
        load.wait()
        store.start()
    for copy in stores:
        copy.wait()


def settle(arrays):
    hbm = pl.BlockSpec(memory_space=pl.ANY)
    count = len(arrays)
    sem = pltpu.SemaphoreType.DMA
    return pl.pallas_call(
        settle_body,
        name="settle",
        out_shape=tuple(jax.ShapeDtypeStruct(a.shape, a.dtype) for a in arrays),
        in_specs=[hbm] * count,
        out_specs=(hbm,) * count,
        scratch_shapes=[pltpu.VMEM(a.shape, a.dtype) for a in arrays] + [sem((count,)), sem((count,))],
    )(*arrays)


def angle_tables(frames, width):
    step = 32
    frequency = np.exp(np.arange(width // 2) * (-2.0 * math.log(10000.0) / width))
    coarse = np.arange(frames // step)[:, None] * step * frequency
    fine = np.arange(step)[:, None] * frequency
    return jnp.asarray(np.stack([np.sin(coarse), np.cos(coarse), np.sin(fine), np.cos(fine)]), f32)


def per_device(n_dp, n_t, inputs, out_grad, norm_gains, first_up, first_down, attend_in, attend_out, position_bias,
               convolve_in, depth_kernel, batch_norm, convolve_out, second_up, second_down):
    rows, D = inputs.shape
    w = attend_in.shape[2]
    R = attend_in.shape[1]
    n_bias = position_bias.shape[2]
    head_dim = n_bias * n_dp
    got = layer_kernel(n_dp, n_t, head_dim, dict(
        fu=first_up, fd=first_down.T, at=attend_in, cw=convolve_in, ao=attend_out.T, co=convolve_out.T, su=second_up,
        sd=second_down.T, gain_in=norm_gains, bias_in=position_bias, tap_in=depth_kernel.T, bn_in=batch_norm, x=inputs,
        og=out_grad, tab=angle_tables(rows * n_t, D)))
    (out, dx0, g_gains, g_fu, g_fd, g_at, g_ao, g_bias, g_cw, g_taps, g_bn, g_co, g_su, g_sd) = settle(got)
    return (out, dx0, g_gains, g_fu, g_fd.T, g_at, g_ao.T, g_bias, g_cw, g_taps.T, g_bn, g_co.T, g_su, g_sd.T)


def solution(mesh):
    n_dp, n_t = mesh.shape["dp"], mesh.shape["tensor"]
    row = P(("dp", "tensor"), None)
    gain = P(None, ("dp", "tensor"))
    up = P("dp", "tensor")
    down = P("tensor", "dp")
    weights = (up, down, P(None, "dp", "tensor"), down, P(None, "tensor", "dp"), P("dp", None, "tensor"),
               P("tensor", None), P(None, "tensor"), down, up, down)
    return jax.shard_map(
        functools.partial(per_device, n_dp, n_t), mesh=mesh,
        in_specs=(row, row, gain) + weights,
        out_specs=(row, row, gain) + weights,
        check_vma=False)
```
